256 devices in a mesh: gx: 8 (over y, core), gy: 32 (over z, x).
Axes of the slice: x: 4, y: 4, z: 8, core: 2. Of those that a mesh axis runs over, the one named last changes fastest.
Arguments:
- offsets: float32 [2, 16, 256, 128], P(None, 'gx', 'gy'), may hold values from 0 to 1
- masses: float32 [16, 256, 128], P('gx', 'gy'), may hold values from 0.01 to 0.04
- counts: int32 [16, 256], P('gx', 'gy'), may hold values from 1 to 128, as said below
- source: float32 [16, 256, 128], P('gx', 'gy'), may hold values from -6 to 6
Outputs:
- density: float32 [16, 256, 128], P('gx', 'gy')
- pressure: float32 [16, 256, 128], P('gx', 'gy')
- residual: float32 [16, 256, 128], P('gx', 'gy')
- peaks: float32 [5], replicated
The draws below stay inside these ranges and needn't reach their ends.
Inputs may be any that keep to these rules, and one draw needn't show every extreme that they name: `counts`: each cell's occupied slots come first; some cell holds 128 particles.
All inputs are finite; a program needn't handle non-finite values.
Results may differ from the reference program's by a relative error of at most 0.0003.
Values sent between devices are 32-bit elements; how exact they have to be, the bound alone decides.
A program may use at most 64 MiB of HBM per device.

```python
import math
import jax
import jax.numpy as jnp
from jax import lax

SLOT = 128
ITERS = 5
NX = 16
NY = 256


def draw_counts(key, part):
    coarse_key = jax.random.fold_in(key, 11)
    fine_key = jax.random.fold_in(key, 12)
    region_rows = (NX + 3) // 4
    region_cols = (NY + 3) // 4
    floor_count = jax.random.randint(coarse_key, (region_rows, region_cols), 1, SLOT + 1)
    floor_count = jnp.repeat(jnp.repeat(floor_count, 4, axis=0), 4, axis=1)[:NX, :NY]
    counts = jax.random.randint(fine_key, (NX, NY), floor_count, SLOT + 1)
    return counts.at[0, 0].set(SLOT).astype(jnp.int32)


def draw_source(key, part):
    rough = jnp.clip(jax.random.normal(jax.random.fold_in(key, 21), (NX, NY, SLOT), jnp.float32), -6.0, 6.0)
    return rough


def level_of(key, dims, cuts, least, top_value):
    def one(dim, parts):
        steps = jax.random.uniform(jax.random.fold_in(jax.random.fold_in(key, 6), dim), (parts,), jnp.float32, least / len(cuts), top_value / len(cuts))
        return jnp.repeat(jnp.exp(steps), dims[dim] // parts).reshape((-1,) + (1,) * (len(dims) - dim - 1))

    level = one(*cuts[0])
    for cut in cuts[1:]:
        level = level * one(*cut)
    return level


def setup_inputs(seed: int = 0) -> dict:
    key_list = jax.random.split(jax.random.key(seed), 5)
    return {
        "offsets": jnp.clip(1.0 * jax.random.uniform(key_list[0], (2, NX, NY, SLOT), jnp.float32) ** level_of(key_list[0], (2, NX, NY, SLOT), ((1, 8), (2, 32)), -0.2, 0.2), 0.0, 1.0),
        "masses": jnp.clip(jnp.exp(math.log(0.04) - 1.3862944 * jax.random.uniform(key_list[1], (NX, NY, SLOT), jnp.float32) ** level_of(key_list[1], (NX, NY, SLOT), ((0, 8), (1, 32)), -0.2, 0.2)), 0.01, 0.04),
        "counts": draw_counts(jax.random.fold_in(key_list[4], 71), 0),
        "source": draw_source(jax.random.fold_in(key_list[4], 71), 0),
    }


BASE_STIFF = 0.5
PAIR_SCALE = 0.05
NEIGHBOUR_STEPS = [(step_x, step_y) for step_x in (-1, 0, 1) for step_y in (-1, 0, 1)]


def near_view(padded, step_x, step_y):
    row_count = padded.shape[-3] - 2
    col_count = padded.shape[-2] - 2
    return padded[..., 1 + step_x:1 + step_x + row_count, 1 + step_y:1 + step_y + col_count, :]


def kernel_terms(own_cells, nearby, step_x, step_y):
    offset_x = (step_x + nearby[0][..., None, :]) - own_cells[0][..., :, None]
    offset_y = (step_y + nearby[1][..., None, :]) - own_cells[1][..., :, None]
    return jnp.maximum(1.0 - (offset_x * offset_x + offset_y * offset_y), 0.0)


def density_block(padded):
    own_cells = near_view(padded, 0, 0)
    summed = jnp.zeros(own_cells.shape[1:], jnp.float32)
    for step_x, step_y in NEIGHBOUR_STEPS:
        nearby = near_view(padded, step_x, step_y)
        falloff = kernel_terms(own_cells, nearby, step_x, step_y)
        summed = summed + jnp.sum(falloff * falloff * falloff * nearby[2][..., None, :], axis=-1)
    return 1.0 + summed


def pair_weights(padded, step_x, step_y):
    own_cells = near_view(padded, 0, 0)
    nearby = near_view(padded, step_x, step_y)
    falloff = kernel_terms(own_cells, nearby, step_x, step_y)
    pairing = own_cells[3][..., :, None] * nearby[3][..., None, :] * (2.0 * PAIR_SCALE) / (own_cells[4][..., :, None] + nearby[4][..., None, :])
    return falloff * falloff * pairing


def diag_block(padded):
    own_cells = near_view(padded, 0, 0)
    summed = jnp.zeros(own_cells.shape[1:], jnp.float32)
    for step_x, step_y in NEIGHBOUR_STEPS:
        summed = summed + jnp.sum(pair_weights(padded, step_x, step_y), axis=-1)
    return BASE_STIFF + summed


def apply_block(padded, padded_field):
    own_cells = near_view(padded, 0, 0)
    summed = jnp.zeros(own_cells.shape[1:], jnp.float32)
    for step_x, step_y in NEIGHBOUR_STEPS:
        summed = summed + jnp.einsum('xyij,xyj->xyi', pair_weights(padded, step_x, step_y), near_view(padded_field, step_x, step_y), precision=lax.Precision.HIGHEST)
    return summed


def reference(offsets, masses, counts, source):
    slot_count = offsets.shape[-1]
    occupied = (jnp.arange(slot_count, dtype=jnp.int32)[None, None, :] < counts[:, :, None]).astype(jnp.float32)
    fields = jnp.stack([offsets[0], offsets[1], masses * occupied, occupied])
    padded = jnp.pad(fields, ((0, 0), (1, 1), (1, 1), (0, 0)))
    row_ids = jnp.arange(fields.shape[1], dtype=jnp.int32)
    density = lax.map(lambda row_index: density_block(lax.dynamic_slice_in_dim(padded, row_index, 3, 1))[0], row_ids)
    full = jnp.concatenate([padded, jnp.pad(density, ((1, 1), (1, 1), (0, 0)))[None]], 0)
    diagonal = lax.map(lambda row_index: diag_block(lax.dynamic_slice_in_dim(full, row_index, 3, 1))[0], row_ids)

    def operate(vector):
        padded_field = jnp.pad(vector, ((1, 1), (1, 1), (0, 0)))
        sums = lax.map(lambda row_index: apply_block(lax.dynamic_slice_in_dim(full, row_index, 3, 1), lax.dynamic_slice_in_dim(padded_field, row_index, 3, 0))[0], row_ids)
        return diagonal * vector - sums

    pressure = jnp.zeros_like(source)
    residual = source * occupied
    scaled = residual / diagonal
    direction = scaled
    precond_now = jnp.sum(residual * scaled)
    peak_list = []
    for step in range(ITERS):
        image = operate(direction)
        step_size = precond_now / jnp.sum(direction * image)
        pressure = pressure + step_size * direction
        residual = residual - step_size * image
        peak_list.append(jnp.max(jnp.abs(residual)))
        scaled = residual / diagonal
        precond_next = jnp.sum(residual * scaled)
        direction = scaled + (precond_next / precond_now) * direction
        precond_now = precond_next
    return density, pressure, residual, jnp.stack(peak_list)
```

```python
import functools

import jax
import jax.numpy as jnp
from jax import lax
from jax.experimental import pallas as pl
from jax.experimental.pallas import tpu as pltpu
from jax.sharding import PartitionSpec as P

MESH = pl.DeviceIdType.MESH
F32 = jnp.float32

ITERS = 5
SLOT = 128
ROWS = 16
COLS = 256
GX = 8
XLEN = 4
ZLEN = 8
PLANE = GX * XLEN
BASE_STIFF = 0.5
FAR = 1000.0
LOW, HIGH = -0.05, 0.85
MID, HALF = (LOW + HIGH) / 2, (HIGH - LOW) / 2
PAIRS = [(i, j) for i in range(ITERS) for j in range(i, ITERS)] + [(i, ITERS) for i in range(ITERS)]
LOOP = 4


def snake(q):
    z, x = lax.div(q, XLEN), lax.rem(q, XLEN)
    return z * XLEN + x + lax.rem(z, 2) * (XLEN - 1 - 2 * x)


def mirrored(g, a):
    return a + lax.rem(g, 2) * (GX - 1 - 2 * a)


def device_of(column):
    group, place = lax.div(column, GX), lax.rem(column, GX)
    return mirrored(group, place), snake(group)


def body(
    off_ref, mass_ref, cnt_ref, src_ref,
    dens_ref, pres_ref, resid_ref, peaks_ref,
    sbuf, inb, xcol, ycol, rcol, wts, part, rb, vb, rows_s, ub, gb,
    g1s, g1, g2s, g2, p1s, p1, p2s, p2, osb, ob,
    in_send, in_recv, rho_send, rho_recv, halo_send, halo_recv,
    red_send, red_recv, out_send, out_recv,
):
    a, q = lax.axis_index("gx"), lax.axis_index("gy")
    z, x = lax.div(q, XLEN), lax.rem(q, XLEN)
    group = snake(q)
    place = mirrored(group, a)
    column = group * GX + place
    has_left, has_right = column > 0, column < COLS - 1
    left = device_of(jnp.maximum(column - 1, 0))
    right = device_of(jnp.minimum(column + 1, COLS - 1))
    plane_index = a * XLEN + x

    inb[...] = jnp.zeros_like(inb)
    rb[...] = jnp.zeros_like(rb)
    vb[...] = jnp.zeros_like(vb)
    osb[...] = jnp.zeros_like(osb)

    barrier = pltpu.get_barrier_semaphore()

    def plane_mate(t):
        other = lax.rem(plane_index + t, PLANE)
        return lax.div(other, XLEN), z * XLEN + lax.rem(other, XLEN)

    def tower_mate(t):
        return a, lax.rem(z + t, ZLEN) * XLEN + x

    def greet(target):
        pl.semaphore_signal(barrier, inc=1, device_id=target, device_id_type=MESH)

    for t in range(1, PLANE):
        greet(plane_mate(t))
    for t in range(1, ZLEN):
        greet(tower_mate(t))
    low_edge = (lax.rem(column, PLANE) == 0) & has_left
    high_edge = (lax.rem(column, PLANE) == PLANE - 1) & has_right
    for edge, step in ((low_edge, -1), (high_edge, 1)):
        @pl.when(edge)
        def _(step=step):
            for k in range(GX):
                greet((k, group + step))

    lane = lax.broadcasted_iota(jnp.int32, (1, SLOT), 1)
    for r in range(2):
        for c in range(GX):
            occ = jnp.where(lane < cnt_ref[r, c], 1.0, 0.0).astype(F32)
            sbuf[c, r, 0:1, :] = off_ref[0, r, c : c + 1, :]
            sbuf[c, r, 1:2, :] = off_ref[1, r, c : c + 1, :]
            sbuf[c, r, 2:3, :] = mass_ref[r, c : c + 1, :] * occ
            sbuf[c, r, 3:4, :] = src_ref[r, c : c + 1, :] * occ

    low_block = (x == 0) & (q > 0)
    high_block = (x == XLEN - 1) & (q < COLS // GX - 1)
    awaited = PLANE - 1 + ZLEN - 1 + low_block.astype(jnp.int32) + high_block.astype(jnp.int32)
    pl.semaphore_wait(barrier, awaited)

    sends = []
    for c in range(GX):
        for d in (-1, 0, 1):
            target_column = q * GX + c + d
            wanted = jnp.logical_and(target_column >= 0, target_column < COLS)
            ta, tq = device_of(jnp.clip(target_column, 0, COLS - 1))
            wanted = jnp.logical_and(wanted, jnp.logical_or(ta != a, tq != q))
            copy = pltpu.make_async_remote_copy(
                src_ref=sbuf.at[c],
                dst_ref=inb.at[1 - d, pl.ds(1 + 2 * a, 2)],
                send_sem=in_send.at[len(sends)],
                recv_sem=in_recv.at[1 - d],
                device_id=(ta, tq),
                device_id_type=MESH,
            )
            pl.when(wanted)(copy.start)
            sends.append((wanted, copy))
    for d in (-1, 0, 1):
        own = column + d - q * GX
        inside = (own >= 0) & (own < GX)
        copy = pltpu.make_async_copy(
            sbuf.at[jnp.clip(own, 0, GX - 1)],
            inb.at[1 + d, pl.ds(1 + 2 * a, 2)],
            in_recv.at[1 + d],
        )
        pl.when(inside)(copy.start)

    def arrived(slot):
        view = inb.at[slot, pl.ds(1, ROWS)]
        pltpu.make_async_copy(view, view, in_recv.at[slot]).wait()

    def spread(row):
        return jnp.transpose(jnp.broadcast_to(row, (SLOT, SLOT)))

    def total_row(block):
        return jnp.sum(jnp.transpose(block), axis=0, keepdims=True)

    arrived(1)

    def columns(r, carry):
        xcol[r] = spread(inb[1, r + 1, 0:1, :])
        ycol[r] = spread(inb[1, r + 1, 1:2, :])
        rows_s[0, pl.ds(r, 1), :] = inb[1, r + 1, 2:3, :]
        rows_s[1, pl.ds(r, 1), :] = inb[1, r + 1, 3:4, :]
        return carry

    lax.fori_loop(0, ROWS, columns, 0, unroll=LOOP)
    pl.when(has_left)(lambda: arrived(0))
    pl.when(has_right)(lambda: arrived(2))

    near = [(dc, dr) for dc in (1, 0, 2) for dr in (0, 1, 2)]

    def falloffs(r, carry):
        rows = []
        for dc, dr in near:
            cell = inb[dc, r + dr]
            mass = cell[2:3, :]
            px = (dr - 1.0) + jnp.where(mass > 0.0, cell[0:1, :], FAR)
            py = (dc - 1.0) + cell[1:2, :]
            rows.append((px, py, mass))
        for h in range(0, SLOT, 64):
            xi, yi = xcol[r, h : h + 64, :], ycol[r, h : h + 64, :]
            acc = jnp.zeros((64, SLOT), F32)
            for k, (px, py, mass) in enumerate(rows):
                ox, oy = px - xi, py - yi
                fall = jnp.maximum(1.0 - (ox * ox + oy * oy), 0.0)
                square = fall * fall
                wts[r, k, h : h + 64, :] = square
                acc = acc + square * fall * mass
            part[r, h : h + 64, :] = acc
        return carry

    lax.fori_loop(0, ROWS, falloffs, 0)

    def density_rows(r, carry):
        rb[1, pl.ds(8 + r, 1), :] = 1.0 + total_row(part[r])
        return carry

    lax.fori_loop(0, ROWS, density_rows, 0, unroll=LOOP)

    def exchange(buf, send, recv):
        copies = []
        for k, (have, target, slot) in enumerate(((has_left, left, 2), (has_right, right, 0))):
            copy = pltpu.make_async_remote_copy(
                src_ref=buf.at[1, pl.ds(8, ROWS)],
                dst_ref=buf.at[slot, pl.ds(8, ROWS)],
                send_sem=send.at[k],
                recv_sem=recv.at[slot],
                device_id=target,
                device_id_type=MESH,
            )
            pl.when(have)(copy.start)
            copies.append((have, copy))

        def wait():
            for have, slot in ((has_left, 0), (has_right, 2)):
                view = buf.at[slot, pl.ds(8, ROWS)]
                pl.when(have)(pltpu.make_async_copy(view, view, recv.at[slot]).wait)

        return wait, copies

    wait_rho, rho_copies = exchange(rb, rho_send, rho_recv)
    sends += rho_copies

    def rho_columns(r, carry):
        rcol[r] = spread(10.0 * rb[1, pl.ds(8 + r, 1), :])
        return carry

    lax.fori_loop(0, ROWS, rho_columns, 0, unroll=LOOP)

    def weights(first, last):
        def run(r, carry):
            rows = [10.0 * rb[dc, pl.ds(7 + r + dr, 1), :] for dc, dr in near[first:last]]
            for h in range(0, SLOT, 64):
                ri = rcol[r, h : h + 64, :]
                acc = jnp.zeros((64, SLOT), F32) if first == 0 else part[r, h : h + 64, :]
                for k, row in enumerate(rows, first):
                    w = wts[r, k, h : h + 64, :] / (ri + row)
                    wts[r, k, h : h + 64, :] = w
                    acc = acc + w
                part[r, h : h + 64, :] = acc
            return carry

        lax.fori_loop(0, ROWS, run, 0)

    weights(0, 3)
    wait_rho()
    weights(3, 9)

    def diagonal_rows(r, carry):
        ub[pl.ds(r, 1), :] = BASE_STIFF + total_row(part[r])
        return carry

    lax.fori_loop(0, ROWS, diagonal_rows, 0, unroll=LOOP)

    occ = jnp.where(rows_s[0] > 0.0, 1.0, 0.0).astype(F32)
    diag = ub[...]
    dinv = occ / diag
    basis = [rows_s[1] * dinv]
    gram_rows = {}

    for k in range(ITERS):
        vb[k, 1, pl.ds(8, ROWS), :] = basis[k]
        wait_halo, halo_copies = exchange(vb.at[k], halo_send.at[k], halo_recv.at[k])
        sends += halo_copies

        def apply_own(r, carry):
            acc = wts[r, 0] * vb[k, 1, pl.ds(7 + r, 1), :]
            for m in (1, 2):
                acc = acc + wts[r, m] * vb[k, 1, pl.ds(7 + r + m, 1), :]
            part[r] = acc
            return carry

        lax.fori_loop(0, ROWS, apply_own, 0, unroll=2)
        scaled = basis[k] * diag
        for i in range(k + 1):
            gram_rows[i, k] = jnp.sum(basis[i] * scaled, axis=0, keepdims=True)
        wait_halo()

        def apply_rest(r, carry):
            acc = part[r]
            for m in range(3, 9):
                dc, dr = near[m]
                acc = acc + wts[r, m] * vb[k, dc, pl.ds(7 + r + dr, 1), :]
            ub[pl.ds(r, 1), :] = total_row(acc)
            return carry

        lax.fori_loop(0, ROWS, apply_rest, 0, unroll=LOOP)
        moved = ub[...] * dinv - MID * basis[k]
        if k == 0:
            basis.append(moved * (1.0 / HALF))
        else:
            basis.append(moved * (2.0 / HALF) - basis[k - 1])

    scaled = basis[ITERS] * diag
    for i in range(ITERS):
        gram_rows[i, ITERS] = jnp.sum(basis[i] * scaled, axis=0, keepdims=True)

    sub24 = lax.broadcasted_iota(jnp.int32, (24, SLOT), 0)
    lane24 = lax.broadcasted_iota(jnp.int32, (24, SLOT), 1)
    sub8 = lax.broadcasted_iota(jnp.int32, (8, SLOT), 0)
    lane8 = lax.broadcasted_iota(jnp.int32, (8, SLOT), 1)

    gb[...] = jnp.zeros_like(gb)
    for k, pair in enumerate(PAIRS):
        gb[k : k + 1, :] = gram_rows[pair]
    sums = jnp.sum(gb[...], axis=1, keepdims=True)
    gram_row = jnp.sum(jnp.where(sub24 == lane24, sums, 0.0), axis=0, keepdims=True)

    def gather(row, own, all_refs, mates, index, count, send_sem, recv_sem):
        own[0] = row
        copies = []
        for t in range(1, count):
            copy = pltpu.make_async_remote_copy(
                src_ref=own.at[0],
                dst_ref=all_refs.at[index],
                send_sem=send_sem,
                recv_sem=recv_sem,
                device_id=mates(t),
                device_id_type=MESH,
            )
            copy.start()
        all_refs[index] = row

        def wait():
            view = all_refs.at[pl.ds(0, count - 1)]
            pltpu.make_async_copy(view, view, recv_sem).wait()

        def wait_sent():
            view = all_refs.at[pl.ds(0, count - 1)]
            pltpu.make_async_copy(view, view, send_sem).wait()

        return wait, wait_sent

    wait_plane, sent_plane = gather(gram_row, g1s, g1, plane_mate, plane_index, PLANE, red_send.at[0], red_recv.at[0])
    wait_plane()
    wait_tower, sent_tower = gather(jnp.sum(g1[...], axis=0), g2s, g2, tower_mate, z, ZLEN, red_send.at[1], red_recv.at[1])
    wait_tower()
    total = jnp.sum(g2[...], axis=0)

    entries = jnp.broadcast_to(
        jnp.sum(jnp.where(sub24 == lane24, total, 0.0), axis=1, keepdims=True), (24, SLOT)
    )
    gram = {}
    for k, (i, j) in enumerate(PAIRS):
        gram[i, j] = gram[j, i] = entries[k : k + 1, :]

    def dot(left_side, right_side):
        out = None
        for i, u in enumerate(left_side):
            inner = None
            for j, v in enumerate(right_side):
                term = gram[i, j] * v
                inner = term if inner is None else inner + term
            out = u * inner if out is None else out + u * inner
        return out

    one = jnp.ones((1, SLOT), F32)
    zero = jnp.zeros((1, SLOT), F32)
    solution_at, residual_at, direction = [], [one], [one]
    residuals = []
    rz = gram[0, 0]
    for k in range(ITERS):
        image = [zero] * (k + 2)
        for j, u in enumerate(direction):
            image[j] = image[j] + (1.0 - MID) * u
            if j == 0:
                image[1] = image[1] - HALF * u
            else:
                image[j + 1] = image[j + 1] - (HALF / 2) * u
                image[j - 1] = image[j - 1] - (HALF / 2) * u
        step = rz / dot(direction, image)
        solution_at = [
            (solution_at[j] if j < len(solution_at) else zero) + step * u for j, u in enumerate(direction)
        ]
        residual_at = [
            (residual_at[j] if j < len(residual_at) else zero) - step * u for j, u in enumerate(image)
        ]
        residuals.append(residual_at)
        if k + 1 < ITERS:
            new = dot(residual_at, residual_at)
            ratio = new / rz
            direction = [
                u + (ratio * direction[j] if j < len(direction) else zero) for j, u in enumerate(residual_at)
            ]
            rz = new

    def combine(factors):
        out = None
        for u, v in zip(factors, basis):
            out = u * v if out is None else out + u * v
        return out

    pressure = combine(solution_at)
    gb[0:8, :] = jnp.zeros((8, SLOT), F32)
    for k in range(ITERS):
        field = combine(residuals[k]) * diag
        gb[k : k + 1, :] = jnp.max(jnp.abs(field), axis=0, keepdims=True)
    peak = jnp.max(gb[0:8, :], axis=1, keepdims=True)
    peak_row = jnp.sum(jnp.where(sub8 == lane8, peak, 0.0), axis=0, keepdims=True)
    wait_peaks, sent_peaks = gather(peak_row, p1s, p1, plane_mate, plane_index, PLANE, red_send.at[2], red_recv.at[2])

    density = rb[1, pl.ds(8, ROWS), :]
    for r in range(ROWS):
        osb[r, 0:1, :] = density[r : r + 1, :]
        osb[r, 1:2, :] = pressure[r : r + 1, :]
        osb[r, 2:3, :] = field[r : r + 1, :]
    for k in range(GX):
        wanted = jnp.logical_or(a != k, group != q)
        copy = pltpu.make_async_remote_copy(
            src_ref=osb.at[pl.ds(2 * k, 2)],
            dst_ref=ob.at[place],
            send_sem=out_send.at[k],
            recv_sem=out_recv,
            device_id=(k, group),
            device_id_type=MESH,
        )
        pl.when(wanted)(copy.start)
        sends.append((wanted, copy))
    local = pltpu.make_async_copy(osb.at[pl.ds(2 * a, 2)], ob.at[place], out_recv)
    pl.when(group == q)(local.start)

    wait_peaks()
    wait_top, sent_top = gather(jnp.max(p1[...], axis=0), p2s, p2, tower_mate, z, ZLEN, red_send.at[3], red_recv.at[3])
    pltpu.make_async_copy(ob, ob, out_recv).wait()
    for r in range(2):
        for c in range(GX):
            dens_ref[r, c : c + 1, :] = ob[c, r, 0:1, :]
            pres_ref[r, c : c + 1, :] = ob[c, r, 1:2, :]
            resid_ref[r, c : c + 1, :] = ob[c, r, 2:3, :]
    wait_top()
    peaks_ref[...] = jnp.max(p2[...], axis=0)

    for wanted, copy in sends:
        pl.when(wanted)(copy.wait_send)
    for wait in (sent_plane, sent_tower, sent_peaks, sent_top):
        wait()


def shard(offsets, masses, counts, source):
    block = jax.ShapeDtypeStruct((2, GX, SLOT), F32)
    vmem = pl.BlockSpec(memory_space=pltpu.VMEM)
    dma = pltpu.SemaphoreType.DMA
    cells = (ROWS, SLOT, SLOT)
    density, pressure, residual, peaks = pl.pallas_call(
        body,
        out_shape=(block, block, block, jax.ShapeDtypeStruct((1, SLOT), F32)),
        in_specs=[vmem, vmem, pl.BlockSpec(memory_space=pltpu.SMEM), vmem],
        out_specs=(vmem, vmem, vmem, vmem),
        scratch_shapes=[
            pltpu.VMEM((GX, 2, 4, SLOT), F32),
            pltpu.VMEM((3, ROWS + 2, 4, SLOT), F32),
            pltpu.VMEM(cells, F32),
            pltpu.VMEM(cells, F32),
            pltpu.VMEM(cells, F32),
            pltpu.VMEM((ROWS, 9, SLOT, SLOT), F32),
            pltpu.VMEM(cells, F32),
            pltpu.VMEM((3, 32, SLOT), F32),
            pltpu.VMEM((ITERS, 3, 32, SLOT), F32),
            pltpu.VMEM((2, ROWS, SLOT), F32),
            pltpu.VMEM((ROWS, SLOT), F32),
            pltpu.VMEM((24, SLOT), F32),
            pltpu.VMEM((1, 1, SLOT), F32),
            pltpu.VMEM((PLANE, 1, SLOT), F32),
            pltpu.VMEM((1, 1, SLOT), F32),
            pltpu.VMEM((ZLEN, 1, SLOT), F32),
            pltpu.VMEM((1, 1, SLOT), F32),
            pltpu.VMEM((PLANE, 1, SLOT), F32),
            pltpu.VMEM((1, 1, SLOT), F32),
            pltpu.VMEM((ZLEN, 1, SLOT), F32),
            pltpu.VMEM((ROWS, 4, SLOT), F32),
            pltpu.VMEM((GX, 2, 4, SLOT), F32),
            dma((24,)),
            dma((3,)),
            dma((2,)),
            dma((3,)),
            dma((ITERS, 2)),
            dma((ITERS, 3)),
            dma((4,)),
            dma((4,)),
            dma((GX,)),
            dma,
        ],
        compiler_params=pltpu.CompilerParams(collective_id=0, has_side_effects=True),
    )(offsets, masses, counts, source)
    return density, pressure, residual, peaks[0, :ITERS]


def solution(mesh):
    return jax.shard_map(
        shard,
        mesh=mesh,
        in_specs=(P(None, "gx", "gy", None), P("gx", "gy", None), P("gx", "gy"), P("gx", "gy", None)),
        out_specs=(P("gx", "gy", None), P("gx", "gy", None), P("gx", "gy", None), P()),
        check_vma=False,
    )
```

```python
import functools

import jax
import jax.numpy as jnp
from jax import lax
from jax.experimental import pallas as pl
from jax.experimental.pallas import tpu as pltpu
from jax.sharding import PartitionSpec as P

MESH = pl.DeviceIdType.MESH
F32 = jnp.float32

ITERS = 5
SLOT = 128
ROWS = 16
COLS = 256
GX = 8
XLEN = 4
ZLEN = 8
PLANE = GX * XLEN
BASE_STIFF = 0.5
FAR = 1000.0
SHIFTS = (0.8125, 0.0625, 0.8125, 0.125, 0.5)
PAIRS = [(i, j) for i in range(ITERS) for j in range(i, ITERS)] + [(i, ITERS) for i in range(ITERS)]
LOOP = 4


def snake(q):
    z, x = lax.div(q, XLEN), lax.rem(q, XLEN)
    return z * XLEN + x + lax.rem(z, 2) * (XLEN - 1 - 2 * x)


def mirrored(g, a):
    return a + lax.rem(g, 2) * (GX - 1 - 2 * a)


def two_sum(a, b):
    s = a + b
    t = s - a
    return s, (a - (s - t)) + (b - t)


def fast_two_sum(a, b):
    s = a + b
    return s, b - (s - a)


def split(a):
    c = 4097.0 * a
    high = c - (c - a)
    return high, a - high


def two_prod(a, b):
    p = a * b
    ah, al = split(a)
    bh, bl = split(b)
    return p, ((ah * bh - p) + ah * bl + al * bh) + al * bl


def pair_add(u, v):
    s, e = two_sum(u[0], v[0])
    return fast_two_sum(s, e + (u[1] + v[1]))


def pair_neg(u):
    return -u[0], -u[1]


def pair_mul(u, v):
    p, e = two_prod(u[0], v[0])
    return fast_two_sum(p, e + (u[0] * v[1] + u[1] * v[0]))


def pair_scale(u, c):
    p, e = two_prod(u[0], c)
    return fast_two_sum(p, e + u[1] * c)


def pair_div(u, v):
    q = u[0] / v[0]
    r = pair_add(u, pair_neg(pair_scale(v, q)))
    return fast_two_sum(q, r[0] / v[0])


def pair_tree(items):
    while len(items) > 1:
        items = [pair_add(*items[k : k + 2]) if k + 1 < len(items) else items[k] for k in range(0, len(items), 2)]
    return items[0]


def pair_dot(u, v):
    out = pair_mul(u, v)
    for shift in (4, 2, 1):
        out = pair_add(out, (pltpu.roll(out[0], shift, 0), pltpu.roll(out[1], shift, 0)))
    return out


def device_of(column):
    group, place = lax.div(column, GX), lax.rem(column, GX)
    return mirrored(group, place), snake(group)


def body(
    off_ref, mass_ref, cnt_ref, src_ref,
    ob, p2,
    sbuf, inb, xcol, ycol, rcol, wts, part, rb, vb, rows_s, ub, gb,
    g1s, g1, g2s, g2, p1s, p1, p2s, osb,
    in_send, in_recv, rho_send, rho_recv, halo_send, halo_recv,
    red_send, red_recv, out_send, out_recv,
):
    a, q = lax.axis_index("gx"), lax.axis_index("gy")
    z, x = lax.div(q, XLEN), lax.rem(q, XLEN)
    group = snake(q)
    place = mirrored(group, a)
    column = group * GX + place
    has_left, has_right = column > 0, column < COLS - 1
    left = device_of(jnp.maximum(column - 1, 0))
    right = device_of(jnp.minimum(column + 1, COLS - 1))
    plane_index = a * XLEN + x

    inb[...] = jnp.zeros_like(inb)
    rb[...] = jnp.zeros_like(rb)
    vb[...] = jnp.zeros_like(vb)
    osb[...] = jnp.zeros_like(osb)
    gb[...] = jnp.zeros_like(gb)
    part[0] = jnp.zeros((SLOT, SLOT), F32)

    barrier = pltpu.get_barrier_semaphore()

    def plane_mate(t):
        other = lax.rem(plane_index + t, PLANE)
        return lax.div(other, XLEN), z * XLEN + lax.rem(other, XLEN)

    def tower_mate(t):
        return a, lax.rem(z + t, ZLEN) * XLEN + x

    def greet(target):
        pl.semaphore_signal(barrier, inc=1, device_id=target, device_id_type=MESH)

    for t in range(1, PLANE):
        greet(plane_mate(t))
    for t in range(1, ZLEN):
        greet(tower_mate(t))
    low_edge = (lax.rem(column, PLANE) == 0) & has_left
    high_edge = (lax.rem(column, PLANE) == PLANE - 1) & has_right
    for edge, step in ((low_edge, -1), (high_edge, 1)):
        @pl.when(edge)
        def _(step=step):
            for k in range(GX):
                greet((k, group + step))

    lane = lax.broadcasted_iota(jnp.int32, (1, SLOT), 1)
    for r in range(2):
        for c in range(GX):
            occ = jnp.where(lane < cnt_ref[r, c], 1.0, 0.0).astype(F32)
            sbuf[c, r, 0:1, :] = off_ref[0, r, c : c + 1, :]
            sbuf[c, r, 1:2, :] = off_ref[1, r, c : c + 1, :]
            sbuf[c, r, 2:3, :] = mass_ref[r, c : c + 1, :] * occ
            sbuf[c, r, 3:4, :] = src_ref[r, c : c + 1, :] * occ

    low_block = (x == 0) & (q > 0)
    high_block = (x == XLEN - 1) & (q < COLS // GX - 1)
    awaited = PLANE - 1 + ZLEN - 1 + low_block.astype(jnp.int32) + high_block.astype(jnp.int32)
    pl.semaphore_wait(barrier, awaited)

    sends = []
    for c in range(GX):
        for d in (-1, 0, 1):
            target_column = q * GX + c + d
            wanted = jnp.logical_and(target_column >= 0, target_column < COLS)
            ta, tq = device_of(jnp.clip(target_column, 0, COLS - 1))
            wanted = jnp.logical_and(wanted, jnp.logical_or(ta != a, tq != q))
            copy = pltpu.make_async_remote_copy(
                src_ref=sbuf.at[c],
                dst_ref=inb.at[1 - d, pl.ds(1 + 2 * a, 2)],
                send_sem=in_send.at[len(sends)],
                recv_sem=in_recv.at[1 - d],
                device_id=(ta, tq),
                device_id_type=MESH,
            )
            pl.when(wanted)(copy.start)
            sends.append((wanted, copy))
    for d in (-1, 0, 1):
        own = column + d - q * GX
        inside = (own >= 0) & (own < GX)
        copy = pltpu.make_async_copy(
            sbuf.at[jnp.clip(own, 0, GX - 1)],
            inb.at[1 + d, pl.ds(1 + 2 * a, 2)],
            in_recv.at[1 + d],
        )
        pl.when(inside)(copy.start)

    def arrived(slot):
        view = inb.at[slot, pl.ds(1, ROWS)]
        pltpu.make_async_copy(view, view, in_recv.at[slot]).wait()

    def spread(row):
        return jnp.transpose(jnp.broadcast_to(row, (SLOT, SLOT)))

    def total_row(block):
        return jnp.sum(jnp.transpose(block), axis=0, keepdims=True)

    arrived(1)

    def columns(r, carry):
        xcol[r] = spread(inb[1, r + 1, 0:1, :])
        ycol[r] = spread(inb[1, r + 1, 1:2, :])
        rows_s[0, pl.ds(r, 1), :] = inb[1, r + 1, 2:3, :]
        rows_s[1, pl.ds(r, 1), :] = inb[1, r + 1, 3:4, :]
        return carry

    def columns(r):
        xcol[r] = spread(inb[1, r + 1, 0:1, :])
        ycol[r] = spread(inb[1, r + 1, 1:2, :])
        rows_s[0, pl.ds(r, 1), :] = inb[1, r + 1, 2:3, :]
        rows_s[1, pl.ds(r, 1), :] = inb[1, r + 1, 3:4, :]

    columns(0)
    pl.when(has_left)(lambda: arrived(0))
    pl.when(has_right)(lambda: arrived(2))

    near = [(dc, dr) for dc in (1, 0, 2) for dr in (0, 1, 2)]

    def density_row(r):
        rb[1, pl.ds(8 + r, 1), :] = 1.0 + total_row(part[r])

    def falloffs(r, carry):
        columns(jnp.minimum(r + 1, ROWS - 1))
        density_row(jnp.maximum(r - 1, 0))
        rows = []
        for dc, dr in near:
            cell = inb[dc, r + dr]
            mass = cell[2:3, :]
            px = (dr - 1.0) + jnp.where(mass > 0.0, cell[0:1, :], FAR)
            py = (dc - 1.0) + cell[1:2, :]
            rows.append((px, py, mass))
        for h in range(0, SLOT, 64):
            xi, yi = xcol[r, h : h + 64, :], ycol[r, h : h + 64, :]
            acc = jnp.zeros((64, SLOT), F32)
            for k, (px, py, mass) in enumerate(rows):
                ox, oy = px - xi, py - yi
                fall = jnp.maximum(1.0 - (ox * ox + oy * oy), 0.0)
                square = fall * fall
                wts[r, k, h : h + 64, :] = square
                acc = acc + square * fall * mass
            part[r, h : h + 64, :] = acc
        return carry

    lax.fori_loop(0, ROWS, falloffs, 0)
    density_row(ROWS - 1)

    def exchange(buf, send, recv):
        copies = []
        for k, (have, target, slot) in enumerate(((has_left, left, 2), (has_right, right, 0))):
            copy = pltpu.make_async_remote_copy(
                src_ref=buf.at[1, pl.ds(8, ROWS)],
                dst_ref=buf.at[slot, pl.ds(8, ROWS)],
                send_sem=send.at[k],
                recv_sem=recv.at[slot],
                device_id=target,
                device_id_type=MESH,
            )
            pl.when(have)(copy.start)
            copies.append((have, copy))

        def wait():
            for have, slot in ((has_left, 0), (has_right, 2)):
                view = buf.at[slot, pl.ds(8, ROWS)]
                pl.when(have)(pltpu.make_async_copy(view, view, recv.at[slot]).wait)

        return wait, copies

    wait_rho, rho_copies = exchange(rb, rho_send, rho_recv)
    sends += rho_copies

    def rho_columns(r, carry):
        rcol[r] = spread(10.0 * rb[1, pl.ds(8 + r, 1), :])
        return carry

    lax.fori_loop(0, ROWS, rho_columns, 0, unroll=ROWS)

    def diagonal_row(r):
        ub[pl.ds(r, 1), :] = BASE_STIFF + total_row(part[r])

    def weights(first, last):
        def run(r, carry):
            if first:
                diagonal_row(jnp.maximum(r - 1, 0))
            rows = [10.0 * rb[dc, pl.ds(7 + r + dr, 1), :] for dc, dr in near[first:last]]
            for h in range(0, SLOT, 64):
                ri = rcol[r, h : h + 64, :]
                acc = jnp.zeros((64, SLOT), F32) if first == 0 else part[r, h : h + 64, :]
                for k, row in enumerate(rows, first):
                    w = wts[r, k, h : h + 64, :] / (ri + row)
                    wts[r, k, h : h + 64, :] = w
                    acc = acc + w
                part[r, h : h + 64, :] = acc
            return carry

        lax.fori_loop(0, ROWS, run, 0)

    weights(0, 3)
    wait_rho()
    weights(3, 9)

    diagonal_row(ROWS - 1)
    occ = jnp.where(rows_s[0] > 0.0, 1.0, 0.0).astype(F32)
    diag = ub[...]
    dinv = occ / diag
    basis = [rows_s[1] * dinv]
    gram_rows = {}

    for k in range(ITERS):
        vb[k, 1, pl.ds(8, ROWS), :] = basis[k]
        wait_halo, halo_copies = exchange(vb.at[k], halo_send.at[k], halo_recv.at[k])
        sends += halo_copies

        def apply_own(r, carry):
            acc = wts[r, 0] * vb[k, 1, pl.ds(7 + r, 1), :]
            for m in (1, 2):
                acc = acc + wts[r, m] * vb[k, 1, pl.ds(7 + r + m, 1), :]
            part[r] = acc
            return carry

        lax.fori_loop(0, ROWS, apply_own, 0, unroll=2)
        scaled = basis[k] * diag
        for i in range(k + 1):
            gram_rows[i, k] = jnp.sum(basis[i] * scaled, axis=0, keepdims=True)
        wait_halo()

        def apply_rest(r, carry):
            acc = part[r]
            for m in range(3, 9):
                dc, dr = near[m]
                acc = acc + wts[r, m] * vb[k, dc, pl.ds(7 + r + dr, 1), :]
            ub[pl.ds(r, 1), :] = total_row(acc)
            return carry

        lax.fori_loop(0, ROWS, apply_rest, 0, unroll=ROWS)
        basis.append(2.0 * (ub[...] * dinv - SHIFTS[k] * basis[k]))

    scaled = basis[ITERS] * diag
    for i in range(ITERS):
        gram_rows[i, ITERS] = jnp.sum(basis[i] * scaled, axis=0, keepdims=True)

    sub8 = lax.broadcasted_iota(jnp.int32, (8, SLOT), 0)
    lane8 = lax.broadcasted_iota(jnp.int32, (8, SLOT), 1)

    for i, j in PAIRS:
        gb[8 * j + i : 8 * j + i + 1, :] = gram_rows[i, j]
        if i != j:
            gb[8 * i + j : 8 * i + j + 1, :] = gram_rows[i, j]
    turned = jnp.transpose(gb[...])
    gram_sum = two_sum(turned[:64], turned[64:])
    for size in (32, 16, 8, 4, 2, 1):
        gram_sum = pair_add((gram_sum[0][:size], gram_sum[1][:size]), (gram_sum[0][size:], gram_sum[1][size:]))

    def gather(rows, own, all_refs, mates, index, count, send_sem, recv_sem):
        for k, row in enumerate(rows):
            own[0, k : k + 1, :] = row
        for t in range(1, count):
            copy = pltpu.make_async_remote_copy(
                src_ref=own.at[0],
                dst_ref=all_refs.at[index],
                send_sem=send_sem,
                recv_sem=recv_sem,
                device_id=mates(t),
                device_id_type=MESH,
            )
            copy.start()
        for k, row in enumerate(rows):
            all_refs[index, k : k + 1, :] = row

        def wait():
            view = all_refs.at[pl.ds(0, count - 1)]
            pltpu.make_async_copy(view, view, recv_sem).wait()

        def wait_sent():
            view = all_refs.at[pl.ds(0, count - 1)]
            pltpu.make_async_copy(view, view, send_sem).wait()

        return wait, wait_sent

    def pairs_of(refs, count):
        return pair_tree([(refs[k, 0:1, :], refs[k, 1:2, :]) for k in range(count)])

    wait_plane, sent_plane = gather(gram_sum, g1s, g1, plane_mate, plane_index, PLANE, red_send.at[0], red_recv.at[0])
    wait_plane()
    plane_sum = pairs_of(g1, PLANE)
    wait_tower, sent_tower = gather(plane_sum, g2s, g2, tower_mate, z, ZLEN, red_send.at[1], red_recv.at[1])
    wait_tower()
    total = pairs_of(g2, ZLEN)
    high, low = spread(total[0]), spread(total[1])
    gram = [(high[8 * j : 8 * j + 8], low[8 * j : 8 * j + 8]) for j in range(ITERS + 1)]

    zero = jnp.zeros((8, SLOT), F32)
    first = jnp.where(sub8 == 0, 1.0, 0.0).astype(F32)
    keep = zero
    for k, shift in enumerate(SHIFTS):
        keep = jnp.where(sub8 == k, 1.0 - shift, keep)

    def part_of(u, k):
        return tuple(jnp.broadcast_to(w[k : k + 1], (8, SLOT)) for w in u)

    solution_at, residual_at, direction = (zero, zero), (first, zero), (first, zero)
    residual_image = gram[0]
    residuals = []
    rz = part_of(gram[0], 0)
    for k in range(ITERS):
        moved = tuple(-0.5 * pltpu.roll(w, 1, 0) for w in direction)
        image = pair_add(pair_scale(direction, keep), moved)
        gram_image = pair_tree([pair_mul(gram[j], part_of(image, j)) for j in range(k + 2)])
        step = pair_div(rz, pair_dot(direction, gram_image))
        solution_at = pair_add(solution_at, pair_mul(step, direction))
        residual_at = pair_add(residual_at, pair_neg(pair_mul(step, image)))
        residuals.append(residual_at[0])
        if k + 1 < ITERS:
            residual_image = pair_add(residual_image, pair_neg(pair_mul(step, gram_image)))
            new = pair_dot(residual_at, residual_image)
            direction = pair_add(residual_at, pair_mul(pair_div(new, rz), direction))
            rz = new

    def combine(factors, count):
        out = None
        for j in range(count):
            term = factors[j : j + 1] * basis[j]
            out = term if out is None else out + term
        return out

    pressure = combine(solution_at[0], ITERS)
    gb[0:8, :] = jnp.zeros((8, SLOT), F32)
    for k in range(ITERS):
        field = combine(residuals[k], k + 2) * diag
        gb[k : k + 1, :] = jnp.max(jnp.abs(field), axis=0, keepdims=True)
    peak = jnp.max(gb[0:8, :], axis=1, keepdims=True)
    peak_row = jnp.sum(jnp.where(sub8 == lane8, peak, 0.0), axis=0, keepdims=True)
    wait_peaks, sent_peaks = gather([peak_row], p1s, p1, plane_mate, plane_index, PLANE, red_send.at[2], red_recv.at[2])

    density = rb[1, pl.ds(8, ROWS), :]
    for r in range(ROWS):
        osb[r, 0:1, :] = density[r : r + 1, :]
        osb[r, 1:2, :] = pressure[r : r + 1, :]
        osb[r, 2:3, :] = field[r : r + 1, :]
    for k in range(GX):
        wanted = jnp.logical_or(a != k, group != q)
        copy = pltpu.make_async_remote_copy(
            src_ref=osb.at[pl.ds(2 * k, 2)],
            dst_ref=ob.at[place],
            send_sem=out_send.at[k],
            recv_sem=out_recv,
            device_id=(k, group),
            device_id_type=MESH,
        )
        pl.when(wanted)(copy.start)
        sends.append((wanted, copy))
    local = pltpu.make_async_copy(osb.at[pl.ds(2 * a, 2)], ob.at[place], out_recv)
    pl.when(group == q)(local.start)

    wait_peaks()
    wait_top, sent_top = gather([jnp.max(p1[...], axis=0)], p2s, p2, tower_mate, z, ZLEN, red_send.at[3], red_recv.at[3])
    pltpu.make_async_copy(ob, ob, out_recv).wait()
    wait_top()

    for wanted, copy in sends:
        pl.when(wanted)(copy.wait_send)
    for wait in (sent_plane, sent_tower, sent_peaks, sent_top):
        wait()


def finish(ob, p2, dens_ref, pres_ref, resid_ref, peaks_ref):
    for r in range(2):
        for c in range(GX):
            dens_ref[r, c : c + 1, :] = ob[c, r, 0:1, :]
            pres_ref[r, c : c + 1, :] = ob[c, r, 1:2, :]
            resid_ref[r, c : c + 1, :] = ob[c, r, 2:3, :]
    peaks_ref[...] = jnp.max(p2[...], axis=0)[0, :ITERS]


def shard(offsets, masses, counts, source):
    block = jax.ShapeDtypeStruct((2, GX, SLOT), F32)
    vmem = pl.BlockSpec(memory_space=pltpu.VMEM)
    dma = pltpu.SemaphoreType.DMA
    cells = (ROWS, SLOT, SLOT)
    gathered, peaks = pl.pallas_call(
        body,
        out_shape=(
            jax.ShapeDtypeStruct((GX, 2, 4, SLOT), F32),
            jax.ShapeDtypeStruct((ZLEN, 1, SLOT), F32),
        ),
        in_specs=[vmem, vmem, pl.BlockSpec(memory_space=pltpu.SMEM), vmem],
        out_specs=(vmem, vmem),
        scratch_shapes=[
            pltpu.VMEM((GX, 2, 4, SLOT), F32),
            pltpu.VMEM((3, ROWS + 2, 4, SLOT), F32),
            pltpu.VMEM(cells, F32),
            pltpu.VMEM(cells, F32),
            pltpu.VMEM(cells, F32),
            pltpu.VMEM((ROWS, 9, SLOT, SLOT), F32),
            pltpu.VMEM(cells, F32),
            pltpu.VMEM((3, 32, SLOT), F32),
            pltpu.VMEM((ITERS, 3, 32, SLOT), F32),
            pltpu.VMEM((2, ROWS, SLOT), F32),
            pltpu.VMEM((ROWS, SLOT), F32),
            pltpu.VMEM((SLOT, SLOT), F32),
            pltpu.VMEM((1, 2, SLOT), F32),
            pltpu.VMEM((PLANE, 2, SLOT), F32),
            pltpu.VMEM((1, 2, SLOT), F32),
            pltpu.VMEM((ZLEN, 2, SLOT), F32),
            pltpu.VMEM((1, 1, SLOT), F32),
            pltpu.VMEM((PLANE, 1, SLOT), F32),
            pltpu.VMEM((1, 1, SLOT), F32),
            pltpu.VMEM((ROWS, 4, SLOT), F32),
            dma((24,)),
            dma((3,)),
            dma((2,)),
            dma((3,)),
            dma((ITERS, 2)),
            dma((ITERS, 3)),
            dma((4,)),
            dma((4,)),
            dma((GX,)),
            dma,
        ],
        compiler_params=pltpu.CompilerParams(collective_id=0, has_side_effects=True),
    )(offsets, masses, counts, source)
    return pl.pallas_call(
        finish,
        out_shape=(block, block, block, jax.ShapeDtypeStruct((ITERS,), F32)),
        in_specs=[vmem, vmem],
        out_specs=(vmem, vmem, vmem, vmem),
    )(gathered, peaks)


def solution(mesh):
    return jax.shard_map(
        shard,
        mesh=mesh,
        in_specs=(P(None, "gx", "gy", None), P("gx", "gy", None), P("gx", "gy"), P("gx", "gy", None)),
        out_specs=(P("gx", "gy", None), P("gx", "gy", None), P("gx", "gy", None), P()),
        check_vma=False,
    )
```

```python
import functools

import jax
import jax.numpy as jnp
from jax import lax
from jax.experimental import pallas as pl
from jax.experimental.pallas import tpu as pltpu
from jax.sharding import PartitionSpec as P

MESH = pl.DeviceIdType.MESH
F32 = jnp.float32

ITERS = 5
SLOT = 128
ROWS = 16
COLS = 256
GX = 8
XLEN = 4
ZLEN = 8
PLANE = GX * XLEN
BASE_STIFF = 0.5
FAR = 1000.0
SHIFTS = (0.8125, 0.0625, 0.8125, 0.125, 0.5)
PAIRS = [(i, j) for i in range(ITERS) for j in range(i, ITERS)] + [(i, ITERS) for i in range(ITERS)]


def hops(step, length):
    return min(step, length - step)


PLANE_STEPS = sorted(
    ((dy, dx, dc) for dy in range(GX // 2) for dx in range(XLEN) for dc in range(2) if (dy, dx, dc) != (0, 0, 0)),
    key=lambda s: -(hops(s[0], GX // 2) + hops(s[1], XLEN) + 0.5 * s[2]),
)
TOWER_STEPS = sorted(range(1, ZLEN), key=lambda s: -hops(s, ZLEN))


def snake(q):
    z, x = lax.div(q, XLEN), lax.rem(q, XLEN)
    return z * XLEN + x + lax.rem(z, 2) * (XLEN - 1 - 2 * x)


def mirrored(g, a):
    return a + lax.rem(g, 2) * (GX - 1 - 2 * a)


def two_sum(a, b):
    s = a + b
    t = s - a
    return s, (a - (s - t)) + (b - t)


def fast_two_sum(a, b):
    s = a + b
    return s, b - (s - a)


def split(a):
    c = 4097.0 * a
    high = c - (c - a)
    return high, a - high


def two_prod(a, b):
    p = a * b
    ah, al = split(a)
    bh, bl = split(b)
    return p, ((ah * bh - p) + ah * bl + al * bh) + al * bl


def pair_add(u, v):
    s, e = two_sum(u[0], v[0])
    return fast_two_sum(s, e + (u[1] + v[1]))


def pair_neg(u):
    return -u[0], -u[1]


def pair_mul(u, v):
    p, e = two_prod(u[0], v[0])
    return fast_two_sum(p, e + (u[0] * v[1] + u[1] * v[0]))


def pair_scale(u, c):
    p, e = two_prod(u[0], c)
    return fast_two_sum(p, e + u[1] * c)


def pair_div(u, v):
    q = u[0] / v[0]
    r = pair_add(u, pair_neg(pair_scale(v, q)))
    return fast_two_sum(q, r[0] / v[0])


def pair_tree(items):
    while len(items) > 1:
        items = [pair_add(*items[k : k + 2]) if k + 1 < len(items) else items[k] for k in range(0, len(items), 2)]
    return items[0]


def pair_dot(u, v):
    out = pair_mul(u, v)
    for shift in (4, 2, 1):
        out = pair_add(out, (pltpu.roll(out[0], shift, 0), pltpu.roll(out[1], shift, 0)))
    return out


def device_of(column):
    group, place = lax.div(column, GX), lax.rem(column, GX)
    return mirrored(group, place), snake(group)


def body(
    off_hbm, mass_hbm, cnt_hbm, src_hbm,
    ob, p2,
    off_ref, mass_ref, cnt_ref, src_ref,
    sbuf, inb, xcol, ycol, rcol, wts, part, rb, vb, rows_s, ub, gb,
    g1s, g1, g2s, g2, p1s, p1, p2s, osb,
    load_sem, in_send, in_recv, rho_send, rho_recv, halo_send, halo_recv,
    red_send, red_recv, out_send, out_recv,
):
    a, q = lax.axis_index("gx"), lax.axis_index("gy")
    z, x = lax.div(q, XLEN), lax.rem(q, XLEN)
    group = snake(q)
    place = mirrored(group, a)
    column = group * GX + place
    has_left, has_right = column > 0, column < COLS - 1
    left = device_of(jnp.maximum(column - 1, 0))
    right = device_of(jnp.minimum(column + 1, COLS - 1))
    plane_index = a * XLEN + x
    near_slot, far_slot = 2 - 2 * lax.rem(column, 2), 2 * lax.rem(column, 2)
    has_far = (column + lax.rem(column, 2) > 0) & (column + lax.rem(column, 2) < COLS)

    loads = [
        pltpu.make_async_copy(src, dst, load_sem.at[k])
        for k, (src, dst) in enumerate(
            ((off_hbm, off_ref), (mass_hbm, mass_ref), (src_hbm, src_ref), (cnt_hbm, cnt_ref))
        )
    ]
    for load in loads:
        load.start()

    rim = jnp.zeros((4, SLOT), F32)
    for slot in range(3):
        inb[slot, 0] = rim
        inb[slot, ROWS + 1] = rim
    wide = jnp.zeros((8, SLOT), F32)
    for slot in range(3):
        for end in (0, 24):
            rb[slot, end : end + 8, :] = wide
            for k in range(ITERS):
                vb[k, slot, end : end + 8, :] = wide
    for have, slot in ((has_left, 0), (has_right, 2)):
        @pl.when(jnp.logical_not(have))
        def _(slot=slot):
            inb[slot] = jnp.zeros((ROWS + 2, 4, SLOT), F32)
            rb[slot] = jnp.zeros((32, SLOT), F32)
            for k in range(ITERS):
                vb[k, slot] = jnp.zeros((32, SLOT), F32)

    barrier = pltpu.get_barrier_semaphore()

    y, core = lax.div(a, 2), lax.rem(a, 2)

    def plane_mate(step):
        dy, dx, dc = step
        return lax.rem(y + dy, GX // 2) * 2 + lax.rem(core + dc, 2), z * XLEN + lax.rem(x + dx, XLEN)

    def tower_mate(step):
        return a, lax.rem(z + step, ZLEN) * XLEN + x

    def greet(target):
        pl.semaphore_signal(barrier, inc=1, device_id=target, device_id_type=MESH)

    for step in TOWER_STEPS:
        greet(tower_mate(step))
    for step in PLANE_STEPS:
        greet(plane_mate(step))
    low_edge = (lax.rem(column, PLANE) == 0) & has_left
    high_edge = (lax.rem(column, PLANE) == PLANE - 1) & has_right
    for edge, step in ((low_edge, -1), (high_edge, 1)):
        @pl.when(edge)
        def _(step=step):
            for k in range(GX):
                greet((k, group + step))

    osb[...] = jnp.zeros_like(osb)
    gb[...] = jnp.zeros_like(gb)
    part[0] = jnp.zeros((SLOT, SLOT), F32)
    for load in loads:
        load.wait()

    lane = lax.broadcasted_iota(jnp.int32, (1, SLOT), 1)
    for r in range(2):
        for c in range(GX):
            occ = jnp.where(lane < cnt_ref[r, c], 1.0, 0.0).astype(F32)
            sbuf[c, r, 0:1, :] = off_ref[0, r, c : c + 1, :]
            sbuf[c, r, 1:2, :] = off_ref[1, r, c : c + 1, :]
            sbuf[c, r, 2:3, :] = mass_ref[r, c : c + 1, :] * occ
            sbuf[c, r, 3:4, :] = src_ref[r, c : c + 1, :] * occ

    low_block = (x == 0) & (q > 0)
    high_block = (x == XLEN - 1) & (q < COLS // GX - 1)
    awaited = PLANE - 1 + ZLEN - 1 + low_block.astype(jnp.int32) + high_block.astype(jnp.int32)
    pl.semaphore_wait(barrier, awaited)

    sends = []
    for t in (4, 3, 5, 2, 6, 1, 7, 0):
        c = lax.rem(a + t, GX)
        for d in (0, -1, 1):
            target_column = q * GX + c + d
            wanted = jnp.logical_and(target_column >= 0, target_column < COLS)
            ta, tq = device_of(jnp.clip(target_column, 0, COLS - 1))
            wanted = jnp.logical_and(wanted, jnp.logical_or(ta != a, tq != q))
            copy = pltpu.make_async_remote_copy(
                src_ref=sbuf.at[c],
                dst_ref=inb.at[1 - d, pl.ds(1 + 2 * a, 2)],
                send_sem=in_send.at[len(sends)],
                recv_sem=in_recv.at[1 - d],
                device_id=(ta, tq),
                device_id_type=MESH,
            )
            pl.when(wanted)(copy.start)
            sends.append((wanted, copy))
    for d in (-1, 0, 1):
        own = column + d - q * GX
        inside = (own >= 0) & (own < GX)
        copy = pltpu.make_async_copy(
            sbuf.at[jnp.clip(own, 0, GX - 1)],
            inb.at[1 + d, pl.ds(1 + 2 * a, 2)],
            in_recv.at[1 + d],
        )
        pl.when(inside)(copy.start)

    def arrived(slot):
        view = inb.at[slot, pl.ds(1, ROWS)]
        pltpu.make_async_copy(view, view, in_recv.at[slot]).wait()

    def spread(row):
        return jnp.transpose(jnp.broadcast_to(row, (SLOT, SLOT)))

    def total_row(block):
        return jnp.sum(jnp.transpose(block), axis=0, keepdims=True)

    arrived(1)

    def columns(r, carry):
        xcol[r] = spread(inb[1, r + 1, 0:1, :])
        ycol[r] = spread(inb[1, r + 1, 1:2, :])
        rows_s[0, pl.ds(r, 1), :] = inb[1, r + 1, 2:3, :]
        rows_s[1, pl.ds(r, 1), :] = inb[1, r + 1, 3:4, :]
        return carry

    def columns(r):
        cell = inb[1, r + 1]
        fields = spread(cell[0:1]), spread(cell[1:2]), cell

        def store():
            xcol[r], ycol[r] = fields[0], fields[1]
            rows_s[0, pl.ds(r, 1), :] = cell[2:3]
            rows_s[1, pl.ds(r, 1), :] = cell[3:4]

        return store

    columns(0)()
    pl.when(has_left)(lambda: arrived(0))
    pl.when(has_right)(lambda: arrived(2))

    blocks = [(slot, dr) for slot in (1, near_slot, far_slot) for dr in (0, 1, 2)]
    side = [0.0] * 3 + [(near_slot - 1).astype(F32)] * 3 + [(far_slot - 1).astype(F32)] * 3

    def density_row(r):
        row = 1.0 + total_row(part[r])

        def store():
            rb[1, pl.ds(8 + r, 1), :] = row

        return store

    def falloffs(r, carry):
        store_columns = columns(jnp.minimum(r + 1, ROWS - 1))
        store_row = density_row(jnp.maximum(r - 1, 0))
        rows = []
        for (slot, dr), step_y in zip(blocks, side):
            cell = inb[slot, r + dr]
            mass = cell[2:3, :]
            px = (dr - 1.0) + jnp.where(mass > 0.0, cell[0:1, :], FAR)
            py = step_y + cell[1:2, :]
            rows.append((px, py, mass))
        for h in range(0, SLOT, 64):
            xi, yi = xcol[r, h : h + 64, :], ycol[r, h : h + 64, :]
            acc = jnp.zeros((64, SLOT), F32)
            for k, (px, py, mass) in enumerate(rows):
                ox, oy = px - xi, py - yi
                fall = jnp.maximum(1.0 - (ox * ox + oy * oy), 0.0)
                square = fall * fall
                wts[r, k, h : h + 64, :] = square
                acc = acc + square * fall * mass
            part[r, h : h + 64, :] = acc
        store_columns()
        store_row()
        return carry

    lax.fori_loop(0, ROWS, falloffs, 0)
    density_row(ROWS - 1)()

    def exchange(buf, send, recv):
        copies = []
        for k, (have, target, slot) in enumerate(((has_left, left, 2), (has_right, right, 0))):
            copy = pltpu.make_async_remote_copy(
                src_ref=buf.at[1, pl.ds(8, ROWS)],
                dst_ref=buf.at[slot, pl.ds(8, ROWS)],
                send_sem=send.at[k],
                recv_sem=recv.at[slot],
                device_id=target,
                device_id_type=MESH,
            )
            pl.when(have)(copy.start)
            copies.append((have, copy))

        def wait(slot):
            view = buf.at[slot, pl.ds(8, ROWS)]
            pltpu.make_async_copy(view, view, recv.at[slot]).wait()

        def wait_near():
            wait(near_slot)

        def wait_far():
            pl.when(has_far)(lambda: wait(far_slot))

        return wait_near, wait_far, copies

    wait_rho_near, wait_rho_far, rho_copies = exchange(rb, rho_send, rho_recv)
    sends += rho_copies

    def rho_columns(r, carry):
        rcol[r] = spread(10.0 * rb[1, pl.ds(8 + r, 1), :])
        return carry

    lax.fori_loop(0, ROWS, rho_columns, 0, unroll=ROWS)

    def weights(first, last):
        def run(r, carry):
            rows = [10.0 * rb[slot, pl.ds(7 + r + dr, 1), :] for slot, dr in blocks[first:last]]
            for h in range(0, SLOT, 64):
                ri = rcol[r, h : h + 64, :]
                acc = jnp.zeros((64, SLOT), F32) if first == 0 else part[r, h : h + 64, :]
                for k, row in enumerate(rows, first):
                    w = wts[r, k, h : h + 64, :] / (ri + row)
                    wts[r, k, h : h + 64, :] = w
                    acc = acc + w
                part[r, h : h + 64, :] = acc
            return carry

        lax.fori_loop(0, ROWS, run, 0)

    weights(0, 3)
    wait_rho_near()
    weights(3, 6)
    wait_rho_far()
    weights(6, 9)

    def diagonal_rows(r, carry):
        ub[pl.ds(r, 1), :] = BASE_STIFF + total_row(part[r])
        return carry

    lax.fori_loop(0, ROWS, diagonal_rows, 0, unroll=ROWS)

    occ = jnp.where(rows_s[0] > 0.0, 1.0, 0.0).astype(F32)
    diag = ub[...]
    dinv = occ / diag
    basis = [rows_s[1] * dinv]
    gram_rows = {}

    for k in range(ITERS):
        vb[k, 1, pl.ds(8, ROWS), :] = basis[k]
        wait_near, wait_far, halo_copies = exchange(vb.at[k], halo_send.at[k], halo_recv.at[k])
        sends += halo_copies

        def apply_own(r, carry):
            acc = wts[r, 0] * vb[k, 1, pl.ds(7 + r, 1), :]
            for m in (1, 2):
                acc = acc + wts[r, m] * vb[k, 1, pl.ds(7 + r + m, 1), :]
            part[r] = acc
            return carry

        lax.fori_loop(0, ROWS, apply_own, 0, unroll=2)
        scaled = basis[k] * diag
        for i in range(k + 1):
            gram_rows[i, k] = jnp.sum(basis[i] * scaled, axis=0, keepdims=True)
        wait_near()

        def apply_near(r, carry):
            acc = part[r]
            for m in range(3, 6):
                slot, dr = blocks[m]
                acc = acc + wts[r, m] * vb[k, slot, pl.ds(7 + r + dr, 1), :]
            part[r] = acc
            return carry

        lax.fori_loop(0, ROWS, apply_near, 0, unroll=2)
        wait_far()

        def apply_far(r, carry):
            acc = part[r]
            for m in range(6, 9):
                slot, dr = blocks[m]
                acc = acc + wts[r, m] * vb[k, slot, pl.ds(7 + r + dr, 1), :]
            ub[pl.ds(r, 1), :] = total_row(acc)
            return carry

        lax.fori_loop(0, ROWS, apply_far, 0, unroll=ROWS)
        basis.append(2.0 * (ub[...] * dinv - SHIFTS[k] * basis[k]))

    scaled = basis[ITERS] * diag
    for i in range(ITERS):
        gram_rows[i, ITERS] = jnp.sum(basis[i] * scaled, axis=0, keepdims=True)

    sub8 = lax.broadcasted_iota(jnp.int32, (8, SLOT), 0)
    lane8 = lax.broadcasted_iota(jnp.int32, (8, SLOT), 1)

    for i, j in PAIRS:
        gb[8 * j + i : 8 * j + i + 1, :] = gram_rows[i, j]
        if i != j:
            gb[8 * i + j : 8 * i + j + 1, :] = gram_rows[i, j]
    turned = jnp.transpose(gb[...])
    gram_sum = two_sum(turned[:64], turned[64:])
    for size in (32, 16, 8, 4, 2, 1):
        gram_sum = pair_add((gram_sum[0][:size], gram_sum[1][:size]), (gram_sum[0][size:], gram_sum[1][size:]))

    def gather(rows, own, all_refs, mate, steps, index, send_sem, recv_sem, by_copy=False):
        count = len(steps) + 1

        for k, row in enumerate(rows):
            own[0, k : k + 1, :] = row
        for step in steps:
            copy = pltpu.make_async_remote_copy(
                src_ref=own.at[0],
                dst_ref=all_refs.at[index],
                send_sem=send_sem,
                recv_sem=recv_sem,
                device_id=mate(step),
                device_id_type=MESH,
            )
            copy.start()
        if by_copy:
            pltpu.make_async_copy(own.at[0], all_refs.at[index], recv_sem).start()
        else:
            for k, row in enumerate(rows):
                all_refs[index, k : k + 1, :] = row

        def wait():
            view = all_refs.at[pl.ds(0, count if by_copy else count - 1)]
            pltpu.make_async_copy(view, view, recv_sem).wait()

        def wait_sent():
            view = all_refs.at[pl.ds(0, count - 1)]
            pltpu.make_async_copy(view, view, send_sem).wait()

        return wait, wait_sent

    def pairs_of(refs, count):
        return pair_tree([(refs[k, 0:1, :], refs[k, 1:2, :]) for k in range(count)])

    wait_plane, sent_plane = gather(gram_sum, g1s, g1, plane_mate, PLANE_STEPS, plane_index, red_send.at[0], red_recv.at[0])
    wait_plane()
    plane_sum = pairs_of(g1, PLANE)
    wait_tower, sent_tower = gather(plane_sum, g2s, g2, tower_mate, TOWER_STEPS, z, red_send.at[1], red_recv.at[1])
    wait_tower()
    total = pairs_of(g2, ZLEN)
    high, low = spread(total[0]), spread(total[1])
    gram = [(high[8 * j : 8 * j + 8], low[8 * j : 8 * j + 8]) for j in range(ITERS + 1)]

    zero = jnp.zeros((8, SLOT), F32)
    first = jnp.where(sub8 == 0, 1.0, 0.0).astype(F32)
    keep = zero
    for k, shift in enumerate(SHIFTS):
        keep = jnp.where(sub8 == k, 1.0 - shift, keep)

    def part_of(u, k):
        return tuple(jnp.broadcast_to(w[k : k + 1], (8, SLOT)) for w in u)

    solution_at, residual_at, direction = (zero, zero), (first, zero), (first, zero)
    residual_image = gram[0]
    residuals = []
    rz = part_of(gram[0], 0)
    for k in range(ITERS):
        moved = tuple(-0.5 * pltpu.roll(w, 1, 0) for w in direction)
        image = pair_add(pair_scale(direction, keep), moved)
        gram_image = pair_tree([pair_mul(gram[j], part_of(image, j)) for j in range(k + 2)])
        step = pair_div(rz, pair_dot(direction, gram_image))
        solution_at = pair_add(solution_at, pair_mul(step, direction))
        residual_at = pair_add(residual_at, pair_neg(pair_mul(step, image)))
        residuals.append(residual_at[0])
        if k + 1 < ITERS:
            residual_image = pair_add(residual_image, pair_neg(pair_mul(step, gram_image)))
            new = pair_dot(residual_at, residual_image)
            direction = pair_add(residual_at, pair_mul(pair_div(new, rz), direction))
            rz = new

    def combine(factors, count):
        out = None
        for j in range(count):
            term = factors[j : j + 1] * basis[j]
            out = term if out is None else out + term
        return out

    pressure = combine(solution_at[0], ITERS)
    gb[0:8, :] = jnp.zeros((8, SLOT), F32)
    for k in range(ITERS):
        field = combine(residuals[k], k + 2) * diag
        gb[k : k + 1, :] = jnp.max(jnp.abs(field), axis=0, keepdims=True)
    peak = jnp.max(gb[0:8, :], axis=1, keepdims=True)
    peak_row = jnp.sum(jnp.where(sub8 == lane8, peak, 0.0), axis=0, keepdims=True)
    wait_peaks, sent_peaks = gather([peak_row], p1s, p1, plane_mate, PLANE_STEPS, plane_index, red_send.at[2], red_recv.at[2])

    density = rb[1, pl.ds(8, ROWS), :]
    for r in range(ROWS):
        osb[r, 0:1, :] = density[r : r + 1, :]
        osb[r, 1:2, :] = pressure[r : r + 1, :]
        osb[r, 2:3, :] = field[r : r + 1, :]
    for k in range(GX):
        wanted = jnp.logical_or(a != k, group != q)
        copy = pltpu.make_async_remote_copy(
            src_ref=osb.at[pl.ds(2 * k, 2)],
            dst_ref=ob.at[place],
            send_sem=out_send.at[k],
            recv_sem=out_recv,
            device_id=(k, group),
            device_id_type=MESH,
        )
        pl.when(wanted)(copy.start)
        sends.append((wanted, copy))
    local = pltpu.make_async_copy(osb.at[pl.ds(2 * a, 2)], ob.at[place], out_recv)
    pl.when(group == q)(local.start)

    wait_peaks()
    wait_top, sent_top = gather([jnp.max(p1[...], axis=0)], p2s, p2, tower_mate, TOWER_STEPS, z, red_send.at[3], red_recv.at[3], by_copy=True)
    pltpu.make_async_copy(ob, ob, out_recv).wait()
    wait_top()

    for wanted, copy in sends:
        pl.when(wanted)(copy.wait_send)
    for wait in (sent_plane, sent_tower, sent_peaks, sent_top):
        wait()


def finish(ob, p2, dens_ref, pres_ref, resid_ref, peaks_ref):
    for r in range(2):
        for c in range(GX):
            dens_ref[r, c : c + 1, :] = ob[c, r, 0:1, :]
            pres_ref[r, c : c + 1, :] = ob[c, r, 1:2, :]
            resid_ref[r, c : c + 1, :] = ob[c, r, 2:3, :]
    peaks_ref[...] = jnp.max(p2[...], axis=0)[0, :ITERS]


def shard(offsets, masses, counts, source):
    block = jax.ShapeDtypeStruct((2, GX, SLOT), F32)
    vmem = pl.BlockSpec(memory_space=pltpu.VMEM)
    dma = pltpu.SemaphoreType.DMA
    cells = (ROWS, SLOT, SLOT)
    gathered, peaks = pl.pallas_call(
        body,
        out_shape=(
            pltpu.VMEM((GX, 2, 4, SLOT), F32),
            pltpu.VMEM((ZLEN, 1, SLOT), F32),
        ),
        in_specs=[pl.BlockSpec(memory_space=pl.ANY)] * 4,
        out_specs=(pl.BlockSpec(memory_space=pl.ANY),) * 2,
        scratch_shapes=[
            pltpu.VMEM((2, 2, GX, SLOT), F32),
            pltpu.VMEM((2, GX, SLOT), F32),
            pltpu.SMEM((2, GX), jnp.int32),
            pltpu.VMEM((2, GX, SLOT), F32),
            pltpu.VMEM((GX, 2, 4, SLOT), F32),
            pltpu.VMEM((3, ROWS + 2, 4, SLOT), F32),
            pltpu.VMEM(cells, F32),
            pltpu.VMEM(cells, F32),
            pltpu.VMEM(cells, F32),
            pltpu.VMEM((ROWS, 9, SLOT, SLOT), F32),
            pltpu.VMEM(cells, F32),
            pltpu.VMEM((3, 32, SLOT), F32),
            pltpu.VMEM((ITERS, 3, 32, SLOT), F32),
            pltpu.VMEM((2, ROWS, SLOT), F32),
            pltpu.VMEM((ROWS, SLOT), F32),
            pltpu.VMEM((SLOT, SLOT), F32),
            pltpu.VMEM((1, 2, SLOT), F32),
            pltpu.VMEM((PLANE, 2, SLOT), F32),
            pltpu.VMEM((1, 2, SLOT), F32),
            pltpu.VMEM((ZLEN, 2, SLOT), F32),
            pltpu.VMEM((1, 1, SLOT), F32),
            pltpu.VMEM((PLANE, 1, SLOT), F32),
            pltpu.VMEM((1, 1, SLOT), F32),
            pltpu.VMEM((ROWS, 4, SLOT), F32),
            dma((4,)),
            dma((24,)),
            dma((3,)),
            dma((2,)),
            dma((3,)),
            dma((ITERS, 2)),
            dma((ITERS, 3)),
            dma((4,)),
            dma((4,)),
            dma((GX,)),
            dma,
        ],
        compiler_params=pltpu.CompilerParams(collective_id=0, has_side_effects=True),
    )(offsets, masses, counts, source)
    return pl.pallas_call(
        finish,
        out_shape=(block, block, block, jax.ShapeDtypeStruct((ITERS,), F32)),
        in_specs=[vmem, vmem],
        out_specs=(vmem, vmem, vmem, vmem),
    )(*(pltpu.with_memory_space_constraint(u, pltpu.VMEM) for u in (gathered, peaks)))


def solution(mesh):
    return jax.shard_map(
        shard,
        mesh=mesh,
        in_specs=(P(None, "gx", "gy", None), P("gx", "gy", None), P("gx", "gy"), P("gx", "gy", None)),
        out_specs=(P("gx", "gy", None), P("gx", "gy", None), P("gx", "gy", None), P()),
        check_vma=False,
    )
```

```python
import functools

import jax
import jax.numpy as jnp
from jax import lax
from jax.experimental import pallas as pl
from jax.experimental.pallas import tpu as pltpu
from jax.sharding import PartitionSpec as P

MESH = pl.DeviceIdType.MESH
F32 = jnp.float32

ITERS = 5
SLOT = 128
ROWS = 16
COLS = 256
GX = 8
XLEN = 4
ZLEN = 8
PLANE = GX * XLEN
BASE_STIFF = 0.5
FAR = 1000.0
SHIFTS = (0.8125, 0.0625, 0.8125, 0.125, 0.5)
PAIRS = [(i, j) for i in range(ITERS) for j in range(i, ITERS)] + [(i, ITERS) for i in range(ITERS)]


def hops(step, length):
    return min(step, length - step)


PLANE_STEPS = sorted(
    ((dy, dx, dc) for dy in range(GX // 2) for dx in range(XLEN) for dc in range(2) if (dy, dx, dc) != (0, 0, 0)),
    key=lambda s: -(hops(s[0], GX // 2) + hops(s[1], XLEN) + 0.5 * s[2]),
)
TOWER_STEPS = sorted(range(1, ZLEN), key=lambda s: -hops(s, ZLEN))


def snake(q):
    z, x = lax.div(q, XLEN), lax.rem(q, XLEN)
    return z * XLEN + x + lax.rem(z, 2) * (XLEN - 1 - 2 * x)


def mirrored(g, a):
    y, core = lax.div(a, 2), lax.rem(a, 2)
    second = lax.div(g, COLS // GX // 2)
    return 2 * (y + lax.rem(g, 2) * (GX // 2 - 1 - 2 * y)) + core + second * (1 - 2 * core)


def two_sum(a, b):
    s = a + b
    t = s - a
    return s, (a - (s - t)) + (b - t)


def fast_two_sum(a, b):
    s = a + b
    return s, b - (s - a)


def split(a):
    c = 4097.0 * a
    high = c - (c - a)
    return high, a - high


def two_prod(a, b):
    p = a * b
    ah, al = split(a)
    bh, bl = split(b)
    return p, ((ah * bh - p) + ah * bl + al * bh) + al * bl


def pair_add(u, v):
    s, e = two_sum(u[0], v[0])
    return fast_two_sum(s, e + (u[1] + v[1]))


def pair_neg(u):
    return -u[0], -u[1]


def pair_mul(u, v):
    p, e = two_prod(u[0], v[0])
    return fast_two_sum(p, e + (u[0] * v[1] + u[1] * v[0]))


def pair_scale(u, c):
    p, e = two_prod(u[0], c)
    return fast_two_sum(p, e + u[1] * c)


def pair_div(u, v):
    q = u[0] / v[0]
    r = pair_add(u, pair_neg(pair_scale(v, q)))
    return fast_two_sum(q, r[0] / v[0])


def pair_tree(items):
    while len(items) > 1:
        items = [pair_add(*items[k : k + 2]) if k + 1 < len(items) else items[k] for k in range(0, len(items), 2)]
    return items[0]


def pair_dot(u, v):
    out = pair_mul(u, v)
    for shift in (4, 2, 1):
        out = pair_add(out, (pltpu.roll(out[0], shift, 0), pltpu.roll(out[1], shift, 0)))
    return out


def device_of(column):
    group, place = lax.div(column, GX), lax.rem(column, GX)
    return mirrored(group, place), snake(group)


def body(
    off_hbm, mass_hbm, cnt_hbm, src_hbm,
    ob, p2,
    off_ref, mass_ref, cnt_ref, src_ref,
    sbuf, inb, xcol, ycol, rcol, wts, part, rb, vb, rows_s, ub, gb,
    g1s, g1, g2s, g2, p1s, p1, p2s, osb,
    load_sem, in_send, in_recv, rho_send, rho_recv, halo_send, halo_recv,
    red_send, red_recv, out_send, out_recv,
):
    a, q = lax.axis_index("gx"), lax.axis_index("gy")
    z, x = lax.div(q, XLEN), lax.rem(q, XLEN)
    group = snake(q)
    place = mirrored(group, a)
    column = group * GX + place
    has_left, has_right = column > 0, column < COLS - 1
    left = device_of(jnp.maximum(column - 1, 0))
    right = device_of(jnp.minimum(column + 1, COLS - 1))
    plane_index = a * XLEN + x
    near_slot, far_slot = 2 - 2 * lax.rem(column, 2), 2 * lax.rem(column, 2)
    has_far = (column + lax.rem(column, 2) > 0) & (column + lax.rem(column, 2) < COLS)

    loads = [
        pltpu.make_async_copy(src, dst, load_sem.at[k])
        for k, (src, dst) in enumerate(
            ((off_hbm, off_ref), (mass_hbm, mass_ref), (src_hbm, src_ref), (cnt_hbm, cnt_ref))
        )
    ]
    for load in loads:
        load.start()

    rim = jnp.zeros((4, SLOT), F32)
    for slot in range(3):
        inb[slot, 0] = rim
        inb[slot, ROWS + 1] = rim
    wide = jnp.zeros((8, SLOT), F32)
    for slot in range(3):
        for end in (0, 24):
            rb[slot, end : end + 8, :] = wide
            for k in range(ITERS):
                vb[k, slot, end : end + 8, :] = wide
    for have, slot in ((has_left, 0), (has_right, 2)):
        @pl.when(jnp.logical_not(have))
        def _(slot=slot):
            inb[slot] = jnp.zeros((ROWS + 2, 4, SLOT), F32)
            rb[slot] = jnp.zeros((32, SLOT), F32)
            for k in range(ITERS):
                vb[k, slot] = jnp.zeros((32, SLOT), F32)

    barrier = pltpu.get_barrier_semaphore()

    y, core = lax.div(a, 2), lax.rem(a, 2)

    def plane_mate(step):
        dy, dx, dc = step
        return lax.rem(y + dy, GX // 2) * 2 + lax.rem(core + dc, 2), z * XLEN + lax.rem(x + dx, XLEN)

    def tower_mate(step):
        return a, lax.rem(z + step, ZLEN) * XLEN + x

    def greet(target):
        pl.semaphore_signal(barrier, inc=1, device_id=target, device_id_type=MESH)

    for step in TOWER_STEPS:
        greet(tower_mate(step))
    for step in PLANE_STEPS:
        greet(plane_mate(step))
    low_edge = (lax.rem(column, PLANE) == 0) & has_left
    high_edge = (lax.rem(column, PLANE) == PLANE - 1) & has_right
    for edge, step in ((low_edge, -1), (high_edge, 1)):
        @pl.when(edge)
        def _(step=step):
            greet(left if step < 0 else right)
            for k in range(GX):
                greet((k, group + step))

    osb[...] = jnp.zeros_like(osb)
    gb[...] = jnp.zeros_like(gb)
    part[0] = jnp.zeros((SLOT, SLOT), F32)
    for load in loads:
        load.wait()

    lane = lax.broadcasted_iota(jnp.int32, (1, SLOT), 1)
    for r in range(2):
        for c in range(GX):
            occ = jnp.where(lane < cnt_ref[r, c], 1.0, 0.0).astype(F32)
            sbuf[c, r, 0:1, :] = off_ref[0, r, c : c + 1, :]
            sbuf[c, r, 1:2, :] = off_ref[1, r, c : c + 1, :]
            sbuf[c, r, 2:3, :] = mass_ref[r, c : c + 1, :] * occ
            sbuf[c, r, 3:4, :] = src_ref[r, c : c + 1, :] * occ

    low_block = (x == 0) & (q > 0)
    high_block = (x == XLEN - 1) & (q < COLS // GX - 1)
    awaited = PLANE - 1 + ZLEN - 1
    for more in (low_block, high_block, low_edge, high_edge):
        awaited = awaited + more.astype(jnp.int32)
    pl.semaphore_wait(barrier, awaited)

    sends = []
    for t in (4, 3, 5, 2, 6, 1, 7, 0):
        c = lax.rem(a + t, GX)
        for d in (0, -1, 1):
            target_column = q * GX + c + d
            wanted = jnp.logical_and(target_column >= 0, target_column < COLS)
            ta, tq = device_of(jnp.clip(target_column, 0, COLS - 1))
            wanted = jnp.logical_and(wanted, jnp.logical_or(ta != a, tq != q))
            copy = pltpu.make_async_remote_copy(
                src_ref=sbuf.at[c],
                dst_ref=inb.at[1 - d, pl.ds(1 + 2 * a, 2)],
                send_sem=in_send.at[len(sends)],
                recv_sem=in_recv.at[1 - d],
                device_id=(ta, tq),
                device_id_type=MESH,
            )
            pl.when(wanted)(copy.start)
            sends.append((wanted, copy))
    for d in (-1, 0, 1):
        own = column + d - q * GX
        inside = (own >= 0) & (own < GX)
        copy = pltpu.make_async_copy(
            sbuf.at[jnp.clip(own, 0, GX - 1)],
            inb.at[1 + d, pl.ds(1 + 2 * a, 2)],
            in_recv.at[1 + d],
        )
        pl.when(inside)(copy.start)

    def arrived(slot):
        view = inb.at[slot, pl.ds(1, ROWS)]
        pltpu.make_async_copy(view, view, in_recv.at[slot]).wait()

    def spread(row):
        return jnp.transpose(jnp.broadcast_to(row, (SLOT, SLOT)))

    def total_row(block):
        return jnp.sum(jnp.transpose(block), axis=0, keepdims=True)

    arrived(1)

    def columns(r, carry):
        xcol[r] = spread(inb[1, r + 1, 0:1, :])
        ycol[r] = spread(inb[1, r + 1, 1:2, :])
        rows_s[0, pl.ds(r, 1), :] = inb[1, r + 1, 2:3, :]
        rows_s[1, pl.ds(r, 1), :] = inb[1, r + 1, 3:4, :]
        return carry

    def columns(r):
        cell = inb[1, r + 1]
        fields = spread(cell[0:1]), spread(cell[1:2]), cell

        def store():
            xcol[r], ycol[r] = fields[0], fields[1]
            rows_s[0, pl.ds(r, 1), :] = cell[2:3]
            rows_s[1, pl.ds(r, 1), :] = cell[3:4]

        return store

    columns(0)()
    pl.when(has_left)(lambda: arrived(0))
    pl.when(has_right)(lambda: arrived(2))

    blocks = [(slot, dr) for slot in (1, near_slot, far_slot) for dr in (0, 1, 2)]
    side = [0.0] * 3 + [(near_slot - 1).astype(F32)] * 3 + [(far_slot - 1).astype(F32)] * 3

    def density_row(r):
        row = 1.0 + total_row(part[r])

        def store():
            rb[1, pl.ds(8 + r, 1), :] = row

        return store

    def falloffs(r, carry):
        store_columns = columns(jnp.minimum(r + 1, ROWS - 1))
        store_row = density_row(jnp.maximum(r - 1, 0))
        rows = []
        for (slot, dr), step_y in zip(blocks, side):
            cell = inb[slot, r + dr]
            mass = cell[2:3, :]
            px = (dr - 1.0) + jnp.where(mass > 0.0, cell[0:1, :], FAR)
            py = step_y + cell[1:2, :]
            rows.append((px, py, mass))
        for h in range(0, SLOT, 64):
            xi, yi = xcol[r, h : h + 64, :], ycol[r, h : h + 64, :]
            acc = jnp.zeros((64, SLOT), F32)
            for k, (px, py, mass) in enumerate(rows):
                ox, oy = px - xi, py - yi
                fall = jnp.maximum(1.0 - (ox * ox + oy * oy), 0.0)
                square = fall * fall
                wts[r, k, h : h + 64, :] = square
                acc = acc + square * fall * mass
            part[r, h : h + 64, :] = acc
        store_columns()
        store_row()
        return carry

    lax.fori_loop(0, ROWS, falloffs, 0)
    density_row(ROWS - 1)()

    def exchange(buf, send, recv):
        copies = []
        for k, (have, target, slot) in enumerate(((has_left, left, 2), (has_right, right, 0))):
            copy = pltpu.make_async_remote_copy(
                src_ref=buf.at[1, pl.ds(8, ROWS)],
                dst_ref=buf.at[slot, pl.ds(8, ROWS)],
                send_sem=send.at[k],
                recv_sem=recv.at[slot],
                device_id=target,
                device_id_type=MESH,
            )
            pl.when(have)(copy.start)
            copies.append((have, copy))

        def wait(slot):
            view = buf.at[slot, pl.ds(8, ROWS)]
            pltpu.make_async_copy(view, view, recv.at[slot]).wait()

        def wait_near():
            wait(near_slot)

        def wait_far():
            pl.when(has_far)(lambda: wait(far_slot))

        return wait_near, wait_far, copies

    wait_rho_near, wait_rho_far, rho_copies = exchange(rb, rho_send, rho_recv)
    sends += rho_copies

    def rho_columns(r, carry):
        rcol[r] = spread(10.0 * rb[1, pl.ds(8 + r, 1), :])
        return carry

    lax.fori_loop(0, ROWS, rho_columns, 0, unroll=ROWS)

    def weights(first, last):
        def run(r, carry):
            rows = [10.0 * rb[slot, pl.ds(7 + r + dr, 1), :] for slot, dr in blocks[first:last]]
            for h in range(0, SLOT, 64):
                ri = rcol[r, h : h + 64, :]
                acc = jnp.zeros((64, SLOT), F32) if first == 0 else part[r, h : h + 64, :]
                for k, row in enumerate(rows, first):
                    w = wts[r, k, h : h + 64, :] / (ri + row)
                    wts[r, k, h : h + 64, :] = w
                    acc = acc + w
                part[r, h : h + 64, :] = acc
            return carry

        lax.fori_loop(0, ROWS, run, 0)

    weights(0, 3)
    wait_rho_near()
    weights(3, 6)
    wait_rho_far()
    weights(6, 9)

    def diagonal_rows(r, carry):
        ub[pl.ds(r, 1), :] = BASE_STIFF + total_row(part[r])
        return carry

    lax.fori_loop(0, ROWS, diagonal_rows, 0, unroll=ROWS)

    occ = jnp.where(rows_s[0] > 0.0, 1.0, 0.0).astype(F32)
    diag = ub[...]
    dinv = occ / diag
    basis = [rows_s[1] * dinv]
    gram_rows = {}

    for k in range(ITERS):
        vb[k, 1, pl.ds(8, ROWS), :] = basis[k]
        wait_near, wait_far, halo_copies = exchange(vb.at[k], halo_send.at[k], halo_recv.at[k])
        sends += halo_copies

        def apply_own(r, carry):
            acc = wts[r, 0] * vb[k, 1, pl.ds(7 + r, 1), :]
            for m in (1, 2):
                acc = acc + wts[r, m] * vb[k, 1, pl.ds(7 + r + m, 1), :]
            part[r] = acc
            return carry

        lax.fori_loop(0, ROWS, apply_own, 0, unroll=2)
        scaled = basis[k] * diag
        for i in range(k + 1):
            gram_rows[i, k] = jnp.sum(basis[i] * scaled, axis=0, keepdims=True)
        wait_near()

        def apply_near(r, carry):
            acc = part[r]
            for m in range(3, 6):
                slot, dr = blocks[m]
                acc = acc + wts[r, m] * vb[k, slot, pl.ds(7 + r + dr, 1), :]
            part[r] = acc
            return carry

        lax.fori_loop(0, ROWS, apply_near, 0, unroll=2)
        wait_far()

        def apply_far(r, carry):
            acc = part[r]
            for m in range(6, 9):
                slot, dr = blocks[m]
                acc = acc + wts[r, m] * vb[k, slot, pl.ds(7 + r + dr, 1), :]
            ub[pl.ds(r, 1), :] = total_row(acc)
            return carry

        lax.fori_loop(0, ROWS, apply_far, 0, unroll=ROWS)
        basis.append(2.0 * (ub[...] * dinv - SHIFTS[k] * basis[k]))

    scaled = basis[ITERS] * diag
    for i in range(ITERS):
        gram_rows[i, ITERS] = jnp.sum(basis[i] * scaled, axis=0, keepdims=True)

    sub8 = lax.broadcasted_iota(jnp.int32, (8, SLOT), 0)
    lane8 = lax.broadcasted_iota(jnp.int32, (8, SLOT), 1)

    for i, j in PAIRS:
        gb[8 * j + i : 8 * j + i + 1, :] = gram_rows[i, j]
        if i != j:
            gb[8 * i + j : 8 * i + j + 1, :] = gram_rows[i, j]
    turned = jnp.transpose(gb[...])
    gram_sum = two_sum(turned[:64], turned[64:])
    for size in (32, 16, 8, 4, 2, 1):
        gram_sum = pair_add((gram_sum[0][:size], gram_sum[1][:size]), (gram_sum[0][size:], gram_sum[1][size:]))

    def gather(rows, own, all_refs, mate, steps, index, send_sem, recv_sem, by_copy=False):
        count = len(steps) + 1

        for k, row in enumerate(rows):
            own[0, k : k + 1, :] = row
        for step in steps:
            copy = pltpu.make_async_remote_copy(
                src_ref=own.at[0],
                dst_ref=all_refs.at[index],
                send_sem=send_sem,
                recv_sem=recv_sem,
                device_id=mate(step),
                device_id_type=MESH,
            )
            copy.start()
        if by_copy:
            pltpu.make_async_copy(own.at[0], all_refs.at[index], recv_sem).start()
        else:
            for k, row in enumerate(rows):
                all_refs[index, k : k + 1, :] = row

        def wait():
            view = all_refs.at[pl.ds(0, count if by_copy else count - 1)]
            pltpu.make_async_copy(view, view, recv_sem).wait()

        def wait_sent():
            view = all_refs.at[pl.ds(0, count - 1)]
            pltpu.make_async_copy(view, view, send_sem).wait()

        return wait, wait_sent

    def pairs_of(refs, count):
        return pair_tree([(refs[k, 0:1, :], refs[k, 1:2, :]) for k in range(count)])

    wait_plane, sent_plane = gather(gram_sum, g1s, g1, plane_mate, PLANE_STEPS, plane_index, red_send.at[0], red_recv.at[0])
    wait_plane()
    plane_sum = pairs_of(g1, PLANE)
    wait_tower, sent_tower = gather(plane_sum, g2s, g2, tower_mate, TOWER_STEPS, z, red_send.at[1], red_recv.at[1])
    wait_tower()
    total = pairs_of(g2, ZLEN)
    high, low = spread(total[0]), spread(total[1])
    gram = [(high[8 * j : 8 * j + 8], low[8 * j : 8 * j + 8]) for j in range(ITERS + 1)]

    zero = jnp.zeros((8, SLOT), F32)
    first = jnp.where(sub8 == 0, 1.0, 0.0).astype(F32)
    keep = zero
    for k, shift in enumerate(SHIFTS):
        keep = jnp.where(sub8 == k, 1.0 - shift, keep)

    def part_of(u, k):
        return tuple(jnp.broadcast_to(w[k : k + 1], (8, SLOT)) for w in u)

    solution_at, residual_at, direction = (zero, zero), (first, zero), (first, zero)
    residual_image = gram[0]
    residuals = []
    rz = part_of(gram[0], 0)
    for k in range(ITERS):
        moved = tuple(-0.5 * pltpu.roll(w, 1, 0) for w in direction)
        image = pair_add(pair_scale(direction, keep), moved)
        gram_image = pair_tree([pair_mul(gram[j], part_of(image, j)) for j in range(k + 2)])
        step = pair_div(rz, pair_dot(direction, gram_image))
        solution_at = pair_add(solution_at, pair_mul(step, direction))
        residual_at = pair_add(residual_at, pair_neg(pair_mul(step, image)))
        residuals.append(residual_at[0])
        if k + 1 < ITERS:
            residual_image = pair_add(residual_image, pair_neg(pair_mul(step, gram_image)))
            new = pair_dot(residual_at, residual_image)
            direction = pair_add(residual_at, pair_mul(pair_div(new, rz), direction))
            rz = new

    def combine(factors, count):
        out = None
        for j in range(count):
            term = factors[j : j + 1] * basis[j]
            out = term if out is None else out + term
        return out

    pressure = combine(solution_at[0], ITERS)
    gb[0:8, :] = jnp.zeros((8, SLOT), F32)
    for k in range(ITERS):
        field = combine(residuals[k], k + 2) * diag
        gb[k : k + 1, :] = jnp.max(jnp.abs(field), axis=0, keepdims=True)
    peak = jnp.max(gb[0:8, :], axis=1, keepdims=True)
    peak_row = jnp.sum(jnp.where(sub8 == lane8, peak, 0.0), axis=0, keepdims=True)
    wait_peaks, sent_peaks = gather([peak_row], p1s, p1, plane_mate, PLANE_STEPS, plane_index, red_send.at[2], red_recv.at[2])

    density = rb[1, pl.ds(8, ROWS), :]
    for r in range(ROWS):
        osb[r, 0:1, :] = density[r : r + 1, :]
        osb[r, 1:2, :] = pressure[r : r + 1, :]
        osb[r, 2:3, :] = field[r : r + 1, :]
    for k in range(GX):
        wanted = jnp.logical_or(a != k, group != q)
        copy = pltpu.make_async_remote_copy(
            src_ref=osb.at[pl.ds(2 * k, 2)],
            dst_ref=ob.at[place],
            send_sem=out_send.at[k],
            recv_sem=out_recv,
            device_id=(k, group),
            device_id_type=MESH,
        )
        pl.when(wanted)(copy.start)
        sends.append((wanted, copy))
    local = pltpu.make_async_copy(osb.at[pl.ds(2 * a, 2)], ob.at[place], out_recv)
    pl.when(group == q)(local.start)

    wait_peaks()
    wait_top, sent_top = gather([jnp.max(p1[...], axis=0)], p2s, p2, tower_mate, TOWER_STEPS, z, red_send.at[3], red_recv.at[3], by_copy=True)
    pltpu.make_async_copy(ob, ob, out_recv).wait()
    wait_top()

    for wanted, copy in sends:
        pl.when(wanted)(copy.wait_send)
    for wait in (sent_plane, sent_tower, sent_peaks, sent_top):
        wait()


def finish(ob, p2, dens_ref, pres_ref, resid_ref, peaks_ref):
    for r in range(2):
        for c in range(GX):
            dens_ref[r, c : c + 1, :] = ob[c, r, 0:1, :]
            pres_ref[r, c : c + 1, :] = ob[c, r, 1:2, :]
            resid_ref[r, c : c + 1, :] = ob[c, r, 2:3, :]
    peaks_ref[...] = jnp.max(p2[...], axis=0)[0, :ITERS]


def shard(offsets, masses, counts, source):
    block = jax.ShapeDtypeStruct((2, GX, SLOT), F32)
    vmem = pl.BlockSpec(memory_space=pltpu.VMEM)
    dma = pltpu.SemaphoreType.DMA
    cells = (ROWS, SLOT, SLOT)
    gathered, peaks = pl.pallas_call(
        body,
        out_shape=(
            pltpu.VMEM((GX, 2, 4, SLOT), F32),
            pltpu.VMEM((ZLEN, 1, SLOT), F32),
        ),
        in_specs=[pl.BlockSpec(memory_space=pl.ANY)] * 4,
        out_specs=(pl.BlockSpec(memory_space=pl.ANY),) * 2,
        scratch_shapes=[
            pltpu.VMEM((2, 2, GX, SLOT), F32),
            pltpu.VMEM((2, GX, SLOT), F32),
            pltpu.SMEM((2, GX), jnp.int32),
            pltpu.VMEM((2, GX, SLOT), F32),
            pltpu.VMEM((GX, 2, 4, SLOT), F32),
            pltpu.VMEM((3, ROWS + 2, 4, SLOT), F32),
            pltpu.VMEM(cells, F32),
            pltpu.VMEM(cells, F32),
            pltpu.VMEM(cells, F32),
            pltpu.VMEM((ROWS, 9, SLOT, SLOT), F32),
            pltpu.VMEM(cells, F32),
            pltpu.VMEM((3, 32, SLOT), F32),
            pltpu.VMEM((ITERS, 3, 32, SLOT), F32),
            pltpu.VMEM((2, ROWS, SLOT), F32),
            pltpu.VMEM((ROWS, SLOT), F32),
            pltpu.VMEM((SLOT, SLOT), F32),
            pltpu.VMEM((1, 2, SLOT), F32),
            pltpu.VMEM((PLANE, 2, SLOT), F32),
            pltpu.VMEM((1, 2, SLOT), F32),
            pltpu.VMEM((ZLEN, 2, SLOT), F32),
            pltpu.VMEM((1, 1, SLOT), F32),
            pltpu.VMEM((PLANE, 1, SLOT), F32),
            pltpu.VMEM((1, 1, SLOT), F32),
            pltpu.VMEM((ROWS, 4, SLOT), F32),
            dma((4,)),
            dma((24,)),
            dma((3,)),
            dma((2,)),
            dma((3,)),
            dma((ITERS, 2)),
            dma((ITERS, 3)),
            dma((4,)),
            dma((4,)),
            dma((GX,)),
            dma,
        ],
        compiler_params=pltpu.CompilerParams(collective_id=0, has_side_effects=True),
    )(offsets, masses, counts, source)
    return pl.pallas_call(
        finish,
        out_shape=(block, block, block, jax.ShapeDtypeStruct((ITERS,), F32)),
        in_specs=[vmem, vmem],
        out_specs=(vmem, vmem, vmem, vmem),
    )(*(pltpu.with_memory_space_constraint(u, pltpu.VMEM) for u in (gathered, peaks)))


def solution(mesh):
    return jax.shard_map(
        shard,
        mesh=mesh,
        in_specs=(P(None, "gx", "gy", None), P("gx", "gy", None), P("gx", "gy"), P("gx", "gy", None)),
        out_specs=(P("gx", "gy", None), P("gx", "gy", None), P("gx", "gy", None), P()),
        check_vma=False,
    )
```

```python
import functools

import jax
import jax.numpy as jnp
from jax import lax
from jax.experimental import pallas as pl
from jax.experimental.pallas import tpu as pltpu
from jax.sharding import PartitionSpec as P

MESH = pl.DeviceIdType.MESH
F32 = jnp.float32

ITERS = 5
SLOT = 128
ROWS = 16
COLS = 256
GX = 8
XLEN = 4
ZLEN = 8
PLANE = GX * XLEN
BASE_STIFF = 0.5
FAR = 1000.0
SHIFTS = (0.8125, 0.0625, 0.8125, 0.125, 0.5)
PAIRS = [(i, j) for i in range(ITERS) for j in range(i, ITERS)]


def hops(step, length):
    return min(step, length - step)


PLANE_STEPS = sorted(
    ((dy, dx, dc) for dy in range(GX // 2) for dx in range(XLEN) for dc in range(2) if (dy, dx, dc) != (0, 0, 0)),
    key=lambda s: -(hops(s[0], GX // 2) + hops(s[1], XLEN) + 0.5 * s[2]),
)
TOWER_STEPS = sorted(range(1, ZLEN), key=lambda s: -hops(s, ZLEN))


def snake(q):
    z, x = lax.div(q, XLEN), lax.rem(q, XLEN)
    return z * XLEN + x + lax.rem(z, 2) * (XLEN - 1 - 2 * x)


def mirrored(g, a):
    y, core = lax.div(a, 2), lax.rem(a, 2)
    second = lax.div(g, COLS // GX // 2)
    return 2 * (y + lax.rem(g, 2) * (GX // 2 - 1 - 2 * y)) + core + second * (1 - 2 * core)


def two_sum(a, b):
    s = a + b
    t = s - a
    return s, (a - (s - t)) + (b - t)


def fast_two_sum(a, b):
    s = a + b
    return s, b - (s - a)


def split(a):
    c = 4097.0 * a
    high = c - (c - a)
    return high, a - high


def two_prod(a, b):
    p = a * b
    ah, al = split(a)
    bh, bl = split(b)
    return p, ((ah * bh - p) + ah * bl + al * bh) + al * bl


def pair_add(u, v):
    s, e = two_sum(u[0], v[0])
    return fast_two_sum(s, e + (u[1] + v[1]))


def pair_neg(u):
    return -u[0], -u[1]


def pair_mul(u, v):
    p, e = two_prod(u[0], v[0])
    return fast_two_sum(p, e + (u[0] * v[1] + u[1] * v[0]))


def pair_scale(u, c):
    p, e = two_prod(u[0], c)
    return fast_two_sum(p, e + u[1] * c)


def pair_div(u, v):
    q = u[0] / v[0]
    r = pair_add(u, pair_neg(pair_scale(v, q)))
    return fast_two_sum(q, r[0] / v[0])


def pair_tree(items):
    while len(items) > 1:
        items = [pair_add(*items[k : k + 2]) if k + 1 < len(items) else items[k] for k in range(0, len(items), 2)]
    return items[0]


def pair_dot(u, v):
    out = pair_mul(u, v)
    for shift in (4, 2, 1):
        out = pair_add(out, (pltpu.roll(out[0], shift, 0), pltpu.roll(out[1], shift, 0)))
    return out


def device_of(column):
    group, place = lax.div(column, GX), lax.rem(column, GX)
    return mirrored(group, place), snake(group)


def body(
    off_hbm, mass_hbm, cnt_hbm, src_hbm,
    ob, p2,
    off_ref, mass_ref, cnt_ref, src_ref,
    sbuf, inb, xcol, ycol, rcol, wts, part, rb, vb, rows_s, ub, gb,
    g1s, g1, g2s, g2, b1s, b1, b2s, b2, p1s, p1, p2s, osb,
    load_sem, in_send, in_recv, cell_send, cell_recv, rho_send, rho_recv, halo_send, halo_recv,
    red_send, red_recv, out_send, out_recv,
):
    a, q = lax.axis_index("gx"), lax.axis_index("gy")
    z, x = lax.div(q, XLEN), lax.rem(q, XLEN)
    group = snake(q)
    place = mirrored(group, a)
    column = group * GX + place
    has_left, has_right = column > 0, column < COLS - 1
    left = device_of(jnp.maximum(column - 1, 0))
    right = device_of(jnp.minimum(column + 1, COLS - 1))
    plane_index = a * XLEN + x
    near_slot, far_slot = 2 - 2 * lax.rem(column, 2), 2 * lax.rem(column, 2)
    has_far = (column + lax.rem(column, 2) > 0) & (column + lax.rem(column, 2) < COLS)

    loads = [
        pltpu.make_async_copy(src, dst, load_sem.at[k])
        for k, (src, dst) in enumerate(
            ((off_hbm, off_ref), (mass_hbm, mass_ref), (src_hbm, src_ref), (cnt_hbm, cnt_ref))
        )
    ]
    for load in loads:
        load.start()

    rim = jnp.zeros((4, SLOT), F32)
    for slot in range(3):
        inb[slot, 0] = rim
        inb[slot, ROWS + 1] = rim
    wide = jnp.zeros((8, SLOT), F32)
    for slot in range(3):
        for end in (0, 24):
            rb[slot, end : end + 8, :] = wide
            for k in range(ITERS):
                vb[k, slot, end : end + 8, :] = wide
    for have, slot in ((has_left, 0), (has_right, 2)):
        @pl.when(jnp.logical_not(have))
        def _(slot=slot):
            inb[slot] = jnp.zeros((ROWS + 2, 4, SLOT), F32)
            rb[slot] = jnp.zeros((32, SLOT), F32)
            for k in range(ITERS):
                vb[k, slot] = jnp.zeros((32, SLOT), F32)

    barrier = pltpu.get_barrier_semaphore()

    y, core = lax.div(a, 2), lax.rem(a, 2)

    def plane_mate(step):
        dy, dx, dc = step
        return lax.rem(y + dy, GX // 2) * 2 + lax.rem(core + dc, 2), z * XLEN + lax.rem(x + dx, XLEN)

    def tower_mate(step):
        return a, lax.rem(z + step, ZLEN) * XLEN + x

    def greet(target):
        pl.semaphore_signal(barrier, inc=1, device_id=target, device_id_type=MESH)

    for step in PLANE_STEPS:
        greet(plane_mate(step))
    for step in TOWER_STEPS:
        greet(tower_mate(step))
    low_edge = (lax.rem(column, PLANE) == 0) & has_left
    high_edge = (lax.rem(column, PLANE) == PLANE - 1) & has_right
    for edge, step in ((low_edge, -1), (high_edge, 1)):
        @pl.when(edge)
        def _(step=step):
            greet(left if step < 0 else right)

    osb[...] = jnp.zeros_like(osb)
    gb[...] = jnp.zeros_like(gb)
    part[0] = jnp.zeros((SLOT, SLOT), F32)
    for load in loads:
        load.wait()

    lane = lax.broadcasted_iota(jnp.int32, (1, SLOT), 1)
    for r in range(2):
        for c in range(GX):
            occ = jnp.where(lane < cnt_ref[r, c], 1.0, 0.0).astype(F32)
            sbuf[c, r, 0:1, :] = off_ref[0, r, c : c + 1, :]
            sbuf[c, r, 1:2, :] = off_ref[1, r, c : c + 1, :]
            sbuf[c, r, 2:3, :] = mass_ref[r, c : c + 1, :] * occ
            sbuf[c, r, 3:4, :] = src_ref[r, c : c + 1, :] * occ

    awaited = PLANE - 1 + ZLEN - 1 + low_edge.astype(jnp.int32) + high_edge.astype(jnp.int32)
    pl.semaphore_wait(barrier, awaited)

    sends = []
    home = snake(q)
    for t in (4, 3, 5, 2, 6, 1, 7, 0):
        target = lax.rem(a + t, GX)
        copy = pltpu.make_async_remote_copy(
            src_ref=sbuf.at[mirrored(q, target)],
            dst_ref=inb.at[1, pl.ds(1 + 2 * a, 2)],
            send_sem=in_send.at[t],
            recv_sem=in_recv,
            device_id=(target, home),
            device_id_type=MESH,
        )
        wanted = jnp.logical_or(target != a, home != q)
        pl.when(wanted)(copy.start)
        sends.append((wanted, copy))
    local = pltpu.make_async_copy(sbuf.at[place], inb.at[1, pl.ds(1 + 2 * a, 2)], in_recv)
    pl.when(home == q)(local.start)

    def exchange(buf, first, send, recv):
        copies = []
        for k, (have, target, slot) in enumerate(((has_left, left, 2), (has_right, right, 0))):
            copy = pltpu.make_async_remote_copy(
                src_ref=buf.at[1, pl.ds(first, ROWS)],
                dst_ref=buf.at[slot, pl.ds(first, ROWS)],
                send_sem=send.at[k],
                recv_sem=recv.at[slot],
                device_id=target,
                device_id_type=MESH,
            )
            pl.when(have)(copy.start)
            copies.append((have, copy))

        def wait(slot):
            view = buf.at[slot, pl.ds(first, ROWS)]
            pltpu.make_async_copy(view, view, recv.at[slot]).wait()

        def wait_near():
            wait(near_slot)

        def wait_far():
            pl.when(has_far)(lambda: wait(far_slot))

        return wait_near, wait_far, copies

    def spread(row):
        return jnp.transpose(jnp.broadcast_to(row, (SLOT, SLOT)))

    def total_row(block):
        return jnp.sum(jnp.transpose(block), axis=0, keepdims=True)

    view = inb.at[1, pl.ds(1, ROWS)]
    pltpu.make_async_copy(view, view, in_recv).wait()
    wait_cells_near, wait_cells_far, cell_copies = exchange(inb, 1, cell_send, cell_recv)
    sends += cell_copies

    def columns(r):
        cell = inb[1, r + 1]
        fields = spread(cell[0:1]), spread(cell[1:2]), cell

        def store():
            xcol[r], ycol[r] = fields[0], fields[1]
            rows_s[0, pl.ds(r, 1), :] = cell[2:3]
            rows_s[1, pl.ds(r, 1), :] = cell[3:4]

        return store

    columns(0)()
    blocks = [(slot, dr) for slot in (1, near_slot, far_slot) for dr in (0, 1, 2)]
    side = [0.0] * 3 + [(near_slot - 1).astype(F32)] * 3 + [(far_slot - 1).astype(F32)] * 3

    def density_row(r):
        row = 1.0 + total_row(part[r])

        def store():
            rb[1, pl.ds(8 + r, 1), :] = row

        return store

    def falloffs(first, last):
        def run(r, carry):
            if first == 0:
                store_columns = columns(jnp.minimum(r + 1, ROWS - 1))
            if last == 9:
                store_row = density_row(jnp.maximum(r - 1, 0))
            rows = []
            for (slot, dr), step_y in zip(blocks[first:last], side[first:last]):
                cell = inb[slot, r + dr]
                mass = cell[2:3, :]
                px = (dr - 1.0) + jnp.where(mass > 0.0, cell[0:1, :], FAR)
                py = step_y + cell[1:2, :]
                rows.append((px, py, mass))
            for h in range(0, SLOT, 64):
                xi, yi = xcol[r, h : h + 64, :], ycol[r, h : h + 64, :]
                acc = jnp.zeros((64, SLOT), F32) if first == 0 else part[r, h : h + 64, :]
                for k, (px, py, mass) in enumerate(rows, first):
                    ox, oy = px - xi, py - yi
                    fall = jnp.maximum(1.0 - (ox * ox + oy * oy), 0.0)
                    square = fall * fall
                    wts[r, k, h : h + 64, :] = square
                    acc = acc + square * fall * mass
                part[r, h : h + 64, :] = acc
            if first == 0:
                store_columns()
            if last == 9:
                store_row()
            return carry

        lax.fori_loop(0, ROWS, run, 0, unroll=2)

    falloffs(0, 3)
    wait_cells_near()
    falloffs(3, 6)
    wait_cells_far()
    falloffs(6, 9)
    density_row(ROWS - 1)()

    wait_rho_near, wait_rho_far, rho_copies = exchange(rb, 8, rho_send, rho_recv)
    sends += rho_copies

    def rho_columns(r, carry):
        rcol[r] = spread(10.0 * rb[1, pl.ds(8 + r, 1), :])
        return carry

    lax.fori_loop(0, ROWS, rho_columns, 0, unroll=ROWS)

    def weights(first, last):
        def run(r, carry):
            rows = [10.0 * rb[slot, pl.ds(7 + r + dr, 1), :] for slot, dr in blocks[first:last]]
            for h in range(0, SLOT, 64):
                ri = rcol[r, h : h + 64, :]
                acc = jnp.zeros((64, SLOT), F32) if first == 0 else part[r, h : h + 64, :]
                for k, row in enumerate(rows, first):
                    w = wts[r, k, h : h + 64, :] / (ri + row)
                    wts[r, k, h : h + 64, :] = w
                    acc = acc + w
                part[r, h : h + 64, :] = acc
            return carry

        lax.fori_loop(0, ROWS, run, 0, unroll=4)

    weights(0, 3)
    wait_rho_near()
    weights(3, 6)
    wait_rho_far()
    weights(6, 9)

    def diagonal_rows(r, carry):
        ub[pl.ds(r, 1), :] = BASE_STIFF + total_row(part[r])
        return carry

    lax.fori_loop(0, ROWS, diagonal_rows, 0, unroll=ROWS)

    occ = jnp.where(rows_s[0] > 0.0, 1.0, 0.0).astype(F32)
    diag = ub[...]
    dinv = occ / diag
    basis = [rows_s[1] * dinv]
    gram_rows = {}
    sub8 = lax.broadcasted_iota(jnp.int32, (8, SLOT), 0)
    lane8 = lax.broadcasted_iota(jnp.int32, (8, SLOT), 1)

    def sublane_sum(block):
        out = two_sum(block[:64], block[64:])
        for size in (32, 16, 8, 4, 2, 1):
            out = pair_add((out[0][:size], out[1][:size]), (out[0][size:], out[1][size:]))
        return out

    def lane_sum(row):
        return sublane_sum(spread(row))

    def pairs_of(refs, count):
        return pair_tree([(refs[k, 0:1, :], refs[k, 1:2, :]) for k in range(count)])

    def gather(rows, own, all_refs, mate, steps, index, send_sem, recv_sem, by_copy=False):
        count = len(steps) + 1

        for k, row in enumerate(rows):
            own[0, k : k + 1, :] = row
        for step in steps:
            copy = pltpu.make_async_remote_copy(
                src_ref=own.at[0],
                dst_ref=all_refs.at[index],
                send_sem=send_sem,
                recv_sem=recv_sem,
                device_id=mate(step),
                device_id_type=MESH,
            )
            copy.start()
        if by_copy:
            pltpu.make_async_copy(own.at[0], all_refs.at[index], recv_sem).start()
        else:
            for k, row in enumerate(rows):
                all_refs[index, k : k + 1, :] = row

        def wait():
            view = all_refs.at[pl.ds(0, count if by_copy else count - 1)]
            pltpu.make_async_copy(view, view, recv_sem).wait()

        def wait_sent():
            view = all_refs.at[pl.ds(0, count - 1)]
            pltpu.make_async_copy(view, view, send_sem).wait()

        return wait, wait_sent


    for k in range(ITERS):
        vb[k, 1, pl.ds(8, ROWS), :] = basis[k]
        wait_near, wait_far, halo_copies = exchange(vb.at[k], 8, halo_send.at[k], halo_recv.at[k])
        sends += halo_copies

        def apply_own(r, carry):
            acc = wts[r, 0] * vb[k, 1, pl.ds(7 + r, 1), :]
            for m in (1, 2):
                acc = acc + wts[r, m] * vb[k, 1, pl.ds(7 + r + m, 1), :]
            part[r] = acc
            return carry

        lax.fori_loop(0, ROWS, apply_own, 0, unroll=4)
        scaled = basis[k] * diag
        for i in range(k + 1):
            gram_rows[i, k] = jnp.sum(basis[i] * scaled, axis=0, keepdims=True)
        if k == ITERS - 1:
            for i, j in PAIRS:
                gb[8 * j + i : 8 * j + i + 1, :] = gram_rows[i, j]
                if i != j:
                    gb[8 * i + j : 8 * i + j + 1, :] = gram_rows[i, j]
            gram_sum = sublane_sum(jnp.transpose(gb[...]))
            wait_plane, sent_plane = gather(
                gram_sum, g1s, g1, plane_mate, PLANE_STEPS, plane_index, red_send.at[0], red_recv.at[0]
            )
        wait_near()

        def apply_near(r, carry):
            acc = part[r]
            for m in range(3, 6):
                slot, dr = blocks[m]
                acc = acc + wts[r, m] * vb[k, slot, pl.ds(7 + r + dr, 1), :]
            part[r] = acc
            return carry

        lax.fori_loop(0, ROWS, apply_near, 0, unroll=4)
        wait_far()

        def apply_far(r, carry):
            acc = part[r]
            for m in range(6, 9):
                slot, dr = blocks[m]
                acc = acc + wts[r, m] * vb[k, slot, pl.ds(7 + r + dr, 1), :]
            ub[pl.ds(r, 1), :] = total_row(acc)
            return carry

        lax.fori_loop(0, ROWS, apply_far, 0, unroll=ROWS)
        basis.append(2.0 * (ub[...] * dinv - SHIFTS[k] * basis[k]))

    last_sum = lane_sum(jnp.sum(basis[ITERS - 1] * ub[...], axis=0, keepdims=True))
    wait_last_plane, sent_last_plane = gather(
        last_sum, b1s, b1, plane_mate, PLANE_STEPS, plane_index, red_send.at[4], red_recv.at[4]
    )
    wait_plane()
    plane_sum = pairs_of(g1, PLANE)
    wait_tower, sent_tower = gather(plane_sum, g2s, g2, tower_mate, TOWER_STEPS, z, red_send.at[1], red_recv.at[1])
    wait_last_plane()
    last_plane_sum = pairs_of(b1, PLANE)
    wait_last_tower, sent_last_tower = gather(
        last_plane_sum, b2s, b2, tower_mate, TOWER_STEPS, z, red_send.at[5], red_recv.at[5]
    )
    wait_tower()
    total = pairs_of(g2, ZLEN)
    high, low = spread(total[0]), spread(total[1])
    gram = [(high[8 * j : 8 * j + 8], low[8 * j : 8 * j + 8]) for j in range(ITERS)]

    zero = jnp.zeros((8, SLOT), F32)
    first = jnp.where(sub8 == 0, 1.0, 0.0).astype(F32)
    keep = zero
    for k, shift in enumerate(SHIFTS):
        keep = jnp.where(sub8 == k, 1.0 - shift, keep)

    def part_of(u, k):
        return tuple(jnp.broadcast_to(w[k : k + 1], (8, SLOT)) for w in u)

    shifted = zero
    for k, shift in enumerate(SHIFTS[:-1]):
        shifted = jnp.where(sub8 == k, 2.0 * (shift - SHIFTS[-1]), shifted)
    following = tuple(pltpu.roll(w, 7, 0) for w in gram[ITERS - 1])
    newest = pair_add(following, pair_scale(gram[ITERS - 1], shifted))
    gram.append(tuple(jnp.where(sub8 < ITERS - 1, w, 0.0) for w in newest))

    solution_at, residual_at, direction = (zero, zero), (first, zero), (first, zero)
    residual_image = gram[0]
    residuals = []
    rz = part_of(gram[0], 0)
    for k in range(ITERS):
        moved = tuple(-0.5 * pltpu.roll(w, 1, 0) for w in direction)
        image = pair_add(pair_scale(direction, keep), moved)
        gram_image = pair_tree([pair_mul(gram[j], part_of(image, j)) for j in range(k + 2)])
        curvature = pair_dot(direction, gram_image)
        if k + 1 < ITERS:
            step = pair_div(rz, curvature)
            solution_at = pair_add(solution_at, pair_mul(step, direction))
            residual_at = pair_add(residual_at, pair_neg(pair_mul(step, image)))
            residuals.append(residual_at[0])
            residual_image = pair_add(residual_image, pair_neg(pair_mul(step, gram_image)))
            new = pair_dot(residual_at, residual_image)
            direction = pair_add(residual_at, pair_mul(pair_div(new, rz), direction))
            rz = new
    corner = pair_mul(part_of(direction, ITERS - 1), part_of(image, ITERS))
    corner = tuple(2.0 * w for w in corner)
    curvature = pair_add(
        curvature, pair_mul(corner, pair_scale(part_of(gram[ITERS - 1], ITERS - 1), -SHIFTS[-1]))
    )

    def combine(factors, count):
        out = None
        for j in range(count):
            term = factors[j : j + 1] * basis[j]
            out = term if out is None else out + term
        return out

    gb[0:8, :] = jnp.zeros((8, SLOT), F32)
    for k in range(ITERS - 1):
        field = combine(residuals[k], k + 2) * diag
        gb[k : k + 1, :] = jnp.max(jnp.abs(field), axis=0, keepdims=True)
    pressure = combine(solution_at[0], ITERS - 1)
    along = combine(direction[0], ITERS)
    drop = combine(image[0], ITERS + 1) * diag
    wait_last_tower()
    last = tuple(jnp.broadcast_to(w, (8, SLOT)) for w in pairs_of(b2, ZLEN))
    step = pair_div(rz, pair_add(curvature, pair_mul(corner, last)))[0][0:1]
    pressure = pressure + step * along
    field = field - step * drop
    gb[ITERS - 1 : ITERS, :] = jnp.max(jnp.abs(field), axis=0, keepdims=True)
    peak = jnp.max(gb[0:8, :], axis=1, keepdims=True)
    peak_row = jnp.sum(jnp.where(sub8 == lane8, peak, 0.0), axis=0, keepdims=True)
    wait_peaks, sent_peaks = gather([peak_row], p1s, p1, plane_mate, PLANE_STEPS, plane_index, red_send.at[2], red_recv.at[2])

    density = rb[1, pl.ds(8, ROWS), :]
    for r in range(ROWS):
        osb[r, 0:1, :] = density[r : r + 1, :]
        osb[r, 1:2, :] = pressure[r : r + 1, :]
        osb[r, 2:3, :] = field[r : r + 1, :]
    for k in range(GX):
        wanted = jnp.logical_or(a != k, group != q)
        copy = pltpu.make_async_remote_copy(
            src_ref=osb.at[pl.ds(2 * k, 2)],
            dst_ref=ob.at[place],
            send_sem=out_send.at[k],
            recv_sem=out_recv,
            device_id=(k, group),
            device_id_type=MESH,
        )
        pl.when(wanted)(copy.start)
        sends.append((wanted, copy))
    local = pltpu.make_async_copy(osb.at[pl.ds(2 * a, 2)], ob.at[place], out_recv)
    pl.when(group == q)(local.start)

    wait_peaks()
    wait_top, sent_top = gather([jnp.max(p1[...], axis=0)], p2s, p2, tower_mate, TOWER_STEPS, z, red_send.at[3], red_recv.at[3], by_copy=True)
    pltpu.make_async_copy(ob, ob, out_recv).wait()
    wait_top()

    for wanted, copy in sends:
        pl.when(wanted)(copy.wait_send)
    for wait in (sent_plane, sent_tower, sent_last_plane, sent_last_tower, sent_peaks, sent_top):
        wait()


def finish(ob, p2, dens_ref, pres_ref, resid_ref, peaks_ref):
    for r in range(2):
        for c in range(GX):
            dens_ref[r, c : c + 1, :] = ob[c, r, 0:1, :]
            pres_ref[r, c : c + 1, :] = ob[c, r, 1:2, :]
            resid_ref[r, c : c + 1, :] = ob[c, r, 2:3, :]
    peaks_ref[...] = jnp.max(p2[...], axis=0)[0, :ITERS]


def shard(offsets, masses, counts, source):
    block = jax.ShapeDtypeStruct((2, GX, SLOT), F32)
    vmem = pl.BlockSpec(memory_space=pltpu.VMEM)
    dma = pltpu.SemaphoreType.DMA
    cells = (ROWS, SLOT, SLOT)
    gathered, peaks = pl.pallas_call(
        body,
        out_shape=(
            pltpu.VMEM((GX, 2, 4, SLOT), F32),
            pltpu.VMEM((ZLEN, 1, SLOT), F32),
        ),
        in_specs=[pl.BlockSpec(memory_space=pl.ANY)] * 4,
        out_specs=(pl.BlockSpec(memory_space=pl.ANY),) * 2,
        scratch_shapes=[
            pltpu.VMEM((2, 2, GX, SLOT), F32),
            pltpu.VMEM((2, GX, SLOT), F32),
            pltpu.SMEM((2, GX), jnp.int32),
            pltpu.VMEM((2, GX, SLOT), F32),
            pltpu.VMEM((GX, 2, 4, SLOT), F32),
            pltpu.VMEM((3, ROWS + 2, 4, SLOT), F32),
            pltpu.VMEM(cells, F32),
            pltpu.VMEM(cells, F32),
            pltpu.VMEM(cells, F32),
            pltpu.VMEM((ROWS, 9, SLOT, SLOT), F32),
            pltpu.VMEM(cells, F32),
            pltpu.VMEM((3, 32, SLOT), F32),
            pltpu.VMEM((ITERS, 3, 32, SLOT), F32),
            pltpu.VMEM((2, ROWS, SLOT), F32),
            pltpu.VMEM((ROWS, SLOT), F32),
            pltpu.VMEM((SLOT, SLOT), F32),
            pltpu.VMEM((1, 2, SLOT), F32),
            pltpu.VMEM((PLANE, 2, SLOT), F32),
            pltpu.VMEM((1, 2, SLOT), F32),
            pltpu.VMEM((ZLEN, 2, SLOT), F32),
            pltpu.VMEM((1, 2, SLOT), F32),
            pltpu.VMEM((PLANE, 2, SLOT), F32),
            pltpu.VMEM((1, 2, SLOT), F32),
            pltpu.VMEM((ZLEN, 2, SLOT), F32),
            pltpu.VMEM((1, 1, SLOT), F32),
            pltpu.VMEM((PLANE, 1, SLOT), F32),
            pltpu.VMEM((1, 1, SLOT), F32),
            pltpu.VMEM((ROWS, 4, SLOT), F32),
            dma((4,)),
            dma((GX,)),
            dma,
            dma((2,)),
            dma((3,)),
            dma((2,)),
            dma((3,)),
            dma((ITERS, 2)),
            dma((ITERS, 3)),
            dma((6,)),
            dma((6,)),
            dma((GX,)),
            dma,
        ],
        compiler_params=pltpu.CompilerParams(collective_id=0, has_side_effects=True),
    )(offsets, masses, counts, source)
    return pl.pallas_call(
        finish,
        out_shape=(block, block, block, jax.ShapeDtypeStruct((ITERS,), F32)),
        in_specs=[vmem, vmem],
        out_specs=(vmem, vmem, vmem, vmem),
    )(*(pltpu.with_memory_space_constraint(u, pltpu.VMEM) for u in (gathered, peaks)))


def solution(mesh):
    return jax.shard_map(
        shard,
        mesh=mesh,
        in_specs=(P(None, "gx", "gy", None), P("gx", "gy", None), P("gx", "gy"), P("gx", "gy", None)),
        out_specs=(P("gx", "gy", None), P("gx", "gy", None), P("gx", "gy", None), P()),
        check_vma=False,
    )
```

```python
import functools

import jax
import jax.numpy as jnp
from jax import lax
from jax.experimental import pallas as pl
from jax.experimental.pallas import tpu as pltpu
from jax.sharding import PartitionSpec as P

MESH = pl.DeviceIdType.MESH
F32 = jnp.float32

ITERS = 5
SLOT = 128
ROWS = 16
COLS = 256
GX = 8
XLEN = 4
ZLEN = 8
PLANE = GX * XLEN
BASE_STIFF = 0.5
FAR = 1000.0
SHIFTS = (0.8125, 0.0625, 0.8125, 0.125, 0.5)
PAIRS = [(i, j) for i in range(ITERS) for j in range(i, ITERS)]


def hops(step, length):
    return min(step, length - step)


PLANE_STEPS = sorted(
    ((dy, dx, dc) for dy in range(GX // 2) for dx in range(XLEN) for dc in range(2) if (dy, dx, dc) != (0, 0, 0)),
    key=lambda s: -(hops(s[0], GX // 2) + hops(s[1], XLEN) + 0.5 * s[2]),
)
TOWER_STEPS = sorted(((dz, core) for dz in range(1, ZLEN) for core in range(2)), key=lambda s: -hops(s[0], ZLEN) + 0.5 * s[1])


def snake(q):
    z, x = lax.div(q, XLEN), lax.rem(q, XLEN)
    return z * XLEN + x + lax.rem(z, 2) * (XLEN - 1 - 2 * x)


def mirrored(g, a):
    y, core = lax.div(a, 2), lax.rem(a, 2)
    second = lax.div(g, COLS // GX // 2)
    return 2 * (y + lax.rem(g, 2) * (GX // 2 - 1 - 2 * y)) + core + second * (1 - 2 * core)


def two_sum(a, b):
    s = a + b
    t = s - a
    return s, (a - (s - t)) + (b - t)


def fast_two_sum(a, b):
    s = a + b
    return s, b - (s - a)


def split(a):
    c = 4097.0 * a
    high = c - (c - a)
    return high, a - high


def two_prod(a, b):
    p = a * b
    ah, al = split(a)
    bh, bl = split(b)
    return p, ((ah * bh - p) + ah * bl + al * bh) + al * bl


def pair_add(u, v):
    s, e = two_sum(u[0], v[0])
    return fast_two_sum(s, e + (u[1] + v[1]))


def pair_neg(u):
    return -u[0], -u[1]


def pair_mul(u, v):
    p, e = two_prod(u[0], v[0])
    return fast_two_sum(p, e + (u[0] * v[1] + u[1] * v[0]))


def pair_scale(u, c):
    p, e = two_prod(u[0], c)
    return fast_two_sum(p, e + u[1] * c)


def pair_div(u, v):
    q = u[0] / v[0]
    r = pair_add(u, pair_neg(pair_scale(v, q)))
    return fast_two_sum(q, r[0] / v[0])


def pair_tree(items):
    while len(items) > 1:
        items = [pair_add(*items[k : k + 2]) if k + 1 < len(items) else items[k] for k in range(0, len(items), 2)]
    return items[0]


def pair_dot(u, v):
    out = pair_mul(u, v)
    for shift in (4, 2, 1):
        out = pair_add(out, (pltpu.roll(out[0], shift, 0), pltpu.roll(out[1], shift, 0)))
    return out


def device_of(column):
    group, place = lax.div(column, GX), lax.rem(column, GX)
    return mirrored(group, place), snake(group)


def body(
    off_hbm, mass_hbm, cnt_hbm, src_hbm,
    ob, p2,
    off_ref, mass_ref, cnt_ref, src_ref,
    sbuf, inb, xcol, ycol, rcol, wts, part, rb, vb, rows_s, ub, gb,
    g1s, g1, g2s, g2, b1s, b1, b2s, b2, p1s, p1, p2s, osb,
    load_sem, in_send, in_recv, cell_send, cell_recv, rho_send, rho_recv, halo_send, halo_recv,
    red_send, red_recv, out_send, out_recv,
):
    a, q = lax.axis_index("gx"), lax.axis_index("gy")
    z, x = lax.div(q, XLEN), lax.rem(q, XLEN)
    group = snake(q)
    place = mirrored(group, a)
    column = group * GX + place
    has_left, has_right = column > 0, column < COLS - 1
    left = device_of(jnp.maximum(column - 1, 0))
    right = device_of(jnp.minimum(column + 1, COLS - 1))
    plane_index = a * XLEN + x
    near_slot, far_slot = 2 - 2 * lax.rem(column, 2), 2 * lax.rem(column, 2)
    has_far = (column + lax.rem(column, 2) > 0) & (column + lax.rem(column, 2) < COLS)

    loads = [
        pltpu.make_async_copy(src, dst, load_sem.at[k])
        for k, (src, dst) in enumerate(
            ((off_hbm, off_ref), (mass_hbm, mass_ref), (src_hbm, src_ref), (cnt_hbm, cnt_ref))
        )
    ]
    for load in loads:
        load.start()

    rim = jnp.zeros((4, SLOT), F32)
    for slot in range(3):
        inb[slot, 0] = rim
        inb[slot, ROWS + 1] = rim
    wide = jnp.zeros((8, SLOT), F32)
    for slot in range(3):
        for end in (0, 24):
            rb[slot, end : end + 8, :] = wide
            for k in range(ITERS):
                vb[k, slot, end : end + 8, :] = wide
    for have, slot in ((has_left, 0), (has_right, 2)):
        @pl.when(jnp.logical_not(have))
        def _(slot=slot):
            inb[slot] = jnp.zeros((ROWS + 2, 4, SLOT), F32)
            rb[slot] = jnp.zeros((32, SLOT), F32)
            for k in range(ITERS):
                vb[k, slot] = jnp.zeros((32, SLOT), F32)

    barrier = pltpu.get_barrier_semaphore()

    y, core = lax.div(a, 2), lax.rem(a, 2)

    def plane_mate(step):
        dy, dx, dc = step
        return lax.rem(y + dy, GX // 2) * 2 + lax.rem(core + dc, 2), z * XLEN + lax.rem(x + dx, XLEN)

    def tower_mate(step):
        return 2 * y + step[1], lax.rem(z + step[0], ZLEN) * XLEN + x

    def greet(target):
        pl.semaphore_signal(barrier, inc=1, device_id=target, device_id_type=MESH)

    for step in PLANE_STEPS:
        greet(plane_mate(step))
    for step in TOWER_STEPS:
        if step[1]:
            greet(tower_mate(step))
    low_edge = (lax.rem(column, PLANE) == 0) & has_left
    high_edge = (lax.rem(column, PLANE) == PLANE - 1) & has_right
    for edge, step in ((low_edge, -1), (high_edge, 1)):
        @pl.when(edge)
        def _(step=step):
            greet(left if step < 0 else right)

    osb[...] = jnp.zeros_like(osb)
    gb[...] = jnp.zeros_like(gb)
    part[0] = jnp.zeros((SLOT, SLOT), F32)
    for load in loads:
        load.wait()

    lane = lax.broadcasted_iota(jnp.int32, (1, SLOT), 1)
    for r in range(2):
        for c in range(GX):
            occ = jnp.where(lane < cnt_ref[r, c], 1.0, 0.0).astype(F32)
            sbuf[c, r, 0:1, :] = off_ref[0, r, c : c + 1, :]
            sbuf[c, r, 1:2, :] = off_ref[1, r, c : c + 1, :]
            sbuf[c, r, 2:3, :] = mass_ref[r, c : c + 1, :] * occ
            sbuf[c, r, 3:4, :] = src_ref[r, c : c + 1, :] * occ

    awaited = PLANE - 1 + 2 * (ZLEN - 1) * core + low_edge.astype(jnp.int32) + high_edge.astype(jnp.int32)
    pl.semaphore_wait(barrier, awaited)

    sends = []
    home = snake(q)
    for t in (4, 3, 5, 2, 6, 1, 7, 0):
        target = lax.rem(a + t, GX)
        copy = pltpu.make_async_remote_copy(
            src_ref=sbuf.at[mirrored(q, target)],
            dst_ref=inb.at[1, pl.ds(1 + 2 * a, 2)],
            send_sem=in_send.at[t],
            recv_sem=in_recv,
            device_id=(target, home),
            device_id_type=MESH,
        )
        wanted = jnp.logical_or(target != a, home != q)
        pl.when(wanted)(copy.start)
        sends.append((wanted, copy))
    local = pltpu.make_async_copy(sbuf.at[place], inb.at[1, pl.ds(1 + 2 * a, 2)], in_recv)
    pl.when(home == q)(local.start)

    def exchange(buf, first, send, recv):
        copies = []
        for k, (have, target, slot) in enumerate(((has_left, left, 2), (has_right, right, 0))):
            copy = pltpu.make_async_remote_copy(
                src_ref=buf.at[1, pl.ds(first, ROWS)],
                dst_ref=buf.at[slot, pl.ds(first, ROWS)],
                send_sem=send.at[k],
                recv_sem=recv.at[slot],
                device_id=target,
                device_id_type=MESH,
            )
            pl.when(have)(copy.start)
            copies.append((have, copy))

        def wait(slot):
            view = buf.at[slot, pl.ds(first, ROWS)]
            pltpu.make_async_copy(view, view, recv.at[slot]).wait()

        def wait_near():
            wait(near_slot)

        def wait_far():
            pl.when(has_far)(lambda: wait(far_slot))

        return wait_near, wait_far, copies

    def spread(row):
        return jnp.transpose(jnp.broadcast_to(row, (SLOT, SLOT)))

    def total_row(block):
        return jnp.sum(jnp.transpose(block), axis=0, keepdims=True)

    view = inb.at[1, pl.ds(1, ROWS)]
    pltpu.make_async_copy(view, view, in_recv).wait()
    wait_cells_near, wait_cells_far, cell_copies = exchange(inb, 1, cell_send, cell_recv)
    sends += cell_copies

    def columns(r):
        cell = inb[1, r + 1]
        fields = spread(cell[0:1]), spread(cell[1:2]), cell

        def store():
            xcol[r], ycol[r] = fields[0], fields[1]
            rows_s[0, pl.ds(r, 1), :] = cell[2:3]
            rows_s[1, pl.ds(r, 1), :] = cell[3:4]

        return store

    columns(0)()
    blocks = [(slot, dr) for slot in (1, near_slot, far_slot) for dr in (0, 1, 2)]
    side = [0.0] * 3 + [(near_slot - 1).astype(F32)] * 3 + [(far_slot - 1).astype(F32)] * 3

    def density_row(r):
        row = 1.0 + total_row(part[r])

        def store():
            rb[1, pl.ds(8 + r, 1), :] = row

        return store

    def falloffs(first, last):
        def run(r, carry):
            if first == 0:
                store_columns = columns(jnp.minimum(r + 1, ROWS - 1))
            rows = []
            for (slot, dr), step_y in zip(blocks[first:last], side[first:last]):
                cell = inb[slot, r + dr]
                mass = cell[2:3, :]
                px = (dr - 1.0) + jnp.where(mass > 0.0, cell[0:1, :], FAR)
                py = step_y + cell[1:2, :]
                rows.append((px, py, mass))
            for h in range(0, SLOT, 64):
                xi, yi = xcol[r, h : h + 64, :], ycol[r, h : h + 64, :]
                acc = jnp.zeros((64, SLOT), F32) if first == 0 else part[r, h : h + 64, :]
                for k, (px, py, mass) in enumerate(rows, first):
                    ox, oy = px - xi, py - yi
                    fall = jnp.maximum(1.0 - (ox * ox + oy * oy), 0.0)
                    square = fall * fall
                    wts[r, k, h : h + 64, :] = square
                    acc = acc + square * fall * mass
                part[r, h : h + 64, :] = acc
            if first == 0:
                store_columns()
            if last == 9:
                density_row(r)()
            return carry

        lax.fori_loop(0, ROWS, run, 0, unroll=16 if last == 9 else 4)

    falloffs(0, 3)
    wait_cells_near()
    falloffs(3, 6)
    wait_cells_far()
    falloffs(6, 9)

    wait_rho_near, wait_rho_far, rho_copies = exchange(rb, 8, rho_send, rho_recv)
    sends += rho_copies

    def rho_columns(r, carry):
        rcol[r] = spread(10.0 * rb[1, pl.ds(8 + r, 1), :])
        return carry

    lax.fori_loop(0, ROWS, rho_columns, 0, unroll=ROWS)

    def weights(first, last):
        def run(r, carry):
            rows = [10.0 * rb[slot, pl.ds(7 + r + dr, 1), :] for slot, dr in blocks[first:last]]
            for h in range(0, SLOT, 64):
                ri = rcol[r, h : h + 64, :]
                acc = jnp.zeros((64, SLOT), F32) if first == 0 else part[r, h : h + 64, :]
                for k, row in enumerate(rows, first):
                    w = wts[r, k, h : h + 64, :] / (ri + row)
                    wts[r, k, h : h + 64, :] = w
                    acc = acc + w
                part[r, h : h + 64, :] = acc
            if last == 9:
                ub[pl.ds(r, 1), :] = BASE_STIFF + total_row(part[r])
            return carry

        lax.fori_loop(0, ROWS, run, 0, unroll=ROWS if last == 9 else 4)

    weights(0, 3)
    wait_rho_near()
    weights(3, 6)
    wait_rho_far()
    weights(6, 9)

    occ = jnp.where(rows_s[0] > 0.0, 1.0, 0.0).astype(F32)
    diag = ub[...]
    dinv = occ / diag
    basis = [rows_s[1] * dinv]
    gram_rows = {}
    sub8 = lax.broadcasted_iota(jnp.int32, (8, SLOT), 0)
    lane8 = lax.broadcasted_iota(jnp.int32, (8, SLOT), 1)

    def sublane_sum(block):
        out = two_sum(block[:64], block[64:])
        for size in (32, 16, 8, 4, 2, 1):
            out = pair_add((out[0][:size], out[1][:size]), (out[0][size:], out[1][size:]))
        return out

    def lane_sum(row):
        return sublane_sum(spread(row))

    def pairs_of(refs, count):
        return pair_tree([(refs[k, 0:1, :], refs[k, 1:2, :]) for k in range(count)])

    def gather(rows, own, all_refs, mate, steps, index, send_sem, recv_sem, spare=None):
        for k, row in enumerate(rows):
            own[0, k : k + 1, :] = row

        def send():
            for step in steps:
                pltpu.make_async_remote_copy(
                    src_ref=own.at[0],
                    dst_ref=all_refs.at[index],
                    send_sem=send_sem,
                    recv_sem=recv_sem,
                    device_id=mate(step),
                    device_id_type=MESH,
                ).start()

        def wait_sent():
            view = (all_refs if spare is None else spare).at[pl.ds(0, len(steps))]
            pltpu.make_async_copy(view, view, send_sem).wait()

        if spare is None:
            send()
        else:
            pl.when(core == 1)(send)
        by_copy = all_refs is p2
        if by_copy:
            pltpu.make_async_copy(own.at[0], all_refs.at[index], recv_sem).start()
        else:
            for k, row in enumerate(rows):
                all_refs[index, k : k + 1, :] = row

        def wait():
            view = all_refs.at[pl.ds(0, all_refs.shape[0] - 1 + by_copy)]
            pltpu.make_async_copy(view, view, recv_sem).wait()

        return wait, (wait_sent if spare is None else lambda: pl.when(core == 1)(wait_sent))


    for k in range(ITERS):
        vb[k, 1, pl.ds(8, ROWS), :] = basis[k]
        wait_near, wait_far, halo_copies = exchange(vb.at[k], 8, halo_send.at[k], halo_recv.at[k])
        sends += halo_copies

        def apply_own(r, carry):
            acc = wts[r, 0] * vb[k, 1, pl.ds(7 + r, 1), :]
            for m in (1, 2):
                acc = acc + wts[r, m] * vb[k, 1, pl.ds(7 + r + m, 1), :]
            part[r] = acc
            return carry

        lax.fori_loop(0, ROWS, apply_own, 0, unroll=4)
        scaled = basis[k] * diag
        for i in range(k + 1):
            gram_rows[i, k] = jnp.sum(basis[i] * scaled, axis=0, keepdims=True)
        if k == ITERS - 1:
            for i, j in PAIRS:
                gb[8 * j + i : 8 * j + i + 1, :] = gram_rows[i, j]
                if i != j:
                    gb[8 * i + j : 8 * i + j + 1, :] = gram_rows[i, j]
            gram_sum = sublane_sum(jnp.transpose(gb[...]))
            wait_plane, sent_plane = gather(
                gram_sum, g1s, g1, plane_mate, PLANE_STEPS, plane_index, red_send.at[0], red_recv.at[0]
            )
        wait_near()

        def apply_near(r, carry):
            acc = part[r]
            for m in range(3, 6):
                slot, dr = blocks[m]
                acc = acc + wts[r, m] * vb[k, slot, pl.ds(7 + r + dr, 1), :]
            part[r] = acc
            return carry

        lax.fori_loop(0, ROWS, apply_near, 0, unroll=4)
        wait_far()

        def apply_far(r, carry):
            acc = part[r]
            for m in range(6, 9):
                slot, dr = blocks[m]
                acc = acc + wts[r, m] * vb[k, slot, pl.ds(7 + r + dr, 1), :]
            ub[pl.ds(r, 1), :] = total_row(acc)
            return carry

        lax.fori_loop(0, ROWS, apply_far, 0, unroll=ROWS)
        basis.append(2.0 * (ub[...] * dinv - SHIFTS[k] * basis[k]))

    last_sum = lane_sum(jnp.sum(basis[ITERS - 1] * ub[...], axis=0, keepdims=True))
    wait_last_plane, sent_last_plane = gather(
        last_sum, b1s, b1, plane_mate, PLANE_STEPS, plane_index, red_send.at[4], red_recv.at[4]
    )
    wait_plane()
    plane_sum = pairs_of(g1, PLANE)
    wait_tower, sent_tower = gather(plane_sum, g2s, g2, tower_mate, TOWER_STEPS, z, red_send.at[1], red_recv.at[1], g1)
    wait_last_plane()
    last_plane_sum = pairs_of(b1, PLANE)
    wait_last_tower, sent_last_tower = gather(
        last_plane_sum, b2s, b2, tower_mate, TOWER_STEPS, z, red_send.at[5], red_recv.at[5], b1
    )
    wait_tower()
    total = pairs_of(g2, ZLEN)
    high, low = spread(total[0]), spread(total[1])
    gram = [(high[8 * j : 8 * j + 8], low[8 * j : 8 * j + 8]) for j in range(ITERS)]

    zero = jnp.zeros((8, SLOT), F32)
    first = jnp.where(sub8 == 0, 1.0, 0.0).astype(F32)
    keep = zero
    for k, shift in enumerate(SHIFTS):
        keep = jnp.where(sub8 == k, 1.0 - shift, keep)

    def part_of(u, k):
        return tuple(jnp.broadcast_to(w[k : k + 1], (8, SLOT)) for w in u)

    shifted = zero
    for k, shift in enumerate(SHIFTS[:-1]):
        shifted = jnp.where(sub8 == k, 2.0 * (shift - SHIFTS[-1]), shifted)
    following = tuple(pltpu.roll(w, 7, 0) for w in gram[ITERS - 1])
    newest = pair_add(following, pair_scale(gram[ITERS - 1], shifted))
    gram.append(tuple(jnp.where(sub8 < ITERS - 1, w, 0.0) for w in newest))

    solution_at, residual_at, direction = (zero, zero), (first, zero), (first, zero)
    residual_image = gram[0]
    residuals = []
    rz = part_of(gram[0], 0)
    for k in range(ITERS):
        moved = tuple(-0.5 * pltpu.roll(w, 1, 0) for w in direction)
        image = pair_add(pair_scale(direction, keep), moved)
        gram_image = pair_tree([pair_mul(gram[j], part_of(image, j)) for j in range(k + 2)])
        curvature = pair_dot(direction, gram_image)
        if k + 1 < ITERS:
            step = pair_div(rz, curvature)
            solution_at = pair_add(solution_at, pair_mul(step, direction))
            residual_at = pair_add(residual_at, pair_neg(pair_mul(step, image)))
            residuals.append(residual_at[0])
            residual_image = pair_add(residual_image, pair_neg(pair_mul(step, gram_image)))
            new = pair_dot(residual_at, residual_image)
            direction = pair_add(residual_at, pair_mul(pair_div(new, rz), direction))
            rz = new
    corner = pair_mul(part_of(direction, ITERS - 1), part_of(image, ITERS))
    corner = tuple(2.0 * w for w in corner)
    curvature = pair_add(
        curvature, pair_mul(corner, pair_scale(part_of(gram[ITERS - 1], ITERS - 1), -SHIFTS[-1]))
    )

    def combine(factors, count):
        out = None
        for j in range(count):
            term = factors[j : j + 1] * basis[j]
            out = term if out is None else out + term
        return out

    gb[0:8, :] = jnp.zeros((8, SLOT), F32)
    for k in range(ITERS - 1):
        field = combine(residuals[k], k + 2) * diag
        gb[k : k + 1, :] = jnp.max(jnp.abs(field), axis=0, keepdims=True)
    pressure = combine(solution_at[0], ITERS - 1)
    along = combine(direction[0], ITERS)
    drop = combine(image[0], ITERS + 1) * diag
    wait_last_tower()
    last = tuple(jnp.broadcast_to(w, (8, SLOT)) for w in pairs_of(b2, ZLEN))
    step = pair_div(rz, pair_add(curvature, pair_mul(corner, last)))[0][0:1]
    pressure = pressure + step * along
    field = field - step * drop
    gb[ITERS - 1 : ITERS, :] = jnp.max(jnp.abs(field), axis=0, keepdims=True)
    peak = jnp.max(gb[0:8, :], axis=1, keepdims=True)
    peak_row = jnp.sum(jnp.where(sub8 == lane8, peak, 0.0), axis=0, keepdims=True)
    wait_peaks, sent_peaks = gather([peak_row], p1s, p1, plane_mate, PLANE_STEPS, plane_index, red_send.at[2], red_recv.at[2])

    density = rb[1, pl.ds(8, ROWS), :]
    for r in range(ROWS):
        osb[r, 0:1, :] = density[r : r + 1, :]
        osb[r, 1:2, :] = pressure[r : r + 1, :]
        osb[r, 2:3, :] = field[r : r + 1, :]
    for k in range(GX):
        wanted = jnp.logical_or(a != k, group != q)
        copy = pltpu.make_async_remote_copy(
            src_ref=osb.at[pl.ds(2 * k, 2)],
            dst_ref=ob.at[place],
            send_sem=out_send.at[k],
            recv_sem=out_recv,
            device_id=(k, group),
            device_id_type=MESH,
        )
        pl.when(wanted)(copy.start)
        sends.append((wanted, copy))
    local = pltpu.make_async_copy(osb.at[pl.ds(2 * a, 2)], ob.at[place], out_recv)
    pl.when(group == q)(local.start)

    wait_peaks()
    wait_top, sent_top = gather([jnp.max(p1[...], axis=0)], p2s, p2, tower_mate, TOWER_STEPS, z, red_send.at[3], red_recv.at[3], p1)
    pltpu.make_async_copy(ob, ob, out_recv).wait()
    wait_top()

    for wanted, copy in sends:
        pl.when(wanted)(copy.wait_send)
    for wait in (sent_plane, sent_tower, sent_last_plane, sent_last_tower, sent_peaks, sent_top):
        wait()


def finish(ob, p2, dens_ref, pres_ref, resid_ref, peaks_ref):
    for r in range(2):
        for c in range(GX):
            dens_ref[r, c : c + 1, :] = ob[c, r, 0:1, :]
            pres_ref[r, c : c + 1, :] = ob[c, r, 1:2, :]
            resid_ref[r, c : c + 1, :] = ob[c, r, 2:3, :]
    peaks_ref[...] = jnp.max(p2[...], axis=0)[0, :ITERS]


def shard(offsets, masses, counts, source):
    block = jax.ShapeDtypeStruct((2, GX, SLOT), F32)
    vmem = pl.BlockSpec(memory_space=pltpu.VMEM)
    dma = pltpu.SemaphoreType.DMA
    cells = (ROWS, SLOT, SLOT)
    gathered, peaks = pl.pallas_call(
        body,
        out_shape=(
            pltpu.VMEM((GX, 2, 4, SLOT), F32),
            pltpu.VMEM((ZLEN, 1, SLOT), F32),
        ),
        in_specs=[pl.BlockSpec(memory_space=pl.ANY)] * 4,
        out_specs=(pl.BlockSpec(memory_space=pl.ANY),) * 2,
        scratch_shapes=[
            pltpu.VMEM((2, 2, GX, SLOT), F32),
            pltpu.VMEM((2, GX, SLOT), F32),
            pltpu.SMEM((2, GX), jnp.int32),
            pltpu.VMEM((2, GX, SLOT), F32),
            pltpu.VMEM((GX, 2, 4, SLOT), F32),
            pltpu.VMEM((3, ROWS + 2, 4, SLOT), F32),
            pltpu.VMEM(cells, F32),
            pltpu.VMEM(cells, F32),
            pltpu.VMEM(cells, F32),
            pltpu.VMEM((ROWS, 9, SLOT, SLOT), F32),
            pltpu.VMEM(cells, F32),
            pltpu.VMEM((3, 32, SLOT), F32),
            pltpu.VMEM((ITERS, 3, 32, SLOT), F32),
            pltpu.VMEM((2, ROWS, SLOT), F32),
            pltpu.VMEM((ROWS, SLOT), F32),
            pltpu.VMEM((SLOT, SLOT), F32),
            pltpu.VMEM((1, 2, SLOT), F32),
            pltpu.VMEM((PLANE, 2, SLOT), F32),
            pltpu.VMEM((1, 2, SLOT), F32),
            pltpu.VMEM((ZLEN, 2, SLOT), F32),
            pltpu.VMEM((1, 2, SLOT), F32),
            pltpu.VMEM((PLANE, 2, SLOT), F32),
            pltpu.VMEM((1, 2, SLOT), F32),
            pltpu.VMEM((ZLEN, 2, SLOT), F32),
            pltpu.VMEM((1, 1, SLOT), F32),
            pltpu.VMEM((PLANE, 1, SLOT), F32),
            pltpu.VMEM((1, 1, SLOT), F32),
            pltpu.VMEM((ROWS, 4, SLOT), F32),
            dma((4,)),
            dma((GX,)),
            dma,
            dma((2,)),
            dma((3,)),
            dma((2,)),
            dma((3,)),
            dma((ITERS, 2)),
            dma((ITERS, 3)),
            dma((6,)),
            dma((6,)),
            dma((GX,)),
            dma,
        ],
        compiler_params=pltpu.CompilerParams(collective_id=0, has_side_effects=True),
    )(offsets, masses, counts, source)
    return pl.pallas_call(
        finish,
        out_shape=(block, block, block, jax.ShapeDtypeStruct((ITERS,), F32)),
        in_specs=[vmem, vmem],
        out_specs=(vmem, vmem, vmem, vmem),
    )(*(pltpu.with_memory_space_constraint(u, pltpu.VMEM) for u in (gathered, peaks)))


def solution(mesh):
    return jax.shard_map(
        shard,
        mesh=mesh,
        in_specs=(P(None, "gx", "gy", None), P("gx", "gy", None), P("gx", "gy"), P("gx", "gy", None)),
        out_specs=(P("gx", "gy", None), P("gx", "gy", None), P("gx", "gy", None), P()),
        check_vma=False,
    )
```

```python
import jax
import jax.numpy as jnp
from jax import lax
from jax.experimental import pallas as pl
from jax.experimental.pallas import tpu as pltpu
from jax.sharding import PartitionSpec as P

MESH = pl.DeviceIdType.MESH
F32 = jnp.float32

ITERS = 5
SLOT = 128
ROWS = 16
COLS = 256
GX = 8
XLEN = 4
ZLEN = 8
PLANE = GX * XLEN
BASE_STIFF = 0.5
FAR = 1000.0
SHIFTS = (0.8125, 0.0625, 0.8125, 0.125, 0.5)
PAIRS = [(i, j) for i in range(ITERS) for j in range(i, ITERS)]


def hops(step, length):
    return min(step, length - step)


PLANE_STEPS = sorted(
    ((dy, dx, dc) for dy in range(GX // 2) for dx in range(XLEN) for dc in range(2) if (dy, dx, dc) != (0, 0, 0)),
    key=lambda s: -(hops(s[0], GX // 2) + hops(s[1], XLEN) + 0.5 * s[2]),
)
WALL_STEPS = sorted(
    ((dy, dc, dz) for dy in range(GX // 2) for dc in range(2) for dz in range(ZLEN) if (dy, dc, dz) != (0, 0, 0)),
    key=lambda s: -(hops(s[0], GX // 2) + 0.5 * s[1] + hops(s[2], ZLEN)),
)
TOWER_STEPS = sorted(((dz, core) for dz in range(1, ZLEN) for core in range(2)), key=lambda s: -hops(s[0], ZLEN) + 0.5 * s[1])


def snake(q):
    z, x = lax.div(q, XLEN), lax.rem(q, XLEN)
    return z * XLEN + x + lax.rem(z, 2) * (XLEN - 1 - 2 * x)


def mirrored(g, a):
    y, core = lax.div(a, 2), lax.rem(a, 2)
    second = lax.div(g, COLS // GX // 2)
    return 2 * (y + lax.rem(g, 2) * (GX // 2 - 1 - 2 * y)) + core + second * (1 - 2 * core)


def two_sum(a, b):
    s = a + b
    t = s - a
    return s, (a - (s - t)) + (b - t)


def fast_two_sum(a, b):
    s = a + b
    return s, b - (s - a)


def split(a):
    c = 4097.0 * a
    high = c - (c - a)
    return high, a - high


def two_prod(a, b):
    p = a * b
    ah, al = split(a)
    bh, bl = split(b)
    return p, ((ah * bh - p) + ah * bl + al * bh) + al * bl


def pair_add(u, v):
    s, e = two_sum(u[0], v[0])
    return fast_two_sum(s, e + (u[1] + v[1]))


def pair_neg(u):
    return -u[0], -u[1]


def pair_mul(u, v):
    p, e = two_prod(u[0], v[0])
    return fast_two_sum(p, e + (u[0] * v[1] + u[1] * v[0]))


def pair_scale(u, c):
    p, e = two_prod(u[0], c)
    return fast_two_sum(p, e + u[1] * c)


def pair_div(u, v):
    q = u[0] / v[0]
    r = pair_add(u, pair_neg(pair_scale(v, q)))
    return fast_two_sum(q, r[0] / v[0])


def pair_tree(items):
    while len(items) > 1:
        items = [pair_add(*items[k : k + 2]) if k + 1 < len(items) else items[k] for k in range(0, len(items), 2)]
    return items[0]


def pair_dot(u, v):
    out = pair_mul(u, v)
    for shift in (4, 2, 1):
        out = pair_add(out, (pltpu.roll(out[0], shift, 0), pltpu.roll(out[1], shift, 0)))
    return out


def device_of(column):
    group, place = lax.div(column, GX), lax.rem(column, GX)
    return mirrored(group, place), snake(group)


def body(
    off_hbm, mass_hbm, cnt_hbm, src_hbm,
    ob, p1,
    off_ref, mass_ref, cnt_ref, src_ref,
    sbuf, inb, xcol, ycol, rcol, wts, part, rb, vb, rows_s, ub, gb,
    g1s, g1, g2s, g2, b1s, b1, b2s, b2, p1s, osb, tb,
    load_sem, in_send, in_recv, cell_send, cell_recv, rho_send, rho_recv, halo_send, halo_recv,
    red_send, red_recv, row_send, row_recv, out_send, out_recv,
):
    a, q = lax.axis_index("gx"), lax.axis_index("gy")
    z, x = lax.div(q, XLEN), lax.rem(q, XLEN)
    group = snake(q)
    place = mirrored(group, a)
    column = group * GX + place
    has_left, has_right = column > 0, column < COLS - 1
    left = device_of(jnp.maximum(column - 1, 0))
    right = device_of(jnp.minimum(column + 1, COLS - 1))
    plane_index = a * XLEN + x
    near_slot, far_slot = 2 - 2 * lax.rem(column, 2), 2 * lax.rem(column, 2)
    has_far = (column + lax.rem(column, 2) > 0) & (column + lax.rem(column, 2) < COLS)

    loads = [
        pltpu.make_async_copy(src, dst, load_sem.at[k])
        for k, (src, dst) in enumerate(
            ((off_hbm, off_ref), (mass_hbm, mass_ref), (src_hbm, src_ref), (cnt_hbm, cnt_ref))
        )
    ]
    for load in loads:
        load.start()

    rim = jnp.zeros((4, SLOT), F32)
    for slot in range(3):
        inb[slot, 0] = rim
        inb[slot, ROWS + 1] = rim
    wide = jnp.zeros((8, SLOT), F32)
    for slot in range(3):
        for end in (0, 24):
            rb[slot, end : end + 8, :] = wide
            for k in range(ITERS):
                vb[k, slot, end : end + 8, :] = wide
    for have, slot in ((has_left, 0), (has_right, 2)):
        @pl.when(jnp.logical_not(have))
        def _(slot=slot):
            inb[slot] = jnp.zeros((ROWS + 2, 4, SLOT), F32)
            rb[slot] = jnp.zeros((32, SLOT), F32)
            for k in range(ITERS):
                vb[k, slot] = jnp.zeros((32, SLOT), F32)

    barrier = pltpu.get_barrier_semaphore()

    y, core = lax.div(a, 2), lax.rem(a, 2)

    def plane_mate(step):
        dy, dx, dc = step
        return lax.rem(y + dy, GX // 2) * 2 + lax.rem(core + dc, 2), z * XLEN + lax.rem(x + dx, XLEN)

    def tower_mate(step):
        return 2 * y + step[1], lax.rem(z + step[0], ZLEN) * XLEN + x

    def wall_mate(step):
        dy, dc, dz = step
        return lax.rem(y + dy, GX // 2) * 2 + lax.rem(core + dc, 2), lax.rem(z + dz, ZLEN) * XLEN + x

    def greet(target):
        pl.semaphore_signal(barrier, inc=1, device_id=target, device_id_type=MESH)

    for step in PLANE_STEPS:
        greet(plane_mate(step))
    for step in TOWER_STEPS:
        if step[1]:
            greet(tower_mate(step))
    low_edge = (lax.rem(column, PLANE) == 0) & has_left
    high_edge = (lax.rem(column, PLANE) == PLANE - 1) & has_right
    for edge, target in ((low_edge, left), (high_edge, right)):
        @pl.when(edge)
        def _(target=target):
            greet(target)

    osb[...] = jnp.zeros_like(osb)
    gb[...] = jnp.zeros_like(gb)
    part[0] = jnp.zeros((SLOT, SLOT), F32)
    for load in loads:
        load.wait()

    lane = lax.broadcasted_iota(jnp.int32, (1, SLOT), 1)
    for r in range(2):
        for c in range(GX):
            occ = jnp.where(lane < cnt_ref[r, c], 1.0, 0.0).astype(F32)
            sbuf[c, r, 0:1, :] = off_ref[0, r, c : c + 1, :]
            sbuf[c, r, 1:2, :] = off_ref[1, r, c : c + 1, :]
            sbuf[c, r, 2:3, :] = mass_ref[r, c : c + 1, :] * occ
            sbuf[c, r, 3:4, :] = src_ref[r, c : c + 1, :] * occ

    awaited = PLANE - 1 + 2 * (ZLEN - 1) * core + low_edge.astype(jnp.int32) + high_edge.astype(jnp.int32)
    pl.semaphore_wait(barrier, awaited)

    sends = []
    home = snake(q)
    for t in (4, 3, 5, 2, 6, 1, 7, 0):
        target = lax.rem(a + t, GX)
        copy = pltpu.make_async_remote_copy(
            src_ref=sbuf.at[mirrored(q, target)],
            dst_ref=inb.at[1, pl.ds(1 + 2 * a, 2)],
            send_sem=in_send.at[t],
            recv_sem=in_recv,
            device_id=(target, home),
            device_id_type=MESH,
        )
        wanted = jnp.logical_or(target != a, home != q)
        pl.when(wanted)(copy.start)
        sends.append((wanted, copy))
    local = pltpu.make_async_copy(sbuf.at[place], inb.at[1, pl.ds(1 + 2 * a, 2)], in_recv)
    pl.when(home == q)(local.start)

    def exchange(buf, first, send, recv):
        copies = []
        for k, (have, target, slot) in enumerate(((has_left, left, 2), (has_right, right, 0))):
            copy = pltpu.make_async_remote_copy(
                src_ref=buf.at[1, pl.ds(first, ROWS)],
                dst_ref=buf.at[slot, pl.ds(first, ROWS)],
                send_sem=send.at[k],
                recv_sem=recv.at[slot],
                device_id=target,
                device_id_type=MESH,
            )
            pl.when(have)(copy.start)
            copies.append((have, copy))

        def wait(slot):
            view = buf.at[slot, pl.ds(first, ROWS)]
            pltpu.make_async_copy(view, view, recv.at[slot]).wait()

        def wait_near():
            wait(near_slot)

        def wait_far():
            pl.when(has_far)(lambda: wait(far_slot))

        return wait_near, wait_far, copies

    def spread(row):
        return jnp.transpose(jnp.broadcast_to(row, (SLOT, SLOT)))

    def total_row(block):
        return jnp.sum(jnp.transpose(block), axis=0, keepdims=True)

    view = inb.at[1, pl.ds(1, ROWS)]
    pltpu.make_async_copy(view, view, in_recv).wait()
    wait_cells_near, wait_cells_far, cell_copies = exchange(inb, 1, cell_send, cell_recv)
    sends += cell_copies

    def columns(r):
        cell = inb[1, r + 1]
        fields = spread(cell[0:1]), spread(cell[1:2]), cell

        def store():
            xcol[r], ycol[r] = fields[0], fields[1]
            rows_s[0, pl.ds(r, 1), :] = cell[2:3]
            rows_s[1, pl.ds(r, 1), :] = cell[3:4]

        return store

    columns(0)()
    blocks = [(slot, dr) for slot in (1, near_slot, far_slot) for dr in (0, 1, 2)]
    side = [0.0] * 3 + [(near_slot - 1).astype(F32)] * 3 + [(far_slot - 1).astype(F32)] * 3

    def density_row(r):
        row = 1.0 + total_row(part[r])

        def store():
            rb[1, pl.ds(8 + r, 1), :] = row

        return store

    def falloffs(first, last):
        def run(r, carry):
            if first == 0:
                store_columns = columns(jnp.minimum(r + 1, ROWS - 1))
            rows = []
            for (slot, dr), step_y in zip(blocks[first:last], side[first:last]):
                cell = inb[slot, r + dr]
                mass = cell[2:3, :]
                px = (dr - 1.0) + jnp.where(mass > 0.0, cell[0:1, :], FAR)
                py = step_y + cell[1:2, :]
                rows.append((px, py, mass))
            for h in range(0, SLOT, 64):
                xi, yi = xcol[r, h : h + 64, :], ycol[r, h : h + 64, :]
                acc = jnp.zeros((64, SLOT), F32) if first == 0 else part[r, h : h + 64, :]
                for k, (px, py, mass) in enumerate(rows, first):
                    ox, oy = px - xi, py - yi
                    fall = jnp.maximum(1.0 - (ox * ox + oy * oy), 0.0)
                    square = fall * fall
                    wts[r, k, h : h + 64, :] = square
                    acc = acc + square * fall * mass
                part[r, h : h + 64, :] = acc
            if first == 0:
                store_columns()
            if last == 9:
                density_row(r)()
            return carry

        lax.fori_loop(0, ROWS, run, 0, unroll=16 if last == 9 else 4)

    falloffs(0, 3)
    wait_cells_near()
    falloffs(3, 6)
    wait_cells_far()
    falloffs(6, 9)

    wait_rho_near, wait_rho_far, rho_copies = exchange(rb, 8, rho_send, rho_recv)
    sends += rho_copies

    def rho_columns(r, carry):
        rcol[r] = spread(10.0 * rb[1, pl.ds(8 + r, 1), :])
        return carry

    lax.fori_loop(0, ROWS, rho_columns, 0, unroll=ROWS)

    def weights(first, last):
        def run(r, carry):
            rows = [10.0 * rb[slot, pl.ds(7 + r + dr, 1), :] for slot, dr in blocks[first:last]]
            for h in range(0, SLOT, 64):
                ri = rcol[r, h : h + 64, :]
                acc = jnp.zeros((64, SLOT), F32) if first == 0 else part[r, h : h + 64, :]
                for k, row in enumerate(rows, first):
                    w = wts[r, k, h : h + 64, :] / (ri + row)
                    wts[r, k, h : h + 64, :] = w
                    acc = acc + w
                part[r, h : h + 64, :] = acc
            if last == 9:
                ub[pl.ds(r, 1), :] = BASE_STIFF + total_row(part[r])
            return carry

        lax.fori_loop(0, ROWS, run, 0, unroll=ROWS if last == 9 else 4)

    weights(0, 3)
    wait_rho_near()
    weights(3, 6)
    wait_rho_far()
    weights(6, 9)

    occ = jnp.where(rows_s[0] > 0.0, 1.0, 0.0).astype(F32)
    diag = ub[...]
    dinv = occ / diag
    basis = [rows_s[1] * dinv]
    gram_rows = {}
    sub8 = lax.broadcasted_iota(jnp.int32, (8, SLOT), 0)
    lane8 = lax.broadcasted_iota(jnp.int32, (8, SLOT), 1)

    def sublane_sum(block):
        out = two_sum(block[:64], block[64:])
        for size in (32, 16, 8, 4, 2, 1):
            out = pair_add((out[0][:size], out[1][:size]), (out[0][size:], out[1][size:]))
        return out

    def lane_sum(row):
        return sublane_sum(spread(row))

    def pairs_of(refs, count):
        return pair_tree([(refs[k, 0:1, :], refs[k, 1:2, :]) for k in range(count)])

    def gather(rows, own, all_refs, mate, steps, index, send_sem, recv_sem, spare=None):
        for k, row in enumerate(rows):
            own[0, k : k + 1, :] = row

        def send():
            for step in steps:
                pltpu.make_async_remote_copy(
                    src_ref=own.at[0],
                    dst_ref=all_refs.at[index],
                    send_sem=send_sem,
                    recv_sem=recv_sem,
                    device_id=mate(step),
                    device_id_type=MESH,
                ).start()

        def wait_sent():
            view = (all_refs if spare is None else spare).at[pl.ds(0, len(steps))]
            pltpu.make_async_copy(view, view, send_sem).wait()

        if spare is None:
            send()
        else:
            pl.when(core == 1)(send)
        by_copy = all_refs is p1
        if by_copy:
            pltpu.make_async_copy(own.at[0], all_refs.at[index], recv_sem).start()
        else:
            for k, row in enumerate(rows):
                all_refs[index, k : k + 1, :] = row

        def wait():
            view = all_refs.at[pl.ds(0, all_refs.shape[0] - 1 + by_copy)]
            pltpu.make_async_copy(view, view, recv_sem).wait()

        return wait, (wait_sent if spare is None else lambda: pl.when(core == 1)(wait_sent))


    def replicate(k):
        tb[k, x] = basis[k] * diag
        for step in (2, 1, 3):
            pltpu.make_async_remote_copy(
                src_ref=tb.at[k, x],
                dst_ref=tb.at[k, x],
                send_sem=row_send.at[k],
                recv_sem=row_recv.at[k],
                device_id=(a, z * XLEN + lax.rem(x + step, XLEN)),
                device_id_type=MESH,
            ).start()

    def wait_replicas(k, sem):
        view = tb.at[k, pl.ds(0, XLEN - 1)]
        pltpu.make_async_copy(view, view, sem.at[k]).wait()

    for k in range(ITERS):
        vb[k, 1, pl.ds(8, ROWS), :] = basis[k]
        wait_near, wait_far, halo_copies = exchange(vb.at[k], 8, halo_send.at[k], halo_recv.at[k])
        sends += halo_copies

        def apply_own(r, carry):
            acc = wts[r, 0] * vb[k, 1, pl.ds(7 + r, 1), :]
            for m in (1, 2):
                acc = acc + wts[r, m] * vb[k, 1, pl.ds(7 + r + m, 1), :]
            part[r] = acc
            return carry

        lax.fori_loop(0, ROWS, apply_own, 0, unroll=4)
        replicate(k)
        scaled = basis[k] * diag
        for i in range(k + 1):
            gram_rows[i, k] = jnp.sum(basis[i] * scaled, axis=0, keepdims=True)
        if k == ITERS - 1:
            for i, j in PAIRS:
                gb[8 * j + i : 8 * j + i + 1, :] = gram_rows[i, j]
                if i != j:
                    gb[8 * i + j : 8 * i + j + 1, :] = gram_rows[i, j]
            gram_sum = sublane_sum(jnp.transpose(gb[...]))
            wait_plane, sent_plane = gather(
                gram_sum, g1s, g1, plane_mate, PLANE_STEPS, plane_index, red_send.at[0], red_recv.at[0]
            )
        wait_near()

        def apply_near(r, carry):
            acc = part[r]
            for m in range(3, 6):
                slot, dr = blocks[m]
                acc = acc + wts[r, m] * vb[k, slot, pl.ds(7 + r + dr, 1), :]
            part[r] = acc
            return carry

        lax.fori_loop(0, ROWS, apply_near, 0, unroll=4)
        wait_far()

        def apply_far(r, carry):
            acc = part[r]
            for m in range(6, 9):
                slot, dr = blocks[m]
                acc = acc + wts[r, m] * vb[k, slot, pl.ds(7 + r + dr, 1), :]
            ub[pl.ds(r, 1), :] = total_row(acc)
            return carry

        lax.fori_loop(0, ROWS, apply_far, 0, unroll=ROWS)
        basis.append(2.0 * (ub[...] * dinv - SHIFTS[k] * basis[k]))

    last_sum = lane_sum(jnp.sum(basis[ITERS - 1] * ub[...], axis=0, keepdims=True))
    wait_last_plane, sent_last_plane = gather(
        last_sum, b1s, b1, plane_mate, PLANE_STEPS, plane_index, red_send.at[4], red_recv.at[4]
    )
    replicate(ITERS)
    wait_plane()
    plane_sum = pairs_of(g1, PLANE)
    wait_tower, sent_tower = gather(plane_sum, g2s, g2, tower_mate, TOWER_STEPS, z, red_send.at[1], red_recv.at[1], g1)
    wait_last_plane()
    last_plane_sum = pairs_of(b1, PLANE)
    wait_last_tower, sent_last_tower = gather(
        last_plane_sum, b2s, b2, tower_mate, TOWER_STEPS, z, red_send.at[5], red_recv.at[5], b1
    )
    wait_tower()
    total = pairs_of(g2, ZLEN)
    high, low = spread(total[0]), spread(total[1])
    gram = [(high[8 * j : 8 * j + 8], low[8 * j : 8 * j + 8]) for j in range(ITERS)]

    zero = jnp.zeros((8, SLOT), F32)
    first = jnp.where(sub8 == 0, 1.0, 0.0).astype(F32)
    keep = zero
    for k, shift in enumerate(SHIFTS):
        keep = jnp.where(sub8 == k, 1.0 - shift, keep)

    def part_of(u, k):
        return tuple(jnp.broadcast_to(w[k : k + 1], (8, SLOT)) for w in u)

    shifted = zero
    for k, shift in enumerate(SHIFTS[:-1]):
        shifted = jnp.where(sub8 == k, 2.0 * (shift - SHIFTS[-1]), shifted)
    following = tuple(pltpu.roll(w, 7, 0) for w in gram[ITERS - 1])
    newest = pair_add(following, pair_scale(gram[ITERS - 1], shifted))
    gram.append(tuple(jnp.where(sub8 < ITERS - 1, w, 0.0) for w in newest))

    solution_at, residual_at, direction = (zero, zero), (first, zero), (first, zero)
    residual_image = gram[0]
    residuals = []
    rz = part_of(gram[0], 0)
    for k in range(ITERS):
        moved = tuple(-0.5 * pltpu.roll(w, 1, 0) for w in direction)
        image = pair_add(pair_scale(direction, keep), moved)
        gram_image = pair_tree([pair_mul(gram[j], part_of(image, j)) for j in range(k + 2)])
        curvature = pair_dot(direction, gram_image)
        if k + 1 < ITERS:
            step = pair_div(rz, curvature)
            solution_at = pair_add(solution_at, pair_mul(step, direction))
            residual_at = pair_add(residual_at, pair_neg(pair_mul(step, image)))
            residuals.append(residual_at[0])
            residual_image = pair_add(residual_image, pair_neg(pair_mul(step, gram_image)))
            new = pair_dot(residual_at, residual_image)
            direction = pair_add(residual_at, pair_mul(pair_div(new, rz), direction))
            rz = new
    corner = pair_mul(part_of(direction, ITERS - 1), part_of(image, ITERS))
    corner = tuple(2.0 * w for w in corner)
    curvature = pair_add(
        curvature, pair_mul(corner, pair_scale(part_of(gram[ITERS - 1], ITERS - 1), -SHIFTS[-1]))
    )

    def combine(factors, count):
        out = None
        for j in range(count):
            term = factors[j : j + 1] * basis[j]
            out = term if out is None else out + term
        return out

    field = combine(residuals[-1], ITERS) * diag
    drop = combine(image[0], ITERS + 1) * diag
    pressure = combine(solution_at[0], ITERS - 1)
    along = combine(direction[0], ITERS)
    for k in range(ITERS + 1):
        wait_replicas(k, row_recv)

    def row_combine(factors, count, t):
        out = None
        for j in range(count):
            term = factors[j : j + 1] * tb[j, t]
            out = term if out is None else out + term
        return out

    gb[0:8, :] = jnp.zeros((8, SLOT), F32)
    peaks = [None] * ITERS

    def raise_peak(k, values):
        values = jnp.abs(values)
        peaks[k] = values if peaks[k] is None else jnp.maximum(peaks[k], values)

    row_fields = []
    for t in range(XLEN):
        for k in range(ITERS - 1):
            values = row_combine(residuals[k], k + 2, t)
            raise_peak(k, values)
        row_fields.append((values, row_combine(image[0], ITERS + 1, t)))
    for k in range(ITERS - 1):
        gb[k : k + 1, :] = jnp.max(peaks[k], axis=0, keepdims=True)
    wait_last_tower()
    last = tuple(jnp.broadcast_to(w, (8, SLOT)) for w in pairs_of(b2, ZLEN))
    step = pair_div(rz, pair_add(curvature, pair_mul(corner, last)))[0][0:1]
    pressure = pressure + step * along
    field = field - step * drop
    for values, change in row_fields:
        raise_peak(ITERS - 1, values - step * change)
    gb[ITERS - 1 : ITERS, :] = jnp.max(peaks[ITERS - 1], axis=0, keepdims=True)
    peak = jnp.max(gb[0:8, :], axis=1, keepdims=True)
    peak_row = jnp.sum(jnp.where(sub8 == lane8, peak, 0.0), axis=0, keepdims=True)
    wait_peaks, sent_peaks = gather([peak_row], p1s, p1, wall_mate, WALL_STEPS, a * ZLEN + z, red_send.at[2], red_recv.at[2])

    density = rb[1, pl.ds(8, ROWS), :]
    for r in range(ROWS):
        osb[r, 0:1, :] = density[r : r + 1, :]
        osb[r, 1:2, :] = pressure[r : r + 1, :]
        osb[r, 2:3, :] = field[r : r + 1, :]
    for k in range(GX):
        wanted = jnp.logical_or(a != k, group != q)
        copy = pltpu.make_async_remote_copy(
            src_ref=osb.at[pl.ds(2 * k, 2)],
            dst_ref=ob.at[place],
            send_sem=out_send.at[k],
            recv_sem=out_recv,
            device_id=(k, group),
            device_id_type=MESH,
        )
        pl.when(wanted)(copy.start)
        sends.append((wanted, copy))
    local = pltpu.make_async_copy(osb.at[pl.ds(2 * a, 2)], ob.at[place], out_recv)
    pl.when(group == q)(local.start)

    wait_peaks()
    pltpu.make_async_copy(ob, ob, out_recv).wait()

    for wanted, copy in sends:
        pl.when(wanted)(copy.wait_send)
    for wait in (sent_plane, sent_tower, sent_last_plane, sent_last_tower, sent_peaks):
        wait()
    for k in range(ITERS + 1):
        wait_replicas(k, row_send)


def finish(ob, p1, dens_ref, pres_ref, resid_ref, peaks_ref):
    for r in range(2):
        for c in range(GX):
            dens_ref[r, c : c + 1, :] = ob[c, r, 0:1, :]
            pres_ref[r, c : c + 1, :] = ob[c, r, 1:2, :]
            resid_ref[r, c : c + 1, :] = ob[c, r, 2:3, :]
    peaks_ref[...] = jnp.max(p1[...], axis=0)[0, :ITERS]


def shard(offsets, masses, counts, source):
    block = jax.ShapeDtypeStruct((2, GX, SLOT), F32)
    vmem = pl.BlockSpec(memory_space=pltpu.VMEM)
    dma = pltpu.SemaphoreType.DMA
    cells = (ROWS, SLOT, SLOT)
    gathered, peaks = pl.pallas_call(
        body,
        out_shape=(
            pltpu.VMEM((GX, 2, 4, SLOT), F32),
            pltpu.VMEM((GX * ZLEN, 1, SLOT), F32),
        ),
        in_specs=[pl.BlockSpec(memory_space=pl.ANY)] * 4,
        out_specs=(pl.BlockSpec(memory_space=pl.ANY),) * 2,
        scratch_shapes=[
            pltpu.VMEM((2, 2, GX, SLOT), F32),
            pltpu.VMEM((2, GX, SLOT), F32),
            pltpu.SMEM((2, GX), jnp.int32),
            pltpu.VMEM((2, GX, SLOT), F32),
            pltpu.VMEM((GX, 2, 4, SLOT), F32),
            pltpu.VMEM((3, ROWS + 2, 4, SLOT), F32),
            pltpu.VMEM(cells, F32),
            pltpu.VMEM(cells, F32),
            pltpu.VMEM(cells, F32),
            pltpu.VMEM((ROWS, 9, SLOT, SLOT), F32),
            pltpu.VMEM(cells, F32),
            pltpu.VMEM((3, 32, SLOT), F32),
            pltpu.VMEM((ITERS, 3, 32, SLOT), F32),
            pltpu.VMEM((2, ROWS, SLOT), F32),
            pltpu.VMEM((ROWS, SLOT), F32),
            pltpu.VMEM((SLOT, SLOT), F32),
            pltpu.VMEM((1, 2, SLOT), F32),
            pltpu.VMEM((PLANE, 2, SLOT), F32),
            pltpu.VMEM((1, 2, SLOT), F32),
            pltpu.VMEM((ZLEN, 2, SLOT), F32),
            pltpu.VMEM((1, 2, SLOT), F32),
            pltpu.VMEM((PLANE, 2, SLOT), F32),
            pltpu.VMEM((1, 2, SLOT), F32),
            pltpu.VMEM((ZLEN, 2, SLOT), F32),
            pltpu.VMEM((1, 1, SLOT), F32),
            pltpu.VMEM((ROWS, 4, SLOT), F32),
            pltpu.VMEM((ITERS + 1, XLEN, ROWS, SLOT), F32),
            dma((4,)),
            dma((GX,)),
            dma,
            dma((2,)),
            dma((3,)),
            dma((2,)),
            dma((3,)),
            dma((ITERS, 2)),
            dma((ITERS, 3)),
            dma((6,)),
            dma((6,)),
            dma((ITERS + 1,)),
            dma((ITERS + 1,)),
            dma((GX,)),
            dma,
        ],
        compiler_params=pltpu.CompilerParams(collective_id=0, has_side_effects=True),
    )(offsets, masses, counts, source)
    return pl.pallas_call(
        finish,
        out_shape=(block, block, block, jax.ShapeDtypeStruct((ITERS,), F32)),
        in_specs=[vmem, vmem],
        out_specs=(vmem, vmem, vmem, vmem),
    )(*(pltpu.with_memory_space_constraint(u, pltpu.VMEM) for u in (gathered, peaks)))


def solution(mesh):
    return jax.shard_map(
        shard,
        mesh=mesh,
        in_specs=(P(None, "gx", "gy", None), P("gx", "gy", None), P("gx", "gy"), P("gx", "gy", None)),
        out_specs=(P("gx", "gy", None), P("gx", "gy", None), P("gx", "gy", None), P()),
        check_vma=False,
    )
```

```python
import jax
import jax.numpy as jnp
from jax import lax
from jax.experimental import pallas as pl
from jax.experimental.pallas import tpu as pltpu
from jax.sharding import PartitionSpec as P

MESH = pl.DeviceIdType.MESH
F32 = jnp.float32

ITERS = 5
SLOT = 128
ROWS = 16
COLS = 256
GX = 8
XLEN = 4
ZLEN = 8
PLANE = GX * XLEN
BASE_STIFF = 0.5
FAR = 1000.0
SHIFTS = (0.8125, 0.0625, 0.8125, 0.125, 0.5)
PAIRS = [(i, j) for i in range(ITERS) for j in range(i, ITERS)]


def hops(step, length):
    return min(step, length - step)


PLANE_STEPS = sorted(
    ((dy, dx, dc) for dy in range(GX // 2) for dx in range(XLEN) for dc in range(2) if (dy, dx, dc) != (0, 0, 0)),
    key=lambda s: -(hops(s[0], GX // 2) + hops(s[1], XLEN) + 0.5 * s[2]),
)
WALL_STEPS = sorted(
    ((dy, core, dz) for dy in range(GX // 2) for core in range(2) for dz in range(ZLEN) if (dy, dz) != (0, 0)),
    key=lambda s: -(hops(s[0], GX // 2) - 0.5 * s[1] + hops(s[2], ZLEN)),
)
TOWER_STEPS = sorted(((dz, core) for dz in range(1, ZLEN) for core in range(2)), key=lambda s: -hops(s[0], ZLEN) + 0.5 * s[1])


def snake(q):
    z, x = lax.div(q, XLEN), lax.rem(q, XLEN)
    return z * XLEN + x + lax.rem(z, 2) * (XLEN - 1 - 2 * x)


def mirrored(g, a):
    y, core = lax.div(a, 2), lax.rem(a, 2)
    second = lax.div(g, COLS // GX // 2)
    return 2 * (y + lax.rem(g, 2) * (GX // 2 - 1 - 2 * y)) + core + second * (1 - 2 * core)


def two_sum(a, b):
    s = a + b
    t = s - a
    return s, (a - (s - t)) + (b - t)


def fast_two_sum(a, b):
    s = a + b
    return s, b - (s - a)


def split(a):
    c = 4097.0 * a
    high = c - (c - a)
    return high, a - high


def two_prod(a, b):
    p = a * b
    ah, al = split(a)
    bh, bl = split(b)
    return p, ((ah * bh - p) + ah * bl + al * bh) + al * bl


def pair_add(u, v):
    s, e = two_sum(u[0], v[0])
    return fast_two_sum(s, e + (u[1] + v[1]))


def pair_neg(u):
    return -u[0], -u[1]


def pair_mul(u, v):
    p, e = two_prod(u[0], v[0])
    return fast_two_sum(p, e + (u[0] * v[1] + u[1] * v[0]))


def pair_scale(u, c):
    p, e = two_prod(u[0], c)
    return fast_two_sum(p, e + u[1] * c)


def pair_div(u, v):
    q = u[0] / v[0]
    r = pair_add(u, pair_neg(pair_scale(v, q)))
    return fast_two_sum(q, r[0] / v[0])


def pair_tree(items):
    while len(items) > 1:
        items = [pair_add(*items[k : k + 2]) if k + 1 < len(items) else items[k] for k in range(0, len(items), 2)]
    return items[0]


def pair_dot(u, v):
    out = pair_mul(u, v)
    for shift in (4, 2, 1):
        out = pair_add(out, (pltpu.roll(out[0], shift, 0), pltpu.roll(out[1], shift, 0)))
    return out


def device_of(column):
    group, place = lax.div(column, GX), lax.rem(column, GX)
    return mirrored(group, place), snake(group)


def body(
    off_hbm, mass_hbm, cnt_hbm, src_hbm,
    ob, p1,
    off_ref, mass_ref, cnt_ref, src_ref,
    sbuf, inb, xcol, ycol, rcol, wts, part, rb, vb, rows_s, ub, gb,
    g1s, g1, g2s, g2, b1s, b1, b2s, b2, p1s, osb, tb,
    load_sem, in_send, in_recv, cell_send, cell_recv, rho_send, rho_recv, halo_send, halo_recv,
    red_send, red_recv, row_send, row_recv, out_send, out_recv,
):
    a, q = lax.axis_index("gx"), lax.axis_index("gy")
    z, x = lax.div(q, XLEN), lax.rem(q, XLEN)
    group = snake(q)
    place = mirrored(group, a)
    column = group * GX + place
    has_left, has_right = column > 0, column < COLS - 1
    left = device_of(jnp.maximum(column - 1, 0))
    right = device_of(jnp.minimum(column + 1, COLS - 1))
    plane_index = a * XLEN + x
    near_slot, far_slot = 2 - 2 * lax.rem(column, 2), 2 * lax.rem(column, 2)
    has_far = (column + lax.rem(column, 2) > 0) & (column + lax.rem(column, 2) < COLS)

    loads = [
        pltpu.make_async_copy(src, dst, load_sem.at[k])
        for k, (src, dst) in enumerate(
            ((off_hbm, off_ref), (mass_hbm, mass_ref), (src_hbm, src_ref), (cnt_hbm, cnt_ref))
        )
    ]
    for load in loads:
        load.start()

    barrier = pltpu.get_barrier_semaphore()

    y, core = lax.div(a, 2), lax.rem(a, 2)

    def plane_mate(step):
        dy, dx, dc = step
        return lax.rem(y + dy, GX // 2) * 2 + lax.rem(core + dc, 2), z * XLEN + lax.rem(x + dx, XLEN)

    def tower_mate(step):
        return 2 * y + step[1], lax.rem(z + step[0], ZLEN) * XLEN + x

    def wall_mate(step):
        dy, there, dz = step
        return lax.rem(y + dy, GX // 2) * 2 + there, lax.rem(z + dz, ZLEN) * XLEN + x

    def greet(target):
        pl.semaphore_signal(barrier, inc=1, device_id=target, device_id_type=MESH)

    for step in PLANE_STEPS:
        greet(plane_mate(step))
    for step in TOWER_STEPS:
        if step[1]:
            greet(tower_mate(step))
    low_edge = (lax.rem(column, PLANE) == 0) & has_left
    high_edge = (lax.rem(column, PLANE) == PLANE - 1) & has_right
    for edge, target in ((low_edge, left), (high_edge, right)):
        @pl.when(edge)
        def _(target=target):
            greet(target)

    rim = jnp.zeros((4, SLOT), F32)
    for slot in range(3):
        inb[slot, 0] = rim
        inb[slot, ROWS + 1] = rim
    wide = jnp.zeros((8, SLOT), F32)
    for slot in range(3):
        for end in (0, 24):
            rb[slot, end : end + 8, :] = wide
            for k in range(ITERS):
                vb[k, slot, end : end + 8, :] = wide
    for have, slot in ((has_left, 0), (has_right, 2)):
        @pl.when(jnp.logical_not(have))
        def _(slot=slot):
            inb[slot] = jnp.zeros((ROWS + 2, 4, SLOT), F32)
            rb[slot] = jnp.zeros((32, SLOT), F32)
            for k in range(ITERS):
                vb[k, slot] = jnp.zeros((32, SLOT), F32)

    osb[...] = jnp.zeros_like(osb)
    gb[...] = jnp.zeros_like(gb)
    part[0] = jnp.zeros((SLOT, SLOT), F32)
    for load in loads:
        load.wait()

    lane = lax.broadcasted_iota(jnp.int32, (1, SLOT), 1)
    for r in range(2):
        for c in range(GX):
            occ = jnp.where(lane < cnt_ref[r, c], 1.0, 0.0).astype(F32)
            sbuf[c, r, 0:1, :] = off_ref[0, r, c : c + 1, :]
            sbuf[c, r, 1:2, :] = off_ref[1, r, c : c + 1, :]
            sbuf[c, r, 2:3, :] = mass_ref[r, c : c + 1, :] * occ
            sbuf[c, r, 3:4, :] = src_ref[r, c : c + 1, :] * occ

    awaited = PLANE - 1 + 2 * (ZLEN - 1) * core + low_edge.astype(jnp.int32) + high_edge.astype(jnp.int32)
    pl.semaphore_wait(barrier, awaited)

    sends = []
    home = snake(q)
    for t in (4, 3, 5, 2, 6, 1, 7, 0):
        target = lax.rem(a + t, GX)
        copy = pltpu.make_async_remote_copy(
            src_ref=sbuf.at[mirrored(q, target)],
            dst_ref=inb.at[1, pl.ds(1 + 2 * a, 2)],
            send_sem=in_send.at[t],
            recv_sem=in_recv,
            device_id=(target, home),
            device_id_type=MESH,
        )
        wanted = jnp.logical_or(target != a, home != q)
        pl.when(wanted)(copy.start)
        sends.append((wanted, copy))
    local = pltpu.make_async_copy(sbuf.at[place], inb.at[1, pl.ds(1 + 2 * a, 2)], in_recv)
    pl.when(home == q)(local.start)

    def exchange(buf, first, send, recv):
        copies = []
        for k, (have, target, slot) in enumerate(((has_left, left, 2), (has_right, right, 0))):
            copy = pltpu.make_async_remote_copy(
                src_ref=buf.at[1, pl.ds(first, ROWS)],
                dst_ref=buf.at[slot, pl.ds(first, ROWS)],
                send_sem=send.at[k],
                recv_sem=recv.at[slot],
                device_id=target,
                device_id_type=MESH,
            )
            pl.when(have)(copy.start)
            copies.append((have, copy))

        def wait(slot):
            view = buf.at[slot, pl.ds(first, ROWS)]
            pltpu.make_async_copy(view, view, recv.at[slot]).wait()

        def wait_near():
            wait(near_slot)

        def wait_far():
            pl.when(has_far)(lambda: wait(far_slot))

        return wait_near, wait_far, copies

    def spread(row):
        return jnp.transpose(jnp.broadcast_to(row, (SLOT, SLOT)))

    def total_row(block):
        return jnp.sum(jnp.transpose(block), axis=0, keepdims=True)

    view = inb.at[1, pl.ds(1, ROWS)]
    pltpu.make_async_copy(view, view, in_recv).wait()
    wait_cells_near, wait_cells_far, cell_copies = exchange(inb, 1, cell_send, cell_recv)
    sends += cell_copies

    def columns(r):
        cell = inb[1, r + 1]
        fields = spread(cell[0:1]), spread(cell[1:2]), cell

        def store():
            xcol[r], ycol[r] = fields[0], fields[1]
            rows_s[0, pl.ds(r, 1), :] = cell[2:3]
            rows_s[1, pl.ds(r, 1), :] = cell[3:4]

        return store

    columns(0)()
    blocks = [(slot, dr) for slot in (1, near_slot, far_slot) for dr in (0, 1, 2)]
    side = [0.0] * 3 + [(near_slot - 1).astype(F32)] * 3 + [(far_slot - 1).astype(F32)] * 3

    def density_row(r):
        row = 1.0 + total_row(part[r])

        def store():
            rb[1, pl.ds(8 + r, 1), :] = row

        return store

    def falloffs(first, last):
        def run(r, carry):
            if first == 0:
                store_columns = columns(jnp.minimum(r + 1, ROWS - 1))
            rows = []
            for (slot, dr), step_y in zip(blocks[first:last], side[first:last]):
                cell = inb[slot, r + dr]
                mass = cell[2:3, :]
                px = (dr - 1.0) + jnp.where(mass > 0.0, cell[0:1, :], FAR)
                py = step_y + cell[1:2, :]
                rows.append((px, py, mass))
            for h in range(0, SLOT, 64):
                xi, yi = xcol[r, h : h + 64, :], ycol[r, h : h + 64, :]
                acc = jnp.zeros((64, SLOT), F32) if first == 0 else part[r, h : h + 64, :]
                for k, (px, py, mass) in enumerate(rows, first):
                    ox, oy = px - xi, py - yi
                    fall = jnp.maximum(1.0 - (ox * ox + oy * oy), 0.0)
                    square = fall * fall
                    wts[r, k, h : h + 64, :] = square
                    acc = acc + square * fall * mass
                part[r, h : h + 64, :] = acc
            if first == 0:
                store_columns()
            if last == 9:
                density_row(r)()
            return carry

        lax.fori_loop(0, ROWS, run, 0, unroll=ROWS)

    falloffs(0, 3)
    wait_cells_near()
    falloffs(3, 6)
    wait_cells_far()
    falloffs(6, 9)

    wait_rho_near, wait_rho_far, rho_copies = exchange(rb, 8, rho_send, rho_recv)
    sends += rho_copies

    def rho_columns(r, carry):
        rcol[r] = spread(10.0 * rb[1, pl.ds(8 + r, 1), :])
        return carry

    lax.fori_loop(0, ROWS, rho_columns, 0, unroll=ROWS)

    def weights(first, last):
        def run(r, carry):
            rows = [10.0 * rb[slot, pl.ds(7 + r + dr, 1), :] for slot, dr in blocks[first:last]]
            for h in range(0, SLOT, 64):
                ri = rcol[r, h : h + 64, :]
                acc = jnp.zeros((64, SLOT), F32) if first == 0 else part[r, h : h + 64, :]
                for k, row in enumerate(rows, first):
                    w = wts[r, k, h : h + 64, :] / (ri + row)
                    wts[r, k, h : h + 64, :] = w
                    acc = acc + w
                part[r, h : h + 64, :] = acc
            if last == 9:
                ub[pl.ds(r, 1), :] = BASE_STIFF + total_row(part[r])
            return carry

        lax.fori_loop(0, ROWS, run, 0, unroll=ROWS if last == 9 else 4)

    weights(0, 3)
    wait_rho_near()
    weights(3, 6)
    wait_rho_far()
    weights(6, 9)

    occ = jnp.where(rows_s[0] > 0.0, 1.0, 0.0).astype(F32)
    diag = ub[...]
    dinv = occ / diag
    basis = [rows_s[1] * dinv]
    gram_rows = {}
    sub8 = lax.broadcasted_iota(jnp.int32, (8, SLOT), 0)
    lane8 = lax.broadcasted_iota(jnp.int32, (8, SLOT), 1)

    def sublane_sum(block):
        out = two_sum(block[:64], block[64:])
        for size in (32, 16, 8, 4, 2, 1):
            out = pair_add((out[0][:size], out[1][:size]), (out[0][size:], out[1][size:]))
        return out

    def lane_sum(row):
        return sublane_sum(spread(row))

    def pairs_of(refs, count):
        return pair_tree([(refs[k, 0:1, :], refs[k, 1:2, :]) for k in range(count)])

    def gather(rows, own, all_refs, mate, steps, index, send_sem, recv_sem, spare=None):
        for k, row in enumerate(rows):
            own[0, k : k + 1, :] = row

        def send():
            for step in steps:
                pltpu.make_async_remote_copy(
                    src_ref=own.at[0],
                    dst_ref=all_refs.at[index],
                    send_sem=send_sem,
                    recv_sem=recv_sem,
                    device_id=mate(step),
                    device_id_type=MESH,
                ).start()

        def wait_sent():
            source = all_refs if spare is None else spare
            for start in range(0, len(steps), PLANE - 1):
                view = source.at[pl.ds(0, min(PLANE - 1, len(steps) - start))]
                pltpu.make_async_copy(view, view, send_sem).wait()

        if spare is None:
            send()
        else:
            pl.when(core == 1)(send)
        by_copy = all_refs is p1
        if by_copy:
            pltpu.make_async_copy(own.at[0], all_refs.at[index], recv_sem).start()
        else:
            for k, row in enumerate(rows):
                all_refs[index, k : k + 1, :] = row

        def wait():
            view = all_refs.at[pl.ds(0, all_refs.shape[0] - 1 + by_copy)]
            pltpu.make_async_copy(view, view, recv_sem).wait()

        return wait, (wait_sent if spare is None else lambda: pl.when(core == 1)(wait_sent))


    def replicate(k):
        here = 2 * x + core
        tb[k, here] = basis[k] * diag
        for dx, dc in ((2, 1), (2, 0), (1, 1), (3, 1), (1, 0), (3, 0), (0, 1)):
            pltpu.make_async_remote_copy(
                src_ref=tb.at[k, here],
                dst_ref=tb.at[k, here],
                send_sem=row_send.at[k],
                recv_sem=row_recv.at[k],
                device_id=(2 * y + lax.rem(core + dc, 2), z * XLEN + lax.rem(x + dx, XLEN)),
                device_id_type=MESH,
            ).start()

    def wait_replicas(k, sem):
        view = tb.at[k, pl.ds(0, 2 * XLEN - 1)]
        pltpu.make_async_copy(view, view, sem.at[k]).wait()

    for k in range(ITERS):
        vb[k, 1, pl.ds(8, ROWS), :] = basis[k]
        wait_near, wait_far, halo_copies = exchange(vb.at[k], 8, halo_send.at[k], halo_recv.at[k])
        sends += halo_copies

        def apply_own(r, carry):
            acc = wts[r, 0] * vb[k, 1, pl.ds(7 + r, 1), :]
            for m in (1, 2):
                acc = acc + wts[r, m] * vb[k, 1, pl.ds(7 + r + m, 1), :]
            part[r] = acc
            return carry

        lax.fori_loop(0, ROWS, apply_own, 0, unroll=4)
        replicate(k)
        scaled = basis[k] * diag
        for i in range(k + 1):
            gram_rows[i, k] = jnp.sum(basis[i] * scaled, axis=0, keepdims=True)
        if k == ITERS - 1:
            for i, j in PAIRS:
                gb[8 * j + i : 8 * j + i + 1, :] = gram_rows[i, j]
                if i != j:
                    gb[8 * i + j : 8 * i + j + 1, :] = gram_rows[i, j]
            gram_sum = sublane_sum(jnp.transpose(gb[...]))
            wait_plane, sent_plane = gather(
                gram_sum, g1s, g1, plane_mate, PLANE_STEPS, plane_index, red_send.at[0], red_recv.at[0]
            )
        wait_near()

        def apply_near(r, carry):
            acc = part[r]
            for m in range(3, 6):
                slot, dr = blocks[m]
                acc = acc + wts[r, m] * vb[k, slot, pl.ds(7 + r + dr, 1), :]
            part[r] = acc
            return carry

        lax.fori_loop(0, ROWS, apply_near, 0, unroll=4)
        wait_far()

        def apply_far(r, carry):
            acc = part[r]
            for m in range(6, 9):
                slot, dr = blocks[m]
                acc = acc + wts[r, m] * vb[k, slot, pl.ds(7 + r + dr, 1), :]
            ub[pl.ds(r, 1), :] = total_row(acc)
            return carry

        lax.fori_loop(0, ROWS, apply_far, 0, unroll=ROWS)
        basis.append(2.0 * (ub[...] * dinv - SHIFTS[k] * basis[k]))

    last_sum = lane_sum(jnp.sum(basis[ITERS - 1] * ub[...], axis=0, keepdims=True))
    wait_last_plane, sent_last_plane = gather(
        last_sum, b1s, b1, plane_mate, PLANE_STEPS, plane_index, red_send.at[4], red_recv.at[4]
    )
    replicate(ITERS)
    wait_plane()
    plane_sum = pairs_of(g1, PLANE)
    wait_tower, sent_tower = gather(plane_sum, g2s, g2, tower_mate, TOWER_STEPS, z, red_send.at[1], red_recv.at[1], g1)
    wait_last_plane()
    last_plane_sum = pairs_of(b1, PLANE)
    wait_last_tower, sent_last_tower = gather(
        last_plane_sum, b2s, b2, tower_mate, TOWER_STEPS, z, red_send.at[5], red_recv.at[5], b1
    )
    wait_tower()
    total = pairs_of(g2, ZLEN)
    high, low = spread(total[0]), spread(total[1])
    gram = [(high[8 * j : 8 * j + 8], low[8 * j : 8 * j + 8]) for j in range(ITERS)]

    zero = jnp.zeros((8, SLOT), F32)
    first = jnp.where(sub8 == 0, 1.0, 0.0).astype(F32)
    keep = zero
    for k, shift in enumerate(SHIFTS):
        keep = jnp.where(sub8 == k, 1.0 - shift, keep)

    def part_of(u, k):
        return tuple(jnp.broadcast_to(w[k : k + 1], (8, SLOT)) for w in u)

    shifted = zero
    for k, shift in enumerate(SHIFTS[:-1]):
        shifted = jnp.where(sub8 == k, 2.0 * (shift - SHIFTS[-1]), shifted)
    following = tuple(pltpu.roll(w, 7, 0) for w in gram[ITERS - 1])
    newest = pair_add(following, pair_scale(gram[ITERS - 1], shifted))
    gram.append(tuple(jnp.where(sub8 < ITERS - 1, w, 0.0) for w in newest))

    solution_at, residual_at, direction = (zero, zero), (first, zero), (first, zero)
    residual_image = gram[0]
    residuals = []
    rz = part_of(gram[0], 0)
    for k in range(ITERS):
        moved = tuple(-0.5 * pltpu.roll(w, 1, 0) for w in direction)
        image = pair_add(pair_scale(direction, keep), moved)
        gram_image = pair_tree([pair_mul(gram[j], part_of(image, j)) for j in range(k + 2)])
        curvature = pair_dot(direction, gram_image)
        if k + 1 < ITERS:
            step = pair_div(rz, curvature)
            solution_at = pair_add(solution_at, pair_mul(step, direction))
            residual_at = pair_add(residual_at, pair_neg(pair_mul(step, image)))
            residuals.append(residual_at[0])
            residual_image = pair_add(residual_image, pair_neg(pair_mul(step, gram_image)))
            new = pair_dot(residual_at, residual_image)
            direction = pair_add(residual_at, pair_mul(pair_div(new, rz), direction))
            rz = new
    corner = pair_mul(part_of(direction, ITERS - 1), part_of(image, ITERS))
    corner = tuple(2.0 * w for w in corner)
    curvature = pair_add(
        curvature, pair_mul(corner, pair_scale(part_of(gram[ITERS - 1], ITERS - 1), -SHIFTS[-1]))
    )

    def combine(factors, count):
        out = None
        for j in range(count):
            term = factors[j : j + 1] * basis[j]
            out = term if out is None else out + term
        return out

    field = combine(residuals[-1], ITERS) * diag
    drop = combine(image[0], ITERS + 1) * diag
    pressure = combine(solution_at[0], ITERS - 1)
    along = combine(direction[0], ITERS)
    for k in range(ITERS + 1):
        wait_replicas(k, row_recv)

    def row_combine(factors, count, t):
        out = None
        for j in range(count):
            term = factors[j : j + 1] * tb[j, t]
            out = term if out is None else out + term
        return out

    gb[0:8, :] = jnp.zeros((8, SLOT), F32)
    peaks = [None] * ITERS

    def raise_peak(k, values):
        values = jnp.abs(values)
        peaks[k] = values if peaks[k] is None else jnp.maximum(peaks[k], values)

    row_fields = []
    for t in range(2 * XLEN):
        for k in range(ITERS - 1):
            values = row_combine(residuals[k], k + 2, t)
            raise_peak(k, values)
        row_fields.append((values, row_combine(image[0], ITERS + 1, t)))
    for k in range(ITERS - 1):
        gb[k : k + 1, :] = jnp.max(peaks[k], axis=0, keepdims=True)
    wait_last_tower()
    last = tuple(jnp.broadcast_to(w, (8, SLOT)) for w in pairs_of(b2, ZLEN))
    step = pair_div(rz, pair_add(curvature, pair_mul(corner, last)))[0][0:1]
    pressure = pressure + step * along
    field = field - step * drop
    for values, change in row_fields:
        raise_peak(ITERS - 1, values - step * change)
    gb[ITERS - 1 : ITERS, :] = jnp.max(peaks[ITERS - 1], axis=0, keepdims=True)
    peak = jnp.max(gb[0:8, :], axis=1, keepdims=True)
    peak_row = jnp.sum(jnp.where(sub8 == lane8, peak, 0.0), axis=0, keepdims=True)
    wait_peaks, sent_peaks = gather(
        [peak_row], p1s, p1, wall_mate, WALL_STEPS, y * ZLEN + z, red_send.at[2], red_recv.at[2], p1
    )

    density = rb[1, pl.ds(8, ROWS), :]
    for r in range(ROWS):
        osb[r, 0:1, :] = density[r : r + 1, :]
        osb[r, 1:2, :] = pressure[r : r + 1, :]
        osb[r, 2:3, :] = field[r : r + 1, :]
    for k in range(GX):
        wanted = jnp.logical_or(a != k, group != q)
        copy = pltpu.make_async_remote_copy(
            src_ref=osb.at[pl.ds(2 * k, 2)],
            dst_ref=ob.at[place],
            send_sem=out_send.at[k],
            recv_sem=out_recv,
            device_id=(k, group),
            device_id_type=MESH,
        )
        pl.when(wanted)(copy.start)
        sends.append((wanted, copy))
    local = pltpu.make_async_copy(osb.at[pl.ds(2 * a, 2)], ob.at[place], out_recv)
    pl.when(group == q)(local.start)

    wait_peaks()
    pltpu.make_async_copy(ob, ob, out_recv).wait()

    for wanted, copy in sends:
        pl.when(wanted)(copy.wait_send)
    for wait in (sent_plane, sent_tower, sent_last_plane, sent_last_tower, sent_peaks):
        wait()
    for k in range(ITERS + 1):
        wait_replicas(k, row_send)


def finish(ob, p1, dens_ref, pres_ref, resid_ref, peaks_ref):
    for r in range(2):
        for c in range(GX):
            dens_ref[r, c : c + 1, :] = ob[c, r, 0:1, :]
            pres_ref[r, c : c + 1, :] = ob[c, r, 1:2, :]
            resid_ref[r, c : c + 1, :] = ob[c, r, 2:3, :]
    peaks_ref[...] = jnp.max(p1[...], axis=0)[0, :ITERS]


def shard(offsets, masses, counts, source):
    block = jax.ShapeDtypeStruct((2, GX, SLOT), F32)
    vmem = pl.BlockSpec(memory_space=pltpu.VMEM)
    dma = pltpu.SemaphoreType.DMA
    cells = (ROWS, SLOT, SLOT)
    gathered, peaks = pl.pallas_call(
        body,
        out_shape=(
            pltpu.VMEM((GX, 2, 4, SLOT), F32),
            pltpu.VMEM((GX // 2 * ZLEN, 1, SLOT), F32),
        ),
        in_specs=[pl.BlockSpec(memory_space=pl.ANY)] * 4,
        out_specs=(pl.BlockSpec(memory_space=pl.ANY),) * 2,
        scratch_shapes=[
            pltpu.VMEM((2, 2, GX, SLOT), F32),
            pltpu.VMEM((2, GX, SLOT), F32),
            pltpu.SMEM((2, GX), jnp.int32),
            pltpu.VMEM((2, GX, SLOT), F32),
            pltpu.VMEM((GX, 2, 4, SLOT), F32),
            pltpu.VMEM((3, ROWS + 2, 4, SLOT), F32),
            pltpu.VMEM(cells, F32),
            pltpu.VMEM(cells, F32),
            pltpu.VMEM(cells, F32),
            pltpu.VMEM((ROWS, 9, SLOT, SLOT), F32),
            pltpu.VMEM(cells, F32),
            pltpu.VMEM((3, 32, SLOT), F32),
            pltpu.VMEM((ITERS, 3, 32, SLOT), F32),
            pltpu.VMEM((2, ROWS, SLOT), F32),
            pltpu.VMEM((ROWS, SLOT), F32),
            pltpu.VMEM((SLOT, SLOT), F32),
            pltpu.VMEM((1, 2, SLOT), F32),
            pltpu.VMEM((PLANE, 2, SLOT), F32),
            pltpu.VMEM((1, 2, SLOT), F32),
            pltpu.VMEM((ZLEN, 2, SLOT), F32),
            pltpu.VMEM((1, 2, SLOT), F32),
            pltpu.VMEM((PLANE, 2, SLOT), F32),
            pltpu.VMEM((1, 2, SLOT), F32),
            pltpu.VMEM((ZLEN, 2, SLOT), F32),
            pltpu.VMEM((1, 1, SLOT), F32),
            pltpu.VMEM((ROWS, 4, SLOT), F32),
            pltpu.VMEM((ITERS + 1, 2 * XLEN, ROWS, SLOT), F32),
            dma((4,)),
            dma((GX,)),
            dma,
            dma((2,)),
            dma((3,)),
            dma((2,)),
            dma((3,)),
            dma((ITERS, 2)),
            dma((ITERS, 3)),
            dma((6,)),
            dma((6,)),
            dma((ITERS + 1,)),
            dma((ITERS + 1,)),
            dma((GX,)),
            dma,
        ],
        compiler_params=pltpu.CompilerParams(collective_id=0, has_side_effects=True),
    )(offsets, masses, counts, source)
    return pl.pallas_call(
        finish,
        out_shape=(block, block, block, jax.ShapeDtypeStruct((ITERS,), F32)),
        in_specs=[vmem, vmem],
        out_specs=(vmem, vmem, vmem, vmem),
    )(*(pltpu.with_memory_space_constraint(u, pltpu.VMEM) for u in (gathered, peaks)))


def solution(mesh):
    return jax.shard_map(
        shard,
        mesh=mesh,
        in_specs=(P(None, "gx", "gy", None), P("gx", "gy", None), P("gx", "gy"), P("gx", "gy", None)),
        out_specs=(P("gx", "gy", None), P("gx", "gy", None), P("gx", "gy", None), P()),
        check_vma=False,
    )
```

```python
import jax
import jax.numpy as jnp
from jax import lax
from jax.experimental import pallas as pl
from jax.experimental.pallas import tpu as pltpu
from jax.sharding import PartitionSpec as P

MESH = pl.DeviceIdType.MESH
F32 = jnp.float32

ITERS = 5
SLOT = 128
ROWS = 16
COLS = 256
GX = 8
XLEN = 4
ZLEN = 8
PLANE = GX * XLEN
BASE_STIFF = 0.5
FAR = 1000.0
SHIFTS = (0.8125, 0.0625, 0.8125, 0.125, 0.5)
PAIRS = [(i, j) for i in range(ITERS) for j in range(i, ITERS)]


def hops(step, length):
    return min(step, length - step)


PLANE_STEPS = sorted(
    ((dy, dx, dc) for dy in range(GX // 2) for dx in range(XLEN) for dc in range(2) if (dy, dx, dc) != (0, 0, 0)),
    key=lambda s: -(hops(s[0], GX // 2) + hops(s[1], XLEN) + 0.5 * s[2]),
)
WALL_STEPS = sorted(
    ((dy, core, dz) for dy in range(GX // 2) for core in range(2) for dz in range(ZLEN) if (dy, dz) != (0, 0)),
    key=lambda s: -(hops(s[0], GX // 2) - 0.5 * s[1] + hops(s[2], ZLEN)),
)
TOWER_STEPS = sorted(((dz, core) for dz in range(1, ZLEN) for core in range(2)), key=lambda s: -hops(s[0], ZLEN) + 0.5 * s[1])


def snake(q):
    z, x = lax.div(q, XLEN), lax.rem(q, XLEN)
    return z * XLEN + x + lax.rem(z, 2) * (XLEN - 1 - 2 * x)


def mirrored(g, a):
    y, core = lax.div(a, 2), lax.rem(a, 2)
    second = lax.div(g, COLS // GX // 2)
    return 2 * (y + lax.rem(g, 2) * (GX // 2 - 1 - 2 * y)) + core + second * (1 - 2 * core)


def two_sum(a, b):
    s = a + b
    t = s - a
    return s, (a - (s - t)) + (b - t)


def fast_two_sum(a, b):
    s = a + b
    return s, b - (s - a)


def split(a):
    c = 4097.0 * a
    high = c - (c - a)
    return high, a - high


def two_prod(a, b):
    p = a * b
    ah, al = split(a)
    bh, bl = split(b)
    return p, ((ah * bh - p) + ah * bl + al * bh) + al * bl


def pair_add(u, v):
    s, e = two_sum(u[0], v[0])
    return fast_two_sum(s, e + (u[1] + v[1]))


def pair_neg(u):
    return -u[0], -u[1]


def pair_mul(u, v):
    p, e = two_prod(u[0], v[0])
    return fast_two_sum(p, e + (u[0] * v[1] + u[1] * v[0]))


def pair_scale(u, c):
    p, e = two_prod(u[0], c)
    return fast_two_sum(p, e + u[1] * c)


def pair_div(u, v):
    q = u[0] / v[0]
    r = pair_add(u, pair_neg(pair_scale(v, q)))
    return fast_two_sum(q, r[0] / v[0])


def pair_tree(items):
    while len(items) > 1:
        items = [pair_add(*items[k : k + 2]) if k + 1 < len(items) else items[k] for k in range(0, len(items), 2)]
    return items[0]


def pair_dot(u, v):
    out = pair_mul(u, v)
    for shift in (4, 2, 1):
        out = pair_add(out, (pltpu.roll(out[0], shift, 0), pltpu.roll(out[1], shift, 0)))
    return out


def device_of(column):
    group, place = lax.div(column, GX), lax.rem(column, GX)
    return mirrored(group, place), snake(group)


def body(
    off_hbm, mass_hbm, cnt_hbm, src_hbm,
    ob, p1,
    off_ref, mass_ref, cnt_ref, src_ref,
    sbuf, inb, xcol, ycol, rcol, wts, part, rb, vb, rows_s, ub, gb,
    g1s, g1, g2s, g2, b1s, b1, b2s, b2, p1s, osb, tb,
    load_sem, in_send, in_recv, cell_send, cell_recv, rho_send, rho_recv, halo_send, halo_recv,
    red_send, red_recv, row_send, row_recv, out_send, out_recv,
):
    a, q = lax.axis_index("gx"), lax.axis_index("gy")
    z, x = lax.div(q, XLEN), lax.rem(q, XLEN)
    group = snake(q)
    place = mirrored(group, a)
    column = group * GX + place
    has_left, has_right = column > 0, column < COLS - 1
    left = device_of(jnp.maximum(column - 1, 0))
    right = device_of(jnp.minimum(column + 1, COLS - 1))
    plane_index = a * XLEN + x
    near_slot, far_slot = 2 - 2 * lax.rem(column, 2), 2 * lax.rem(column, 2)
    has_far = (column + lax.rem(column, 2) > 0) & (column + lax.rem(column, 2) < COLS)

    loads = [
        pltpu.make_async_copy(src, dst, load_sem.at[k])
        for k, (src, dst) in enumerate(
            ((off_hbm, off_ref), (mass_hbm, mass_ref), (src_hbm, src_ref), (cnt_hbm, cnt_ref))
        )
    ]
    for load in loads:
        load.start()

    barrier = pltpu.get_barrier_semaphore()

    y, core = lax.div(a, 2), lax.rem(a, 2)

    def plane_mate(step):
        dy, dx, dc = step
        return lax.rem(y + dy, GX // 2) * 2 + lax.rem(core + dc, 2), z * XLEN + lax.rem(x + dx, XLEN)

    def tower_mate(step):
        return 2 * y + step[1], lax.rem(z + step[0], ZLEN) * XLEN + x

    def wall_mate(step):
        dy, there, dz = step
        return lax.rem(y + dy, GX // 2) * 2 + there, lax.rem(z + dz, ZLEN) * XLEN + x

    def greet(target):
        pl.semaphore_signal(barrier, inc=1, device_id=target, device_id_type=MESH)

    for step in PLANE_STEPS:
        greet(plane_mate(step))
    for step in TOWER_STEPS:
        if step[1]:
            greet(tower_mate(step))
    low_edge = (lax.rem(column, PLANE) == 0) & has_left
    high_edge = (lax.rem(column, PLANE) == PLANE - 1) & has_right
    for edge, target in ((low_edge, left), (high_edge, right)):
        @pl.when(edge)
        def _(target=target):
            greet(target)

    rim = jnp.zeros((4, SLOT), F32)
    for slot in range(3):
        inb[slot, 0] = rim
        inb[slot, ROWS + 1] = rim
    wide = jnp.zeros((8, SLOT), F32)
    for slot in range(3):
        for end in (0, 24):
            rb[slot, end : end + 8, :] = wide
            for k in range(ITERS):
                vb[k, slot, end : end + 8, :] = wide
    for have, slot in ((has_left, 0), (has_right, 2)):
        @pl.when(jnp.logical_not(have))
        def _(slot=slot):
            inb[slot] = jnp.zeros((ROWS + 2, 4, SLOT), F32)
            rb[slot] = jnp.zeros((32, SLOT), F32)
            for k in range(ITERS):
                vb[k, slot] = jnp.zeros((32, SLOT), F32)

    osb[...] = jnp.zeros_like(osb)
    gb[...] = jnp.zeros_like(gb)
    part[0] = jnp.zeros((SLOT, SLOT), F32)
    for load in loads:
        load.wait()

    lane = lax.broadcasted_iota(jnp.int32, (1, SLOT), 1)
    for r in range(2):
        for c in range(GX):
            occ = jnp.where(lane < cnt_ref[r, c], 1.0, 0.0).astype(F32)
            sbuf[c, r, 0:1, :] = off_ref[0, r, c : c + 1, :]
            sbuf[c, r, 1:2, :] = off_ref[1, r, c : c + 1, :]
            sbuf[c, r, 2:3, :] = mass_ref[r, c : c + 1, :] * occ
            sbuf[c, r, 3:4, :] = src_ref[r, c : c + 1, :] * occ

    awaited = PLANE - 1 + 2 * (ZLEN - 1) * core + low_edge.astype(jnp.int32) + high_edge.astype(jnp.int32)
    pl.semaphore_wait(barrier, awaited)

    sends = []
    home = snake(q)
    for t in (4, 3, 5, 2, 6, 1, 7, 0):
        target = lax.rem(a + t, GX)
        copy = pltpu.make_async_remote_copy(
            src_ref=sbuf.at[mirrored(q, target)],
            dst_ref=inb.at[1, pl.ds(1 + 2 * a, 2)],
            send_sem=in_send,
            recv_sem=in_recv,
            device_id=(target, home),
            device_id_type=MESH,
        )
        wanted = jnp.logical_or(target != a, home != q)
        pl.when(wanted)(copy.start)
    local = pltpu.make_async_copy(sbuf.at[place], inb.at[1, pl.ds(1 + 2 * a, 2)], in_recv)
    pl.when(home == q)(local.start)

    def exchange(buf, first, send, recv):
        for have, target, slot in ((has_left, left, 2), (has_right, right, 0)):
            copy = pltpu.make_async_remote_copy(
                src_ref=buf.at[1, pl.ds(first, ROWS)],
                dst_ref=buf.at[slot, pl.ds(first, ROWS)],
                send_sem=send,
                recv_sem=recv.at[slot // 2],
                device_id=target,
                device_id_type=MESH,
            )
            pl.when(have)(copy.start)

        def wait(slot):
            view = buf.at[slot, pl.ds(first, ROWS)]
            pltpu.make_async_copy(view, view, recv.at[lax.div(slot, 2)]).wait()

        def wait_near():
            wait(near_slot)

        def wait_far():
            pl.when(has_far)(lambda: wait(far_slot))

        def wait_sent():
            one, both = buf.at[1, pl.ds(first, ROWS)], buf.at[pl.ds(0, 2), pl.ds(first, ROWS)]
            inner = has_left & has_right
            pl.when(inner)(pltpu.make_async_copy(both, both, send).wait)
            pl.when(jnp.logical_not(inner))(pltpu.make_async_copy(one, one, send).wait)

        return wait_near, wait_far, wait_sent

    def spread(row):
        return jnp.transpose(jnp.broadcast_to(row, (SLOT, SLOT)))

    def total_row(block):
        return jnp.sum(jnp.transpose(block), axis=0, keepdims=True)

    view = inb.at[1, pl.ds(1, ROWS)]
    pltpu.make_async_copy(view, view, in_recv).wait()
    wait_cells_near, wait_cells_far, cells_sent = exchange(inb, 1, cell_send, cell_recv)
    sends.append(cells_sent)

    def columns(r):
        cell = inb[1, r + 1]
        fields = spread(cell[0:1]), spread(cell[1:2]), cell

        def store():
            xcol[r], ycol[r] = fields[0], fields[1]
            rows_s[0, pl.ds(r, 1), :] = cell[2:3]
            rows_s[1, pl.ds(r, 1), :] = cell[3:4]

        return store

    columns(0)()
    blocks = [(slot, dr) for slot in (1, near_slot, far_slot) for dr in (0, 1, 2)]
    side = [0.0] * 3 + [(near_slot - 1).astype(F32)] * 3 + [(far_slot - 1).astype(F32)] * 3

    def density_row(r):
        row = 1.0 + total_row(part[r])

        def store():
            rb[1, pl.ds(8 + r, 1), :] = row

        return store

    def falloffs(first, last):
        def run(r, carry):
            if first == 0:
                store_columns = columns(jnp.minimum(r + 1, ROWS - 1))
            rows = []
            for (slot, dr), step_y in zip(blocks[first:last], side[first:last]):
                cell = inb[slot, r + dr]
                mass = cell[2:3, :]
                px = (dr - 1.0) + jnp.where(mass > 0.0, cell[0:1, :], FAR)
                py = step_y + cell[1:2, :]
                rows.append((px, py, mass))
            for h in range(0, SLOT, 64):
                xi, yi = xcol[r, h : h + 64, :], ycol[r, h : h + 64, :]
                acc = jnp.zeros((64, SLOT), F32) if first == 0 else part[r, h : h + 64, :]
                for k, (px, py, mass) in enumerate(rows, first):
                    ox, oy = px - xi, py - yi
                    fall = jnp.maximum(1.0 - (ox * ox + oy * oy), 0.0)
                    square = fall * fall
                    wts[r, k, h : h + 64, :] = square
                    acc = acc + square * fall * mass
                part[r, h : h + 64, :] = acc
            if first == 0:
                store_columns()
            if last == 9:
                density_row(r)()
            return carry

        lax.fori_loop(0, ROWS, run, 0, unroll=ROWS)

    falloffs(0, 3)
    wait_cells_near()
    falloffs(3, 6)
    wait_cells_far()
    falloffs(6, 9)

    wait_rho_near, wait_rho_far, rho_sent = exchange(rb, 8, rho_send, rho_recv)
    sends.append(rho_sent)

    def rho_columns(r, carry):
        rcol[r] = spread(10.0 * rb[1, pl.ds(8 + r, 1), :])
        return carry

    lax.fori_loop(0, ROWS, rho_columns, 0, unroll=ROWS)

    def weights(first, last):
        def run(r, carry):
            rows = [10.0 * rb[slot, pl.ds(7 + r + dr, 1), :] for slot, dr in blocks[first:last]]
            for h in range(0, SLOT, 64):
                ri = rcol[r, h : h + 64, :]
                acc = jnp.zeros((64, SLOT), F32) if first == 0 else part[r, h : h + 64, :]
                for k, row in enumerate(rows, first):
                    w = wts[r, k, h : h + 64, :] / (ri + row)
                    wts[r, k, h : h + 64, :] = w
                    acc = acc + w
                part[r, h : h + 64, :] = acc
            if last == 9:
                ub[pl.ds(r, 1), :] = BASE_STIFF + total_row(part[r])
            return carry

        lax.fori_loop(0, ROWS, run, 0, unroll=ROWS if last == 9 else 4)

    weights(0, 3)
    wait_rho_near()
    weights(3, 6)
    wait_rho_far()
    weights(6, 9)

    occ = jnp.where(rows_s[0] > 0.0, 1.0, 0.0).astype(F32)
    diag = ub[...]
    dinv = occ / diag
    basis = [rows_s[1] * dinv]
    gram_rows = {}
    sub8 = lax.broadcasted_iota(jnp.int32, (8, SLOT), 0)
    lane8 = lax.broadcasted_iota(jnp.int32, (8, SLOT), 1)

    def sublane_sum(block):
        out = two_sum(block[:64], block[64:])
        for size in (32, 16, 8, 4, 2, 1):
            out = pair_add((out[0][:size], out[1][:size]), (out[0][size:], out[1][size:]))
        return out

    def lane_sum(row):
        return sublane_sum(spread(row))

    def pairs_of(refs, count):
        return pair_tree([(refs[k, 0:1, :], refs[k, 1:2, :]) for k in range(count)])

    def gather(rows, own, all_refs, mate, steps, index, recv_sem, everyone):
        for k, row in enumerate(rows):
            own[0, k : k + 1, :] = row

        def send():
            for step in steps:
                pltpu.make_async_remote_copy(
                    src_ref=own.at[0],
                    dst_ref=all_refs.at[index],
                    send_sem=red_send,
                    recv_sem=recv_sem,
                    device_id=mate(step),
                    device_id_type=MESH,
                ).start()

        if everyone:
            send()
        else:
            pl.when(core == 1)(send)
        by_copy = all_refs is p1
        if by_copy:
            pltpu.make_async_copy(own.at[0], all_refs.at[index], recv_sem).start()
        else:
            for k, row in enumerate(rows):
                all_refs[index, k : k + 1, :] = row

        def wait():
            view = all_refs.at[pl.ds(0, all_refs.shape[0] - 1 + by_copy)]
            pltpu.make_async_copy(view, view, recv_sem).wait()

        return wait


    def replicate(k):
        here = 2 * x + core
        tb[k, here] = basis[k] * diag
        for dx, dc in ((2, 1), (2, 0), (1, 1), (3, 1), (1, 0), (3, 0), (0, 1)):
            pltpu.make_async_remote_copy(
                src_ref=tb.at[k, here],
                dst_ref=tb.at[k, here],
                send_sem=row_send,
                recv_sem=row_recv,
                device_id=(2 * y + lax.rem(core + dc, 2), z * XLEN + lax.rem(x + dx, XLEN)),
                device_id_type=MESH,
            ).start()

    def wait_replicas(sem):
        view = tb.at[:, pl.ds(0, 2 * XLEN - 1)]
        pltpu.make_async_copy(view, view, sem).wait()

    for k in range(ITERS):
        vb[k, 1, pl.ds(8, ROWS), :] = basis[k]
        wait_near, wait_far, halo_sent = exchange(vb.at[k], 8, halo_send.at[k], halo_recv.at[k])
        sends.append(halo_sent)

        def apply_own(r, carry):
            acc = wts[r, 0] * vb[k, 1, pl.ds(7 + r, 1), :]
            for m in (1, 2):
                acc = acc + wts[r, m] * vb[k, 1, pl.ds(7 + r + m, 1), :]
            part[r] = acc
            return carry

        lax.fori_loop(0, ROWS, apply_own, 0, unroll=4)
        replicate(k)
        scaled = basis[k] * diag
        for i in range(k + 1):
            gram_rows[i, k] = jnp.sum(basis[i] * scaled, axis=0, keepdims=True)
        if k == ITERS - 1:
            for i, j in PAIRS:
                gb[8 * j + i : 8 * j + i + 1, :] = gram_rows[i, j]
                if i != j:
                    gb[8 * i + j : 8 * i + j + 1, :] = gram_rows[i, j]
            gram_sum = sublane_sum(jnp.transpose(gb[...]))
            wait_plane = gather(
                gram_sum, g1s, g1, plane_mate, PLANE_STEPS, plane_index, red_recv.at[0], True
            )
        wait_near()

        def apply_near(r, carry):
            acc = part[r]
            for m in range(3, 6):
                slot, dr = blocks[m]
                acc = acc + wts[r, m] * vb[k, slot, pl.ds(7 + r + dr, 1), :]
            part[r] = acc
            return carry

        lax.fori_loop(0, ROWS, apply_near, 0, unroll=4)
        wait_far()

        def apply_far(r, carry):
            acc = part[r]
            for m in range(6, 9):
                slot, dr = blocks[m]
                acc = acc + wts[r, m] * vb[k, slot, pl.ds(7 + r + dr, 1), :]
            ub[pl.ds(r, 1), :] = total_row(acc)
            return carry

        lax.fori_loop(0, ROWS, apply_far, 0, unroll=ROWS)
        basis.append(2.0 * (ub[...] * dinv - SHIFTS[k] * basis[k]))

    last_sum = lane_sum(jnp.sum(basis[ITERS - 1] * ub[...], axis=0, keepdims=True))
    wait_last_plane = gather(
        last_sum, b1s, b1, plane_mate, PLANE_STEPS, plane_index, red_recv.at[3], True
    )
    replicate(ITERS)
    wait_plane()
    plane_sum = pairs_of(g1, PLANE)
    wait_tower = gather(plane_sum, g2s, g2, tower_mate, TOWER_STEPS, z, red_recv.at[1], False)
    wait_last_plane()
    last_plane_sum = pairs_of(b1, PLANE)
    wait_last_tower = gather(
        last_plane_sum, b2s, b2, tower_mate, TOWER_STEPS, z, red_recv.at[4], False
    )
    wait_tower()
    total = pairs_of(g2, ZLEN)
    high, low = spread(total[0]), spread(total[1])
    gram = [(high[8 * j : 8 * j + 8], low[8 * j : 8 * j + 8]) for j in range(ITERS)]

    zero = jnp.zeros((8, SLOT), F32)
    first = jnp.where(sub8 == 0, 1.0, 0.0).astype(F32)
    keep = zero
    for k, shift in enumerate(SHIFTS):
        keep = jnp.where(sub8 == k, 1.0 - shift, keep)

    def part_of(u, k):
        return tuple(jnp.broadcast_to(w[k : k + 1], (8, SLOT)) for w in u)

    shifted = zero
    for k, shift in enumerate(SHIFTS[:-1]):
        shifted = jnp.where(sub8 == k, 2.0 * (shift - SHIFTS[-1]), shifted)
    following = tuple(pltpu.roll(w, 7, 0) for w in gram[ITERS - 1])
    newest = pair_add(following, pair_scale(gram[ITERS - 1], shifted))
    gram.append(tuple(jnp.where(sub8 < ITERS - 1, w, 0.0) for w in newest))

    solution_at, residual_at, direction = (zero, zero), (first, zero), (first, zero)
    residual_image = gram[0]
    residuals = []
    rz = part_of(gram[0], 0)
    for k in range(ITERS):
        moved = tuple(-0.5 * pltpu.roll(w, 1, 0) for w in direction)
        image = pair_add(pair_scale(direction, keep), moved)
        gram_image = pair_tree([pair_mul(gram[j], part_of(image, j)) for j in range(k + 2)])
        curvature = pair_dot(direction, gram_image)
        if k + 1 < ITERS:
            step = pair_div(rz, curvature)
            solution_at = pair_add(solution_at, pair_mul(step, direction))
            residual_at = pair_add(residual_at, pair_neg(pair_mul(step, image)))
            residuals.append(residual_at[0])
            residual_image = pair_add(residual_image, pair_neg(pair_mul(step, gram_image)))
            new = pair_dot(residual_at, residual_image)
            direction = pair_add(residual_at, pair_mul(pair_div(new, rz), direction))
            rz = new
    corner = pair_mul(part_of(direction, ITERS - 1), part_of(image, ITERS))
    corner = tuple(2.0 * w for w in corner)
    curvature = pair_add(
        curvature, pair_mul(corner, pair_scale(part_of(gram[ITERS - 1], ITERS - 1), -SHIFTS[-1]))
    )

    def combine(factors, count):
        out = None
        for j in range(count):
            term = factors[j : j + 1] * basis[j]
            out = term if out is None else out + term
        return out

    field = combine(residuals[-1], ITERS) * diag
    drop = combine(image[0], ITERS + 1) * diag
    pressure = combine(solution_at[0], ITERS - 1)
    along = combine(direction[0], ITERS)
    wait_replicas(row_recv)

    def row_combine(factors, count, t):
        out = None
        for j in range(count):
            term = factors[j : j + 1] * tb[j, t]
            out = term if out is None else out + term
        return out

    gb[0:8, :] = jnp.zeros((8, SLOT), F32)
    peaks = [None] * ITERS

    def raise_peak(k, values):
        values = jnp.abs(values)
        peaks[k] = values if peaks[k] is None else jnp.maximum(peaks[k], values)

    row_fields = []
    for t in range(2 * XLEN):
        for k in range(ITERS - 1):
            values = row_combine(residuals[k], k + 2, t)
            raise_peak(k, values)
        row_fields.append((values, row_combine(image[0], ITERS + 1, t)))
    for k in range(ITERS - 1):
        gb[k : k + 1, :] = jnp.max(peaks[k], axis=0, keepdims=True)
    wait_last_tower()
    last = tuple(jnp.broadcast_to(w, (8, SLOT)) for w in pairs_of(b2, ZLEN))
    step = pair_div(rz, pair_add(curvature, pair_mul(corner, last)))[0][0:1]
    pressure = pressure + step * along
    field = field - step * drop
    for values, change in row_fields:
        raise_peak(ITERS - 1, values - step * change)
    gb[ITERS - 1 : ITERS, :] = jnp.max(peaks[ITERS - 1], axis=0, keepdims=True)
    peak = jnp.max(gb[0:8, :], axis=1, keepdims=True)
    peak_row = jnp.sum(jnp.where(sub8 == lane8, peak, 0.0), axis=0, keepdims=True)
    wait_peaks = gather(
        [peak_row], p1s, p1, wall_mate, WALL_STEPS, y * ZLEN + z, red_recv.at[2], False
    )

    density = rb[1, pl.ds(8, ROWS), :]
    for r in range(ROWS):
        osb[r, 0:1, :] = density[r : r + 1, :]
        osb[r, 1:2, :] = pressure[r : r + 1, :]
        osb[r, 2:3, :] = field[r : r + 1, :]
    for k in range(GX):
        wanted = jnp.logical_or(a != k, group != q)
        copy = pltpu.make_async_remote_copy(
            src_ref=osb.at[pl.ds(2 * k, 2)],
            dst_ref=ob.at[place],
            send_sem=out_send,
            recv_sem=out_recv,
            device_id=(k, group),
            device_id_type=MESH,
        )
        pl.when(wanted)(copy.start)
    local = pltpu.make_async_copy(osb.at[pl.ds(2 * a, 2)], ob.at[place], out_recv)
    pl.when(group == q)(local.start)

    wait_peaks()
    pltpu.make_async_copy(ob, ob, out_recv).wait()

    for wait in sends:
        wait()
    wait_replicas(row_send)
    for sem, kept, cell in ((in_send, sbuf, 1), (out_send, osb, 2)):
        some, all_ = kept.at[pl.ds(0, (GX - 1) * cell)], kept.at[pl.ds(0, GX * cell)]
        pl.when(home == q)(pltpu.make_async_copy(some, some, sem).wait)
        pl.when(home != q)(pltpu.make_async_copy(all_, all_, sem).wait)
    planes = part.at[0, pl.ds(0, 4 * len(PLANE_STEPS))]
    total_sent = part.at[0:2, pl.ds(0, 2 * len(PLANE_STEPS) + 2 * len(TOWER_STEPS) + len(WALL_STEPS) // 2)]
    pl.when(core == 0)(pltpu.make_async_copy(planes, planes, red_send).wait)
    pl.when(core == 1)(pltpu.make_async_copy(total_sent, total_sent, red_send).wait)


def finish(ob, p1, dens_ref, pres_ref, resid_ref, peaks_ref):
    for r in range(2):
        for c in range(GX):
            dens_ref[r, c : c + 1, :] = ob[c, r, 0:1, :]
            pres_ref[r, c : c + 1, :] = ob[c, r, 1:2, :]
            resid_ref[r, c : c + 1, :] = ob[c, r, 2:3, :]
    peaks_ref[...] = jnp.max(p1[...], axis=0)[0, :ITERS]


def shard(offsets, masses, counts, source):
    block = jax.ShapeDtypeStruct((2, GX, SLOT), F32)
    vmem = pl.BlockSpec(memory_space=pltpu.VMEM)
    dma = pltpu.SemaphoreType.DMA
    cells = (ROWS, SLOT, SLOT)
    gathered, peaks = pl.pallas_call(
        body,
        out_shape=(
            pltpu.VMEM((GX, 2, 4, SLOT), F32),
            pltpu.VMEM((GX // 2 * ZLEN, 1, SLOT), F32),
        ),
        in_specs=[pl.BlockSpec(memory_space=pl.ANY)] * 4,
        out_specs=(pl.BlockSpec(memory_space=pl.ANY),) * 2,
        scratch_shapes=[
            pltpu.VMEM((2, 2, GX, SLOT), F32),
            pltpu.VMEM((2, GX, SLOT), F32),
            pltpu.SMEM((2, GX), jnp.int32),
            pltpu.VMEM((2, GX, SLOT), F32),
            pltpu.VMEM((GX, 2, 4, SLOT), F32),
            pltpu.VMEM((3, ROWS + 2, 4, SLOT), F32),
            pltpu.VMEM(cells, F32),
            pltpu.VMEM(cells, F32),
            pltpu.VMEM(cells, F32),
            pltpu.VMEM((ROWS, 9, SLOT, SLOT), F32),
            pltpu.VMEM(cells, F32),
            pltpu.VMEM((3, 32, SLOT), F32),
            pltpu.VMEM((ITERS, 3, 32, SLOT), F32),
            pltpu.VMEM((2, ROWS, SLOT), F32),
            pltpu.VMEM((ROWS, SLOT), F32),
            pltpu.VMEM((SLOT, SLOT), F32),
            pltpu.VMEM((1, 2, SLOT), F32),
            pltpu.VMEM((PLANE, 2, SLOT), F32),
            pltpu.VMEM((1, 2, SLOT), F32),
            pltpu.VMEM((ZLEN, 2, SLOT), F32),
            pltpu.VMEM((1, 2, SLOT), F32),
            pltpu.VMEM((PLANE, 2, SLOT), F32),
            pltpu.VMEM((1, 2, SLOT), F32),
            pltpu.VMEM((ZLEN, 2, SLOT), F32),
            pltpu.VMEM((1, 1, SLOT), F32),
            pltpu.VMEM((ROWS, 4, SLOT), F32),
            pltpu.VMEM((ITERS + 1, 2 * XLEN, ROWS, SLOT), F32),
            dma((4,)),
            dma,
            dma,
            dma,
            dma((2,)),
            dma,
            dma((2,)),
            dma((ITERS,)),
            dma((ITERS, 2)),
            dma,
            dma((5,)),
            dma,
            dma,
            dma,
            dma,
        ],
        compiler_params=pltpu.CompilerParams(collective_id=0, has_side_effects=True),
    )(offsets, masses, counts, source)
    return pl.pallas_call(
        finish,
        out_shape=(block, block, block, jax.ShapeDtypeStruct((ITERS,), F32)),
        in_specs=[vmem, vmem],
        out_specs=(vmem, vmem, vmem, vmem),
    )(*(pltpu.with_memory_space_constraint(u, pltpu.VMEM) for u in (gathered, peaks)))


def solution(mesh):
    return jax.shard_map(
        shard,
        mesh=mesh,
        in_specs=(P(None, "gx", "gy", None), P("gx", "gy", None), P("gx", "gy"), P("gx", "gy", None)),
        out_specs=(P("gx", "gy", None), P("gx", "gy", None), P("gx", "gy", None), P()),
        check_vma=False,
    )
```
